256 devices in a mesh: paths: 8 (over x, core), cpty: 32 (over z, y).
Axes of the slice: x: 4, y: 4, z: 8, core: 2. Of those that a mesh axis runs over, the one named last changes fastest.
Arguments:
- factors: bfloat16 [64, 12288], P(None, 'paths'), may hold values from -6 to 6
- loadings: bfloat16 [64, 65536], P(None, 'cpty'), may hold values from -2 to 2
- notional: bfloat16 [65536], P('cpty'), may hold values from 0.25 to 0.796875
- strike: bfloat16 [65536], P('cpty'), may hold values from 2 to 8
- curvature: bfloat16 [65536], P('cpty'), may hold values from 1 to 3
- trade_cpty: int32 [65536], P('cpty'), may hold values from 0 to 4095, as said below
Outputs:
- exposure: bfloat16 [12288, 4096], P('paths', 'cpty')
- moment: float32 [4096, 4096], P('paths', 'cpty')
The draws below stay inside these ranges and needn't reach their ends.
Inputs may be any that keep to these rules, and one draw needn't show every extreme that they name: `trade_cpty`: of the trades in the book of one index of cpty, at most 128 belong to the counterparties numbered k * 128 to (k + 1) * 128 - 1 for any k; in every draw some such k receives exactly 128 from every book.
All inputs are finite; a program needn't handle non-finite values.
Results may differ from the reference program's by a relative error of at most 0.0064.
Values may be sent and summed in bfloat16 or wider, within the bound.
A program may use at most 128 MiB of HBM per device.

```python
import math
import jax
import jax.numpy as jnp
from jax import lax

F = 64
CP_DEV = 128
TR_DEV = 2048
SLOT = 128
PATHS = 12288
CPTY = 4096
TRADES = 65536


def draw_trade_cpty(key, part):
    block_count = TRADES // TR_DEV
    owner_count = CPTY // CP_DEV
    base = jax.random.fold_in(key, 11)
    key_heavy, key_blocks = jax.random.split(base, 2)
    heavy_owner = jax.random.randint(key_heavy, (), 0, owner_count)

    def one_block(block_key):
        key_slots, key_shuffle, key_local = jax.random.split(block_key, 3)
        others = jax.random.permutation(key_slots, (owner_count - 1) * SLOT)[:TR_DEV - SLOT] // SLOT
        others = others + (others >= heavy_owner).astype(jnp.int32)
        owners = jnp.concatenate([jnp.full((SLOT,), heavy_owner, jnp.int32), others.astype(jnp.int32)])
        owners = jax.random.permutation(key_shuffle, owners)
        local_ids = jax.random.randint(key_local, (TR_DEV,), 0, CP_DEV)
        return owners * CP_DEV + local_ids
    result = jax.vmap(one_block)(jax.random.split(key_blocks, block_count))
    return result.reshape(-1).astype(jnp.int32)


def levels(rng, dims, cuts, low, top_value):
    factor_of = 1.0
    for dim, parts in cuts:
        heights = jax.random.uniform(jax.random.fold_in(jax.random.fold_in(rng, 6), dim), (parts,), jnp.float32, low / len(cuts), top_value / len(cuts))
        factor_of = factor_of * jnp.repeat(jnp.exp(heights), dims[dim] // parts).reshape((-1,) + (1,) * (len(dims) - 1 - dim))
    return factor_of


def normal_values(stream_key, dims, spread, most, cuts=(), held_as=jnp.bfloat16):
    gain = levels(stream_key, dims, cuts, -0.22, 0.18) if cuts else 1.0
    drawn = jax.random.normal(stream_key, dims, jnp.float32) * spread * gain
    return jnp.minimum(jnp.maximum(drawn, -most), most).astype(held_as)


def setup_inputs(seed: int = 0) -> dict:
    streams_of = jax.random.split(jax.random.key(seed), 7)
    return {
        "factors": normal_values(streams_of[0], (F, PATHS), 1.0, 6.0, ((1, 8),)),
        "loadings": normal_values(streams_of[1], (F, TRADES), (F // 9) ** -0.5, 2.0, ((1, 32),)),
        "notional": jnp.clip(jnp.exp(math.log(0.796875) - 1.1592369 * jax.random.uniform(streams_of[2], (TRADES,), jnp.float32) ** levels(streams_of[2], (TRADES,), ((0, 32),), -0.2, 0.2)), 0.25, 0.796875).astype(jnp.bfloat16),
        "strike": jnp.clip(2.0 + 6.0 * jax.random.uniform(streams_of[3], (TRADES,), jnp.float32) ** levels(streams_of[3], (TRADES,), ((0, 32),), -0.2, 0.2), 2.0, 8.0).astype(jnp.bfloat16),
        "curvature": jnp.clip(1.0 + 2.0 * jax.random.uniform(streams_of[4], (TRADES,), jnp.float32) ** levels(streams_of[4], (TRADES,), ((0, 32),), -0.2, 0.2), 1.0, 3.0).astype(jnp.bfloat16),
        "trade_cpty": draw_trade_cpty(jax.random.fold_in(streams_of[6], 71), 0),
    }


def reference(factors, loadings, notional, strike, curvature, trade_cpty):
    block_count = TRADES // TR_DEV
    load_blocks = jnp.transpose(loadings.reshape(F, block_count, TR_DEV), (1, 0, 2))
    note_blocks = notional.reshape(block_count, TR_DEV)
    strike_blocks = strike.reshape(block_count, TR_DEV)
    curve_blocks = curvature.reshape(block_count, TR_DEV)
    cpty_blocks = trade_cpty.reshape(block_count, TR_DEV).astype(jnp.int32)
    drivers = jnp.transpose(factors)

    def accumulate(carried, pieces):
        loading_cols, note_part, strike_part, curve_part, cpty_ids = pieces
        linear = jnp.dot(drivers, loading_cols, preferred_element_type=jnp.float32)
        value = note_part.astype(jnp.float32) * (linear + curve_part.astype(jnp.float32) * jnp.tanh(linear - strike_part.astype(jnp.float32)))
        value = value.astype(jnp.bfloat16)
        netted_part = jax.ops.segment_sum(jnp.transpose(value.astype(jnp.float32)), cpty_ids, num_segments=CPTY)
        return carried + netted_part, None

    start_sum = jnp.zeros((CPTY, PATHS), jnp.float32)
    netted_rows, _ = lax.scan(accumulate, start_sum, (load_blocks, note_blocks, strike_blocks, curve_blocks, cpty_blocks))
    exposure = jnp.maximum(jnp.transpose(netted_rows), 0.0).astype(jnp.bfloat16)
    moment = jnp.dot(jnp.transpose(exposure), exposure, preferred_element_type=jnp.float32) / PATHS
    return exposure, moment
```

```python
import jax
import jax.numpy as jnp
from jax import lax
from jax.experimental import pallas as pl
from jax.experimental.pallas import tpu as pltpu
from jax.sharding import PartitionSpec as P

NP, NZ, NY = 8, 8, 4
CP = 128
ROWS = 80
SLOT = 128
F = 64
CH = 4
BF, F32 = jnp.bfloat16, jnp.float32
NT = (((1,), (1,)), ((), ()))


def remote(src, dst, ssem, rsem, p, c):
    return pltpu.make_async_remote_copy(
        src_ref=src, dst_ref=dst, send_sem=ssem, recv_sem=rsem,
        device_id={"paths": p, "cpty": c}, device_id_type=pl.DeviceIdType.MESH,
    )


def kernel(fac_ref, load_ref, term_ref, id_ref, exp_ref, mom_ref,
           desc, pack, trades, hot, ft, net, own, at, rm, rp, acc, rsb, rr, fs, fr,
           s1, r1, s2, r2, sy, ry, szp, rzp, szm, rzm, srs, rrs, sf, rf):
    p = lax.axis_index("paths")
    c = lax.axis_index("cpty")
    z, y = c // NY, c % NY
    paths = fac_ref.shape[1]
    rows = paths // CH
    count = id_ref.shape[1]
    first = lax.rem(p - c + 32, 8)
    targets = [first + 8 * i for i in range(4)]
    up, down = lax.rem(z + 1, NZ) * NY + y, lax.rem(z + NZ - 1, NZ) * NY + y

    barrier = pltpu.get_barrier_semaphore()

    def greet(pp, cc):
        pl.semaphore_signal(barrier, inc=1, device_id={"paths": pp, "cpty": cc},
                            device_id_type=pl.DeviceIdType.MESH)

    for k in targets:
        @pl.when(k != c)
        def _(k=k):
            greet(p, k)
    for r in range(1, NP):
        greet(lax.rem(p + r, NP), c)
    greet(p, up)
    greet(p, down)
    for r in range(1, NY):
        greet(p, z * NY + lax.rem(y + r, NY))

    desc[0:F, :] = load_ref[...]
    desc[F:ROWS, :] = term_ref[...]
    ids = id_ref[...]
    owner = ids // CP
    block = 256
    upper = (lax.broadcasted_iota(jnp.int32, (block, block), 0)
             < lax.broadcasted_iota(jnp.int32, (block, block), 1)).astype(BF)
    eq = (lax.broadcasted_iota(jnp.int32, (NZ * NY, count), 0) == owner).astype(F32)
    base = jnp.zeros((NZ * NY, 1), F32)
    ranks = []
    for b in range(count // block):
        part = eq[:, b * block:(b + 1) * block]
        before = jnp.dot(part.astype(BF), upper, preferred_element_type=F32) + base
        base = base + jnp.sum(part, axis=1, keepdims=True)
        ranks.append(jnp.sum(part * before, axis=0, keepdims=True))
    rank = jnp.concatenate(ranks, axis=1).astype(jnp.int32)
    mine = lax.rem(owner + c, 8) == p
    code = jnp.where(mine, (owner // 8) * SLOT + rank, -1)
    total = jnp.zeros((ROWS, 4 * SLOT), F32)
    step = 512
    for b in range(count // step):
        cols = slice(b * step, (b + 1) * step)
        chosen = (lax.broadcasted_iota(jnp.int32, (4 * SLOT, step), 0) == code[:, cols]).astype(F32).astype(BF)
        total = total + lax.dot_general(desc[:, cols], chosen, NT, preferred_element_type=F32)
    for i in range(4):
        pack[i] = total[:, i * SLOT:(i + 1) * SLOT].astype(BF)
    ft[...] = jnp.transpose(fac_ref[...].astype(F32)).astype(BF)

    pl.semaphore_wait(barrier, NP - 1 + 2 + NY - 1 + 4 - (lax.rem(2 * c, 8) == p).astype(jnp.int32))

    place = c // 8
    for i, k in enumerate(targets):
        copy = remote(pack.at[i], trades.at[p, place], s1.at[i], r1.at[place], p, k)

        @pl.when(k != c)
        def _(copy=copy):
            copy.start()

        @pl.when(k == c)
        def _(i=i):
            trades[p, place] = pack[i]
    for i, k in enumerate(targets):
        arrive = remote(pack.at[i], trades.at[p, i], s1.at[i], r1.at[i], p, k)

        @pl.when(k != c)
        def _(arrive=arrive):
            arrive.wait_recv()
    spread = []
    for r in range(1, NP):
        copy = remote(trades.at[p], trades.at[p], s2.at[r], r2.at[r], lax.rem(p + r, NP), c)
        copy.start()
        spread.append(copy)

    def tile_of(pp):
        t = trades[pp]
        return jnp.concatenate([t[i] for i in range(4)], axis=1)

    def price(j, pp):
        full = tile_of(pp)
        terms = full[F:ROWS, :].astype(F32)
        lin = jnp.dot(ft[j * rows:(j + 1) * rows, :], full[0:F, :], preferred_element_type=F32)
        value = terms[0:1, :] * (lin + terms[2:3, :] * jnp.tanh(lin - terms[1:2, :]))
        return lax.dot_general(value.astype(BF), hot[pp], NT, preferred_element_type=F32)

    sends = []

    def go(copy):
        copy.start()
        sends.append(copy)

    def ring(s, j):
        pair = []
        if s < 3 or j < 2:
            src = own.at[j] if s == 0 else rm.at[s - 1, j]
            pair.append(remote(src, rm.at[s, j], szp.at[s, j], rzp.at[s, j], p, up))
        if s < 3 or j >= 2:
            src = own.at[j] if s == 0 else rp.at[s - 1, j]
            pair.append(remote(src, rp.at[s, j], szm.at[s, j], rzm.at[s, j], p, down))
        return pair

    def add(slot, j, value):
        if j == 0:
            acc[slot] = value
        else:
            acc[slot] += value

    def left(j):
        return at[j].reshape(NY * CP, rows)

    def ship(d):
        rsb[d] = acc[d].astype(BF)
        zz = lax.rem(z + d, NZ)
        r = lax.rem(zz - p + NP, NP)
        copy = remote(rsb.at[d], rr.at[r], srs.at[d], rrs.at[r], zz, c)

        @pl.when(r != 0)
        def _():
            copy.start()

    for t in range(CH + 4):
        if t < CH:
            j = t
            net[...] = jnp.zeros_like(net)

            def body(r, _):
                pp = lax.rem(p + r, NP)
                if j == 0:
                    @pl.when(r > 0)
                    def _():
                        src = lax.rem(p - r + NP, NP)
                        remote(trades.at[src], trades.at[src], s2.at[r], r2.at[r], src, c).wait_recv()

                    pp = lax.rem(p - r + NP, NP)
                    t4 = trades[pp]
                    label = jnp.concatenate([t4[i][F:ROWS, :] for i in range(4)], axis=1).astype(F32)[3:4, :]
                    hot[pp] = (lax.broadcasted_iota(jnp.int32, (CP, 4 * SLOT), 0).astype(F32) == label).astype(F32).astype(BF)
                net[...] += price(j, pp)
                return 0

            lax.fori_loop(0, NP, body, 0)
            block_f = jnp.maximum(net[...], 0.0)
            block_b = block_f.astype(BF)
            own[j] = block_b
            exp_ref[j * rows:(j + 1) * rows, :] = block_b
            at[j, y] = jnp.transpose(block_f).astype(BF)
            for copy in ring(0, j):
                go(copy)
            for r in range(1, NY):
                go(remote(at.at[j, y], at.at[j, y], sy.at[j, r], ry.at[j, r], p, z * NY + lax.rem(y + r, NY)))
        for s in (1, 2, 3):
            j = t - s
            if 0 <= j < CH:
                for copy in ring(s - 1, j):
                    copy.wait_recv()
                for copy in ring(s, j):
                    go(copy)
        j = t - 1
        if 0 <= j < CH:
            for r in range(1, NY):
                src = lax.rem(y + NY - r, NY)
                remote(at.at[j, src], at.at[j, src], sy.at[j, r], ry.at[j, r], p, z * NY + src).wait_recv()
            add(0, j, jnp.dot(left(j), own[j], preferred_element_type=F32))
        for s in (1, 2, 3):
            j = t - s
            if 0 <= j < CH:
                both = jnp.concatenate([rm[s - 1, j], rp[s - 1, j]], axis=1)
                res = jnp.dot(left(j), both, preferred_element_type=F32)
                add(NZ - s, j, res[:, :CP])
                add(s, j, res[:, CP:])
        j = t - 4
        if 0 <= j < CH:
            for copy in ring(3, j):
                copy.wait_recv()
            far = rm[3, j] if j < 2 else rp[3, j]
            add(4, j, jnp.dot(left(j), far, preferred_element_type=F32))
        if t >= 4:
            done = {4: (0, 1, 7), 5: (2, 6), 6: (3, 5), 7: (4,)}[t]
            for d in done:
                ship(d)

    whole = rsb[lax.rem(p - z + NP, NP)].astype(F32)
    for r in range(1, NP):
        src = lax.rem(p - r + NP, NP)
        remote(rsb.at[0], rr.at[r], srs.at[0], rrs.at[r], src, c).wait_recv()
        whole = whole + rr[r].astype(F32)
    whole = whole * (1.0 / (paths * NP))
    for i in range(NY):
        fs[i] = jnp.transpose(whole[i * CP:(i + 1) * CP, :]).astype(BF)
    for r in range(1, NY):
        yy = lax.rem(y + r, NY)
        go(remote(fs.at[yy], fr.at[r], sf.at[r], rf.at[r], p, z * NY + yy))
    mom_ref[y] = fs[y].astype(F32)
    for r in range(1, NY):
        src = lax.rem(y + NY - r, NY)
        remote(fs.at[src], fr.at[r], sf.at[r], rf.at[r], p, z * NY + src).wait_recv()
        mom_ref[src] = fr[r].astype(F32)

    for i, k in enumerate(targets):
        copy = remote(pack.at[i], trades.at[p, place], s1.at[i], r1.at[place], p, k)

        @pl.when(k != c)
        def _(copy=copy):
            copy.wait_send()
    for copy in spread:
        copy.wait_send()
    for copy in sends:
        copy.wait_send()
    for d in range(NZ):
        zz = lax.rem(z + d, NZ)
        r = lax.rem(zz - p + NP, NP)
        copy = remote(rsb.at[d], rr.at[r], srs.at[d], rrs.at[r], zz, c)

        @pl.when(r != 0)
        def _(copy=copy):
            copy.wait_send()


def on_device(factors, loadings, notional, strike, curvature, trade_cpty):
    count, paths = loadings.shape[1], factors.shape[1]
    rows = paths // CH
    local = (trade_cpty % CP).astype(BF)
    terms = jnp.concatenate(
        [jnp.stack([notional, strike, curvature, local]), jnp.zeros((ROWS - F - 4, count), BF)], axis=0)
    vmem = pl.BlockSpec(memory_space=pltpu.VMEM)
    dma = pltpu.SemaphoreType.DMA
    exposure, moment = pl.pallas_call(
        kernel,
        out_shape=(jax.ShapeDtypeStruct((paths, CP), BF), jax.ShapeDtypeStruct((NY, CP, CP), F32)),
        in_specs=[vmem] * 4,
        out_specs=(vmem, vmem),
        scratch_shapes=[
            pltpu.VMEM((ROWS, count), BF),
            pltpu.VMEM((4, ROWS, SLOT), BF),
            pltpu.VMEM((NP, 4, ROWS, SLOT), BF),
            pltpu.VMEM((NP, CP, 4 * SLOT), BF),
            pltpu.VMEM((paths, F), BF),
            pltpu.VMEM((rows, CP), F32),
            pltpu.VMEM((CH, rows, CP), BF),
            pltpu.VMEM((CH, NY, CP, rows), BF),
            pltpu.VMEM((4, CH, rows, CP), BF),
            pltpu.VMEM((4, CH, rows, CP), BF),
            pltpu.VMEM((NZ, NY * CP, CP), F32),
            pltpu.VMEM((NZ, NY * CP, CP), BF),
            pltpu.VMEM((NP, NY * CP, CP), BF),
            pltpu.VMEM((NY, CP, CP), BF),
            pltpu.VMEM((NY, CP, CP), BF),
            dma((4,)), dma((4,)), dma((NP,)), dma((NP,)),
            dma((CH, NY)), dma((CH, NY)),
            dma((4, CH)), dma((4, CH)), dma((4, CH)), dma((4, CH)),
            dma((NZ,)), dma((NP,)), dma((NY,)), dma((NY,)),
        ],
        compiler_params=pltpu.CompilerParams(
            collective_id=0, has_side_effects=True, vmem_limit_bytes=50 * 1024 * 1024),
    )(factors, loadings, terms, trade_cpty[None, :])
    return exposure, moment.reshape(NY * CP, CP)


def solution(mesh):
    in_specs = (P(None, "paths"), P(None, "cpty"), P("cpty"), P("cpty"), P("cpty"), P("cpty"))
    out_specs = (P("paths", "cpty"), P("paths", "cpty"))
    return jax.shard_map(
        on_device, mesh=mesh, in_specs=in_specs, out_specs=out_specs, check_vma=False
    )
```

```python
import jax
import jax.numpy as jnp
from jax import lax
from jax.experimental import pallas as pl
from jax.experimental.pallas import tpu as pltpu
from jax.sharding import PartitionSpec as P

NP, NX, NZ, NY = 8, 4, 8, 4
FAR = 4
CP = 128
ROWS = 80
SLOT = 128
F = 64
CH = 4
BF, F32 = jnp.bfloat16, jnp.float32
NT = (((1,), (1,)), ((), ()))


def remote(src, dst, ssem, rsem, p, c):
    return pltpu.make_async_remote_copy(
        src_ref=src, dst_ref=dst, send_sem=ssem, recv_sem=rsem,
        device_id={"paths": p, "cpty": c}, device_id_type=pl.DeviceIdType.MESH,
    )


def kernel(fac_ref, load_ref, term_ref, id_ref, exp_ref, mom_ref,
           desc, pack, trades, hot, ft, net, own, at, ring_in, acc, rsb, rr, keep, turn, fa, fb,
           s1, r1, s2, r2, sy, ry, sz, rz, srs, rrs, sa, ra, sb, rb):
    p = lax.axis_index("paths")
    c = lax.axis_index("cpty")
    z, y = c // NY, c % NY
    paths = fac_ref.shape[1]
    rows = paths // CH
    count = id_ref.shape[1]
    first = lax.rem(p - c + 32, 8)
    targets = [first + 8 * i for i in range(4)]
    x, core = p // 2, p % 2
    sign = 1 - 2 * core
    ahead, behind = lax.rem(z - sign + NZ, NZ), lax.rem(z + sign + NZ, NZ)
    y_ahead, y_back = lax.rem(y - sign + NY, NY), lax.rem(y + sign + NY, NY)
    far_here, far_ahead = z // FAR, ahead // FAR

    barrier = pltpu.get_barrier_semaphore()

    def greet(pp, cc):
        pl.semaphore_signal(barrier, inc=1, device_id={"paths": pp, "cpty": cc},
                            device_id_type=pl.DeviceIdType.MESH)

    for k in targets:
        @pl.when(k != c)
        def _(k=k):
            greet(p, k)
    for r in range(1, NP):
        greet(lax.rem(p + r, NP), c)
    greet(p, ahead * NY + y)
    greet(p, behind * NY + y)
    for r in range(1, NY):
        greet(p, z * NY + lax.rem(y + r, NY))

    desc[0:F, :] = load_ref[...]
    desc[F:ROWS, :] = term_ref[...]
    ids = id_ref[...]
    owner = ids // CP
    block = 256
    upper = (lax.broadcasted_iota(jnp.int32, (block, block), 0)
             < lax.broadcasted_iota(jnp.int32, (block, block), 1)).astype(BF)
    eq = (lax.broadcasted_iota(jnp.int32, (NZ * NY, count), 0) == owner).astype(F32)
    base = jnp.zeros((NZ * NY, 1), F32)
    ranks = []
    for b in range(count // block):
        part = eq[:, b * block:(b + 1) * block]
        before = jnp.dot(part.astype(BF), upper, preferred_element_type=F32) + base
        base = base + jnp.sum(part, axis=1, keepdims=True)
        ranks.append(jnp.sum(part * before, axis=0, keepdims=True))
    rank = jnp.concatenate(ranks, axis=1).astype(jnp.int32)
    mine = lax.rem(owner + c, 8) == p
    code = jnp.where(mine, (owner // 8) * SLOT + rank, -1)
    total = jnp.zeros((ROWS, 4 * SLOT), F32)
    step = 512
    for b in range(count // step):
        cols = slice(b * step, (b + 1) * step)
        chosen = (lax.broadcasted_iota(jnp.int32, (4 * SLOT, step), 0) == code[:, cols]).astype(F32).astype(BF)
        total = total + lax.dot_general(desc[:, cols], chosen, NT, preferred_element_type=F32)
    for i in range(4):
        pack[i] = total[:, i * SLOT:(i + 1) * SLOT].astype(BF)
    ft[...] = jnp.transpose(fac_ref[...].astype(F32)).astype(BF)

    pl.semaphore_wait(barrier, NP - 1 + 2 + NY - 1 + 4 - (lax.rem(2 * c, 8) == p).astype(jnp.int32))

    place = c // 8
    for i, k in enumerate(targets):
        copy = remote(pack.at[i], trades.at[p, place], s1.at[i], r1.at[place], p, k)

        @pl.when(k != c)
        def _(copy=copy):
            copy.start()

        @pl.when(k == c)
        def _(i=i):
            trades[p, place] = pack[i]
    for i, k in enumerate(targets):
        arrive = remote(pack.at[i], trades.at[p, i], s1.at[i], r1.at[i], p, k)

        @pl.when(k != c)
        def _(arrive=arrive):
            arrive.wait_recv()
    spread = []
    for r in range(1, NP):
        copy = remote(trades.at[p], trades.at[p], s2.at[r], r2.at[r], lax.rem(p + r, NP), c)
        copy.start()
        spread.append(copy)

    def tile_of(pp):
        t = trades[pp]
        return jnp.concatenate([t[i] for i in range(4)], axis=1)

    def price(j, pp):
        full = tile_of(pp)
        terms = full[F:ROWS, :].astype(F32)
        lin = jnp.dot(ft[j * rows:(j + 1) * rows, :], full[0:F, :], preferred_element_type=F32)
        value = terms[0:1, :] * (lin + terms[2:3, :] * jnp.tanh(lin - terms[1:2, :]))
        return lax.dot_general(value.astype(BF), hot[pp], NT, preferred_element_type=F32)

    sends = []

    def go(copy):
        copy.start()
        sends.append(copy)

    def ring(s, j):
        src = own.at[j] if s == 0 else ring_in.at[s - 1, j]
        slot = j if s < FAR - 1 else j // 2
        return remote(src, ring_in.at[s, slot], sz.at[s, slot], rz.at[s, slot], p, ahead * NY + y)

    def side(j, way):
        origin = y if way < 2 else y_back
        target = y_back if way == 1 else y_ahead
        return remote(at.at[j, origin], at.at[j, origin], sy.at[j, way], ry.at[j, way], p, z * NY + target)

    def side_wait(j, way):
        origin = (y_back, y_ahead, lax.rem(y + 2, NY))[way]
        remote(at.at[j, origin], at.at[j, origin], sy.at[j, way], ry.at[j, way], p, z * NY + y_back).wait_recv()

    def add(d, j, value, start):
        if start:
            acc[d] = value
        else:
            acc[d] += value

    def left(j):
        return at[j].reshape(NY * CP, rows)

    def cell(d):
        return lax.rem(z + sign * d + NZ, NZ)

    def ship(d):
        rsb[d] = acc[d].reshape(NY, CP, CP).astype(BF)
        for r in range(1, NX):
            xx = lax.rem(x + r, NX)
            go(remote(rsb.at[d, xx], rr.at[d, r], srs.at[d, r], rrs.at[d, r], 2 * xx + core, c))

    def turned(d):
        return remote(turn.at[d], fa.at[core, y], sa.at[d], ra.at[core, y], cell(d), z * NY + x)

    def turned_home(d):
        return (cell(d) == p) & (x == y)

    def direct(d):
        return remote(keep.at[d], fb.at[core, x], sb.at[d], rb.at[core, x], z, cell(d) * NY + y)

    def collect(d):
        whole = acc[d, pl.ds(pl.multiple_of(x * CP, CP), CP), :]
        for r in range(1, NX):
            src = lax.rem(x - r + NX, NX)
            remote(rsb.at[d, src], rr.at[d, r], srs.at[d, r], rrs.at[d, r], 2 * src + core, c).wait_recv()
            whole = whole + rr[d, r].astype(F32)
        whole = whole * (1.0 / (paths * NP))
        if d > 0:
            keep[d] = whole.astype(BF)
            go(direct(d))
        turn[d] = jnp.transpose(whole).astype(BF)

        @pl.when(jnp.logical_not(turned_home(d)))
        def _():
            turned(d).start()

        @pl.when(turned_home(d))
        def _():
            fa[core, y] = turn[d]

    for t in range(CH + FAR):
        if t < CH:
            j = t
            net[...] = jnp.zeros_like(net)

            def body(r, _):
                pp = lax.rem(p + r, NP)
                if j == 0:
                    @pl.when(r > 0)
                    def _():
                        src = lax.rem(p - r + NP, NP)
                        remote(trades.at[src], trades.at[src], s2.at[r], r2.at[r], src, c).wait_recv()

                    pp = lax.rem(p - r + NP, NP)
                    t4 = trades[pp]
                    label = jnp.concatenate([t4[i][F:ROWS, :] for i in range(4)], axis=1).astype(F32)[3:4, :]
                    hot[pp] = (lax.broadcasted_iota(jnp.int32, (CP, 4 * SLOT), 0).astype(F32) == label).astype(F32).astype(BF)
                net[...] += price(j, pp)
                return 0

            lax.fori_loop(0, NP, body, 0)
            block_f = jnp.maximum(net[...], 0.0)
            block_b = block_f.astype(BF)
            own[j] = block_b
            exp_ref[j * rows:(j + 1) * rows, :] = block_b
            at[j, y] = jnp.transpose(block_f).astype(BF)
            go(ring(0, j))
            go(side(j, 0))
            go(side(j, 1))
        for s in range(1, FAR):
            j = t - s
            if 0 <= j < CH:
                ring(s - 1, j).wait_recv()
                if s < FAR - 1:
                    go(ring(s, j))
                else:
                    copy = ring(s, j)

                    @pl.when(far_ahead == j % 2)
                    def _(copy=copy):
                        copy.start()
        j = t - 1
        if 0 <= j < CH:
            side_wait(j, 0)
            go(side(j, 2))
            side_wait(j, 1)
        j = t - 2
        if 0 <= j < CH:
            side_wait(j, 2)
            add(0, j, jnp.dot(left(j), own[j], preferred_element_type=F32), j == 0)
            add(1, j, jnp.dot(left(j), ring_in[0, j], preferred_element_type=F32), j == 0)
            add(2, j, jnp.dot(left(j), ring_in[1, j], preferred_element_type=F32), j == 0)
        j = t - 3
        if 0 <= j < CH:
            add(3, j, jnp.dot(left(j), ring_in[2, j], preferred_element_type=F32), j == 0)
        j = t - FAR
        if 0 <= j < CH:
            @pl.when(far_here == j % 2)
            def _(j=j):
                ring(FAR - 1, j).wait_recv()
                add(FAR, j, jnp.dot(left(j), ring_in[FAR - 1, j // 2], preferred_element_type=F32), j < 2)
        if t == 5:
            for d in (0, 1, 2):
                ship(d)
        if t == 6:
            ship(3)
            for d in (0, 1, 2):
                collect(d)
    ship(FAR)
    collect(3)
    collect(FAR)

    delta = lax.rem(p - z + NZ, NZ)
    mom_ref[...] = jnp.zeros_like(mom_ref)
    for k in range(2):
        near = (delta <= FAR) if k == 0 else ((delta >= FAR) | (delta == 0))
        away = ((delta >= FAR) if k == 0 else ((delta <= FAR) & (delta > 0)))
        for i in range(NY):
            @pl.when(near & jnp.logical_not((core == k) & (i == y) & (x == y)))
            def _(k=k, i=i):
                remote(turn.at[0], fa.at[k, i], sa.at[0], ra.at[k, i], 2 * y + k, z * NY + i).wait_recv()

            @pl.when(near)
            def _(k=k, i=i):
                mom_ref[i] += fa[k, i].astype(F32)

            @pl.when(away)
            def _(k=k, i=i):
                remote(turn.at[0], fb.at[k, i], sb.at[0], rb.at[k, i], 2 * i + k, p * NY + y).wait_recv()
                mom_ref[i] += fb[k, i].astype(F32)

    for i, k in enumerate(targets):
        copy = remote(pack.at[i], trades.at[p, place], s1.at[i], r1.at[place], p, k)

        @pl.when(k != c)
        def _(copy=copy):
            copy.wait_send()
    for copy in spread:
        copy.wait_send()
    for copy in sends:
        copy.wait_send()
    for j in range(CH):
        copy = ring(FAR - 1, j)

        @pl.when(far_ahead == j % 2)
        def _(copy=copy):
            copy.wait_send()
    for d in range(FAR + 1):
        @pl.when(jnp.logical_not(turned_home(d)))
        def _(d=d):
            turned(d).wait_send()


def on_device(factors, loadings, notional, strike, curvature, trade_cpty):
    count, paths = loadings.shape[1], factors.shape[1]
    rows = paths // CH
    local = (trade_cpty % CP).astype(BF)
    terms = jnp.concatenate(
        [jnp.stack([notional, strike, curvature, local]), jnp.zeros((ROWS - F - 4, count), BF)], axis=0)
    vmem = pl.BlockSpec(memory_space=pltpu.VMEM)
    dma = pltpu.SemaphoreType.DMA
    exposure, moment = pl.pallas_call(
        kernel,
        out_shape=(jax.ShapeDtypeStruct((paths, CP), BF), jax.ShapeDtypeStruct((NY, CP, CP), F32)),
        in_specs=[vmem] * 4,
        out_specs=(vmem, vmem),
        scratch_shapes=[
            pltpu.VMEM((ROWS, count), BF),
            pltpu.VMEM((4, ROWS, SLOT), BF),
            pltpu.VMEM((NP, 4, ROWS, SLOT), BF),
            pltpu.VMEM((NP, CP, 4 * SLOT), BF),
            pltpu.VMEM((paths, F), BF),
            pltpu.VMEM((rows, CP), F32),
            pltpu.VMEM((CH, rows, CP), BF),
            pltpu.VMEM((CH, NY, CP, rows), BF),
            pltpu.VMEM((FAR, CH, rows, CP), BF),
            pltpu.VMEM((FAR + 1, NY * CP, CP), F32),
            pltpu.VMEM((FAR + 1, NY, CP, CP), BF),
            pltpu.VMEM((FAR + 1, NX, CP, CP), BF),
            pltpu.VMEM((FAR + 1, CP, CP), BF),
            pltpu.VMEM((FAR + 1, CP, CP), BF),
            pltpu.VMEM((2, NY, CP, CP), BF),
            pltpu.VMEM((2, NX, CP, CP), BF),
            dma((4,)), dma((4,)), dma((NP,)), dma((NP,)),
            dma((CH, 3)), dma((CH, 3)), dma((FAR, CH)), dma((FAR, CH)),
            dma((FAR + 1, NX)), dma((FAR + 1, NX)),
            dma((FAR + 1,)), dma((2, NY)), dma((FAR + 1,)), dma((2, NX)),
        ],
        compiler_params=pltpu.CompilerParams(
            collective_id=0, has_side_effects=True, vmem_limit_bytes=50 * 1024 * 1024),
    )(factors, loadings, terms, trade_cpty[None, :])
    return exposure, moment.reshape(NY * CP, CP)


def solution(mesh):
    in_specs = (P(None, "paths"), P(None, "cpty"), P("cpty"), P("cpty"), P("cpty"), P("cpty"))
    out_specs = (P("paths", "cpty"), P("paths", "cpty"))
    return jax.shard_map(
        on_device, mesh=mesh, in_specs=in_specs, out_specs=out_specs, check_vma=False
    )
```

```python
import jax
import jax.numpy as jnp
from jax import lax
from jax.experimental import pallas as pl
from jax.experimental.pallas import tpu as pltpu
from jax.sharding import PartitionSpec as P

NP, NX, NZ, NY = 8, 4, 8, 4
FAR = 4
CP = 128
ROWS = 80
SLOT = 128
F = 64
CH = 4
BF, F32 = jnp.bfloat16, jnp.float32
NT = (((1,), (1,)), ((), ()))


def remote(src, dst, ssem, rsem, p, c):
    return pltpu.make_async_remote_copy(
        src_ref=src, dst_ref=dst, send_sem=ssem, recv_sem=rsem,
        device_id={"paths": p, "cpty": c}, device_id_type=pl.DeviceIdType.MESH,
    )


def kernel(fac_ref, load_ref, term_ref, id_ref, exp_ref, mom_ref,
           desc, pack, trades, hot, ft, net, own, at, ring_in, acc, rsb, rr, keep, turn, fa, fb,
           s1, r1, s2, r2, sy, ry, sz, rz, srs, rrs, sa, ra, sb, rb):
    p = lax.axis_index("paths")
    c = lax.axis_index("cpty")
    z, y = c // NY, c % NY
    paths = fac_ref.shape[1]
    rows = paths // CH
    count = id_ref.shape[1]
    first = lax.rem(p - c + 32, 8)
    targets = [first + 8 * i for i in range(4)]
    x, core = p // 2, p % 2
    sign = 1 - 2 * core
    ahead, behind = lax.rem(z - sign + NZ, NZ), lax.rem(z + sign + NZ, NZ)
    y_ahead, y_back = lax.rem(y - sign + NY, NY), lax.rem(y + sign + NY, NY)
    far_here, far_ahead = z // FAR, ahead // FAR

    barrier = pltpu.get_barrier_semaphore()

    def greet(pp, cc):
        pl.semaphore_signal(barrier, inc=1, device_id={"paths": pp, "cpty": cc},
                            device_id_type=pl.DeviceIdType.MESH)

    for k in targets:
        @pl.when(k != c)
        def _(k=k):
            greet(p, k)
    for r in range(1, NP):
        greet(lax.rem(p + r, NP), c)
    greet(p, ahead * NY + y)
    greet(p, behind * NY + y)
    for r in range(1, NY):
        greet(p, z * NY + lax.rem(y + r, NY))

    desc[0:F, :] = load_ref[...]
    desc[F:ROWS, :] = term_ref[...]
    ids = id_ref[...]
    owner = ids // CP
    block = 256
    upper = (lax.broadcasted_iota(jnp.int32, (block, block), 0)
             < lax.broadcasted_iota(jnp.int32, (block, block), 1)).astype(BF)
    eq = (lax.broadcasted_iota(jnp.int32, (NZ * NY, count), 0) == owner).astype(F32)
    base = jnp.zeros((NZ * NY, 1), F32)
    ranks = []
    for b in range(count // block):
        part = eq[:, b * block:(b + 1) * block]
        before = jnp.dot(part.astype(BF), upper, preferred_element_type=F32) + base
        base = base + jnp.sum(part, axis=1, keepdims=True)
        ranks.append(jnp.sum(part * before, axis=0, keepdims=True))
    rank = jnp.concatenate(ranks, axis=1).astype(jnp.int32)
    mine = lax.rem(owner + c, 8) == p
    code = jnp.where(mine, (owner // 8) * SLOT + rank, -1)
    total = jnp.zeros((ROWS, 4 * SLOT), F32)
    step = 512
    for b in range(count // step):
        cols = slice(b * step, (b + 1) * step)
        chosen = (lax.broadcasted_iota(jnp.int32, (4 * SLOT, step), 0) == code[:, cols]).astype(F32).astype(BF)
        total = total + lax.dot_general(desc[:, cols], chosen, NT, preferred_element_type=F32)
    for i in range(4):
        pack[i] = total[:, i * SLOT:(i + 1) * SLOT].astype(BF)
    ft[...] = jnp.transpose(fac_ref[...].astype(F32)).astype(BF)

    pl.semaphore_wait(barrier, NP - 1 + 2 + NY - 1 + 4 - (lax.rem(2 * c, 8) == p).astype(jnp.int32))

    place = c // 8
    for i, k in enumerate(targets):
        copy = remote(pack.at[i], trades.at[p, place], s1.at[i], r1.at[place], p, k)

        @pl.when(k != c)
        def _(copy=copy):
            copy.start()

        @pl.when(k == c)
        def _(i=i):
            trades[p, place] = pack[i]
    for i, k in enumerate(targets):
        arrive = remote(pack.at[i], trades.at[p, i], s1.at[i], r1.at[i], p, k)

        @pl.when(k != c)
        def _(arrive=arrive):
            arrive.wait_recv()
    spread = []
    for r in range(1, NP):
        copy = remote(trades.at[p], trades.at[p], s2.at[r], r2.at[r], lax.rem(p + r, NP), c)
        copy.start()
        spread.append(copy)

    def tile_of(pp):
        t = trades[pp]
        return jnp.concatenate([t[i] for i in range(4)], axis=1)

    def price(j, pp):
        full = tile_of(pp)
        terms = full[F:ROWS, :].astype(F32)
        lin = jnp.dot(ft[j * rows:(j + 1) * rows, :], full[0:F, :], preferred_element_type=F32)
        value = terms[0:1, :] * (lin + terms[2:3, :] * jnp.tanh(lin - terms[1:2, :]))
        return lax.dot_general(value.astype(BF), hot[pp], NT, preferred_element_type=F32)

    sends = []

    def go(copy):
        copy.start()
        sends.append(copy)

    def ring(s, j):
        src = own.at[j] if s == 0 else ring_in.at[s - 1, j]
        slot = j if s < FAR - 1 else j // 2
        return remote(src, ring_in.at[s, slot], sz.at[s, slot], rz.at[s, slot], p, ahead * NY + y)

    def side(j, way):
        origin = y if way < 2 else y_back
        target = y_back if way == 1 else y_ahead
        return remote(at.at[j, origin], at.at[j, origin], sy.at[j, way], ry.at[j, way], p, z * NY + target)

    def side_wait(j, way):
        origin = (y_back, y_ahead, lax.rem(y + 2, NY))[way]
        remote(at.at[j, origin], at.at[j, origin], sy.at[j, way], ry.at[j, way], p, z * NY + y_back).wait_recv()

    def add(d, j, value, start):
        if start:
            acc[d] = value
        else:
            acc[d] += value

    def left(j):
        return at[j].reshape(NY * CP, rows)

    def cell(d):
        return lax.rem(z + sign * d + NZ, NZ)

    def ship(d):
        rsb[d] = acc[d].reshape(NY, CP, CP).astype(BF)
        for r in range(1, NX):
            xx = lax.rem(x + r, NX)
            go(remote(rsb.at[d, xx], rr.at[d, r], srs.at[d, r], rrs.at[d, r], 2 * xx + core, c))

    def turned(d):
        return remote(turn.at[d], fa.at[core, y], sa.at[d], ra.at[core, y], cell(d), z * NY + x)

    def turned_home(d):
        return (cell(d) == p) & (x == y)

    def direct(d):
        return remote(keep.at[d], fb.at[core, x], sb.at[d], rb.at[core, x], z, cell(d) * NY + y)

    def collect(d):
        whole = acc[d, pl.ds(pl.multiple_of(x * CP, CP), CP), :]
        for r in range(1, NX):
            src = lax.rem(x - r + NX, NX)
            remote(rsb.at[d, src], rr.at[d, r], srs.at[d, r], rrs.at[d, r], 2 * src + core, c).wait_recv()
            whole = whole + rr[d, r].astype(F32)
        whole = whole * (1.0 / (paths * NP))
        if d > 0:
            keep[d] = whole.astype(BF)
            go(direct(d))
        turn[d] = jnp.transpose(whole).astype(BF)

        @pl.when(jnp.logical_not(turned_home(d)))
        def _():
            turned(d).start()

        @pl.when(turned_home(d))
        def _():
            fa[core, y] = turn[d]

    for t in range(CH + FAR + 1):
        if t < CH:
            j = t
            net[...] = jnp.zeros_like(net)

            def body(r, _):
                pp = lax.rem(p + r, NP)
                if j == 0:
                    @pl.when(r > 0)
                    def _():
                        src = lax.rem(p - r + NP, NP)
                        remote(trades.at[src], trades.at[src], s2.at[r], r2.at[r], src, c).wait_recv()

                    pp = lax.rem(p - r + NP, NP)
                    t4 = trades[pp]
                    label = jnp.concatenate([t4[i][F:ROWS, :] for i in range(4)], axis=1).astype(F32)[3:4, :]
                    hot[pp] = (lax.broadcasted_iota(jnp.int32, (CP, 4 * SLOT), 0).astype(F32) == label).astype(F32).astype(BF)
                net[...] += price(j, pp)
                return 0

            lax.fori_loop(0, NP, body, 0, unroll=1 if j == 0 else NP)
            block_f = jnp.maximum(net[...], 0.0)
            block_b = block_f.astype(BF)
            own[j] = block_b
            exp_ref[j * rows:(j + 1) * rows, :] = block_b
            at[j, y] = jnp.transpose(block_f).astype(BF)
            go(ring(0, j))
            go(side(j, 0))
            go(side(j, 1))
        for s in range(1, FAR):
            j = t - 1 - s
            if 0 <= j < CH:
                ring(s - 1, j).wait_recv()
                if s < FAR - 1:
                    go(ring(s, j))
                else:
                    copy = ring(s, j)

                    @pl.when(far_ahead == j % 2)
                    def _(copy=copy):
                        copy.start()
        j = t - 2
        if 0 <= j < CH:
            side_wait(j, 0)
            go(side(j, 2))
            side_wait(j, 1)
        j = t - 3
        if 0 <= j < CH:
            side_wait(j, 2)
            add(0, j, jnp.dot(left(j), own[j], preferred_element_type=F32), j == 0)
            for d in (1, 2):
                add(d, j, jnp.dot(left(j), ring_in[d - 1, j], preferred_element_type=F32), j == 0)
            if j == CH - 1:
                for d in (0, 1, 2):
                    ship(d)
        j = t - 4
        if 0 <= j < CH:
            add(3, j, jnp.dot(left(j), ring_in[2, j], preferred_element_type=F32), j == 0)
            if j == CH - 1:
                ship(3)
        j = t - 1 - FAR
        if 0 <= j < CH:
            @pl.when(far_here == j % 2)
            def _(j=j):
                ring(FAR - 1, j).wait_recv()
                add(FAR, j, jnp.dot(left(j), ring_in[FAR - 1, j // 2], preferred_element_type=F32), j < 2)
    ship(FAR)
    for d in range(FAR + 1):
        collect(d)

    delta = lax.rem(p - z + NZ, NZ)
    mom_ref[...] = jnp.zeros_like(mom_ref)
    for k in range(2):
        near = (delta <= FAR) if k == 0 else ((delta >= FAR) | (delta == 0))
        away = ((delta >= FAR) if k == 0 else ((delta <= FAR) & (delta > 0)))
        for i in range(NY):
            @pl.when(near & jnp.logical_not((core == k) & (i == y) & (x == y)))
            def _(k=k, i=i):
                remote(turn.at[0], fa.at[k, i], sa.at[0], ra.at[k, i], 2 * y + k, z * NY + i).wait_recv()

            @pl.when(near)
            def _(k=k, i=i):
                mom_ref[i] += fa[k, i].astype(F32)

            @pl.when(away)
            def _(k=k, i=i):
                remote(turn.at[0], fb.at[k, i], sb.at[0], rb.at[k, i], 2 * i + k, p * NY + y).wait_recv()
                mom_ref[i] += fb[k, i].astype(F32)

    for i, k in enumerate(targets):
        copy = remote(pack.at[i], trades.at[p, place], s1.at[i], r1.at[place], p, k)

        @pl.when(k != c)
        def _(copy=copy):
            copy.wait_send()
    for copy in spread:
        copy.wait_send()
    for copy in sends:
        copy.wait_send()
    for j in range(CH):
        copy = ring(FAR - 1, j)

        @pl.when(far_ahead == j % 2)
        def _(copy=copy):
            copy.wait_send()
    for d in range(FAR + 1):
        @pl.when(jnp.logical_not(turned_home(d)))
        def _(d=d):
            turned(d).wait_send()


def on_device(factors, loadings, notional, strike, curvature, trade_cpty):
    count, paths = loadings.shape[1], factors.shape[1]
    rows = paths // CH
    local = (trade_cpty % CP).astype(BF)
    terms = jnp.concatenate(
        [jnp.stack([notional, strike, curvature, local]), jnp.zeros((ROWS - F - 4, count), BF)], axis=0)
    vmem = pl.BlockSpec(memory_space=pltpu.VMEM)
    dma = pltpu.SemaphoreType.DMA
    exposure, moment = pl.pallas_call(
        kernel,
        out_shape=(jax.ShapeDtypeStruct((paths, CP), BF), jax.ShapeDtypeStruct((NY, CP, CP), F32)),
        in_specs=[vmem] * 4,
        out_specs=(vmem, vmem),
        scratch_shapes=[
            pltpu.VMEM((ROWS, count), BF),
            pltpu.VMEM((4, ROWS, SLOT), BF),
            pltpu.VMEM((NP, 4, ROWS, SLOT), BF),
            pltpu.VMEM((NP, CP, 4 * SLOT), BF),
            pltpu.VMEM((paths, F), BF),
            pltpu.VMEM((rows, CP), F32),
            pltpu.VMEM((CH, rows, CP), BF),
            pltpu.VMEM((CH, NY, CP, rows), BF),
            pltpu.VMEM((FAR, CH, rows, CP), BF),
            pltpu.VMEM((FAR + 1, NY * CP, CP), F32),
            pltpu.VMEM((FAR + 1, NY, CP, CP), BF),
            pltpu.VMEM((FAR + 1, NX, CP, CP), BF),
            pltpu.VMEM((FAR + 1, CP, CP), BF),
            pltpu.VMEM((FAR + 1, CP, CP), BF),
            pltpu.VMEM((2, NY, CP, CP), BF),
            pltpu.VMEM((2, NX, CP, CP), BF),
            dma((4,)), dma((4,)), dma((NP,)), dma((NP,)),
            dma((CH, 3)), dma((CH, 3)), dma((FAR, CH)), dma((FAR, CH)),
            dma((FAR + 1, NX)), dma((FAR + 1, NX)),
            dma((FAR + 1,)), dma((2, NY)), dma((FAR + 1,)), dma((2, NX)),
        ],
        compiler_params=pltpu.CompilerParams(
            collective_id=0, has_side_effects=True, vmem_limit_bytes=50 * 1024 * 1024),
    )(factors, loadings, terms, trade_cpty[None, :])
    return exposure, moment.reshape(NY * CP, CP)


def solution(mesh):
    in_specs = (P(None, "paths"), P(None, "cpty"), P("cpty"), P("cpty"), P("cpty"), P("cpty"))
    out_specs = (P("paths", "cpty"), P("paths", "cpty"))
    return jax.shard_map(
        on_device, mesh=mesh, in_specs=in_specs, out_specs=out_specs, check_vma=False
    )
```

```python
import jax
import jax.numpy as jnp
from jax import lax
from jax.experimental import pallas as pl
from jax.experimental.pallas import tpu as pltpu
from jax.sharding import PartitionSpec as P

NP, NX, NZ, NY = 8, 4, 8, 4
FAR = 4
CP = 128
ROWS = 80
SLOT = 128
F = 64
CH = 4
BF, F32 = jnp.bfloat16, jnp.float32
NT = (((1,), (1,)), ((), ()))


def remote(src, dst, ssem, rsem, p, c):
    return pltpu.make_async_remote_copy(
        src_ref=src, dst_ref=dst, send_sem=ssem, recv_sem=rsem,
        device_id={"paths": p, "cpty": c}, device_id_type=pl.DeviceIdType.MESH,
    )


def kernel(fac_ref, load_ref, term_ref, id_ref, exp_ref, mom_ref,
           desc, pack, trades, hot, ft, net, own, at, ring_in, acc, rsb, mid, rr, keep, turn, fa, fb,
           s1, r1, s2, r2, sy, ry, sz, rz, srs, rrs, sa, ra, sb, rb):
    p = lax.axis_index("paths")
    c = lax.axis_index("cpty")
    z, y = c // NY, c % NY
    paths = fac_ref.shape[1]
    rows = paths // CH
    count = id_ref.shape[1]
    first = lax.rem(p - c + 32, 8)
    targets = [first + 8 * i for i in range(4)]
    x, core = p // 2, p % 2
    sign = 1 - 2 * core
    ahead, behind = lax.rem(z - sign + NZ, NZ), lax.rem(z + sign + NZ, NZ)
    y_ahead, y_back = lax.rem(y - sign + NY, NY), lax.rem(y + sign + NY, NY)
    far_here, far_ahead = z // FAR, ahead // FAR

    barrier = pltpu.get_barrier_semaphore()

    def greet(pp, cc):
        pl.semaphore_signal(barrier, inc=1, device_id={"paths": pp, "cpty": cc},
                            device_id_type=pl.DeviceIdType.MESH)

    for k in targets:
        @pl.when(k != c)
        def _(k=k):
            greet(p, k)
    for r in range(1, NP):
        greet(lax.rem(p + r, NP), c)
    greet(p, ahead * NY + y)
    greet(p, behind * NY + y)
    for r in range(1, NY):
        greet(p, z * NY + lax.rem(y + r, NY))

    desc[0:F, :] = load_ref[...]
    desc[F:ROWS, :] = term_ref[...]
    ids = id_ref[...]
    owner = ids // CP
    block = 256
    upper = (lax.broadcasted_iota(jnp.int32, (block, block), 0)
             < lax.broadcasted_iota(jnp.int32, (block, block), 1)).astype(BF)
    eq = (lax.broadcasted_iota(jnp.int32, (NZ * NY, count), 0) == owner).astype(F32)
    base = jnp.zeros((NZ * NY, 1), F32)
    ranks = []
    for b in range(count // block):
        part = eq[:, b * block:(b + 1) * block]
        before = jnp.dot(part.astype(BF), upper, preferred_element_type=F32) + base
        base = base + jnp.sum(part, axis=1, keepdims=True)
        ranks.append(jnp.sum(part * before, axis=0, keepdims=True))
    rank = jnp.concatenate(ranks, axis=1).astype(jnp.int32)
    mine = lax.rem(owner + c, 8) == p
    code = jnp.where(mine, (owner // 8) * SLOT + rank, -1)
    total = jnp.zeros((ROWS, 4 * SLOT), F32)
    step = 512
    for b in range(count // step):
        cols = slice(b * step, (b + 1) * step)
        chosen = (lax.broadcasted_iota(jnp.int32, (4 * SLOT, step), 0) == code[:, cols]).astype(F32).astype(BF)
        total = total + lax.dot_general(desc[:, cols], chosen, NT, preferred_element_type=F32)
    for i in range(4):
        pack[i] = total[:, i * SLOT:(i + 1) * SLOT].astype(BF)
    ft[...] = jnp.transpose(fac_ref[...].astype(F32)).astype(BF)

    pl.semaphore_wait(barrier, NP - 1 + 2 + NY - 1 + 4 - (lax.rem(2 * c, 8) == p).astype(jnp.int32))

    place = c // 8
    for i, k in enumerate(targets):
        copy = remote(pack.at[i], trades.at[p, place], s1.at[i], r1.at[place], p, k)

        @pl.when(k != c)
        def _(copy=copy):
            copy.start()

        @pl.when(k == c)
        def _(i=i):
            trades[p, place] = pack[i]
    for i, k in enumerate(targets):
        arrive = remote(pack.at[i], trades.at[p, i], s1.at[i], r1.at[i], p, k)

        @pl.when(k != c)
        def _(arrive=arrive):
            arrive.wait_recv()
    sends = []

    def go(copy):
        copy.start()
        sends.append(copy)

    x_ahead, x_back, x_far = lax.rem(x - sign + NX, NX), lax.rem(x + sign + NX, NX), lax.rem(x + 2, NX)
    partner = 2 * x + 1 - core
    mates = [2 * i + core for i in (x, x_back, x_ahead, x_far)]
    others = [2 * i + 1 - core for i in (x, x_ahead, x_back, x_far)]

    def across(i):
        return remote(trades.at[mates[i]], trades.at[mates[i]], s2.at[i], r2.at[i], partner, c)

    def across_wait(i):
        remote(trades.at[others[i]], trades.at[others[i]], s2.at[i], r2.at[i], partner, c).wait_recv()

    def along(i):
        src = mates[1] if i == 3 else p
        dst = mates[1] if i == 2 else mates[2]
        return remote(trades.at[src], trades.at[src], s2.at[NX + i], r2.at[NX + i], dst, c)

    def along_wait(i):
        remote(trades.at[mates[i]], trades.at[mates[i]], s2.at[NX + i], r2.at[NX + i], partner, c).wait_recv()

    def tile_of(pp):
        t = trades[pp]
        return jnp.concatenate([t[i] for i in range(4)], axis=1)

    def price(j, pp):
        full = tile_of(pp)
        terms = full[F:ROWS, :].astype(F32)
        lin = jnp.dot(ft[j * rows:(j + 1) * rows, :], full[0:F, :], preferred_element_type=F32)
        value = terms[0:1, :] * (lin + terms[2:3, :] * jnp.tanh(lin - terms[1:2, :]))
        return lax.dot_general(value.astype(BF), hot[pp], NT, preferred_element_type=F32)

    def ring(s, j):
        src = own.at[j] if s == 0 else ring_in.at[s - 1, j]
        slot = j if s < FAR - 1 else j // 2
        return remote(src, ring_in.at[s, slot], sz.at[s, slot], rz.at[s, slot], p, ahead * NY + y)

    def side(j, way):
        origin = y if way < 2 else y_back
        target = y_back if way == 1 else y_ahead
        return remote(at.at[j, origin], at.at[j, origin], sy.at[j, way], ry.at[j, way], p, z * NY + target)

    def side_wait(j, way):
        origin = (y_back, y_ahead, lax.rem(y + 2, NY))[way]
        remote(at.at[j, origin], at.at[j, origin], sy.at[j, way], ry.at[j, way], p, z * NY + y_back).wait_recv()

    def add(d, j, value, start):
        if start:
            acc[d] = value
        else:
            acc[d] += value

    def left(j):
        return at[j].reshape(NY * CP, rows)

    def dots(d, j):
        right = own[j] if d == 0 else ring_in[d - 1, j]
        add(d, j, jnp.dot(left(j), right, preferred_element_type=F32), j == 0)

    def cell(d):
        return lax.rem(z + sign * d + NZ, NZ)

    near_x, wide_x = x + 1 - 2 * (x % 2), NX - 1 - x
    first_x = near_x + core * (wide_x - near_x)
    second_x = wide_x + core * (near_x - wide_x)
    passed = 6 - x - first_x - second_x

    def tile(d, i):
        return acc[d, pl.ds(pl.multiple_of(i * CP, CP), CP), :]

    def reduce(d, i):
        src, to = ((rsb.at[d, first_x], first_x), (rsb.at[d, passed], first_x), (mid.at[d], second_x))[i]
        return remote(src, rr.at[d, i], srs.at[d, i], rrs.at[d, i], 2 * to + core, c)

    def ship(d):
        rsb[d] = acc[d].reshape(NY, CP, CP).astype(BF)
        go(reduce(d, 1))
        go(reduce(d, 0))

    def pass_on(d):
        reduce(d, 1).wait_recv()
        mid[d] = (tile(d, second_x) + rr[d, 1].astype(F32)).astype(BF)
        go(reduce(d, 2))

    def turned(d):
        return remote(turn.at[d], fa.at[core, y], sa.at[d], ra.at[core, y], cell(d), z * NY + x)

    def turned_home(d):
        return (cell(d) == p) & (x == y)

    def direct(d):
        return remote(keep.at[d], fb.at[core, x], sb.at[d], rb.at[core, x], z, cell(d) * NY + y)

    def collect(d):
        reduce(d, 0).wait_recv()
        reduce(d, 2).wait_recv()
        whole = tile(d, x) + rr[d, 0].astype(F32) + rr[d, 2].astype(F32)
        whole = whole * (1.0 / (paths * NP))
        if d > 0:
            keep[d] = whole.astype(BF)
            go(direct(d))
        turn[d] = jnp.transpose(whole).astype(BF)

        @pl.when(jnp.logical_not(turned_home(d)))
        def _():
            turned(d).start()

        @pl.when(turned_home(d))
        def _():
            fa[core, y] = turn[d]

    for t in range(CH + FAR + 1):
        if t < CH:
            j = t
            net[...] = jnp.zeros_like(net)

            def take(pp):
                t4 = trades[pp]
                label = jnp.concatenate([t4[i][F:ROWS, :] for i in range(4)], axis=1).astype(F32)[3:4, :]
                hot[pp] = (lax.broadcasted_iota(jnp.int32, (CP, 4 * SLOT), 0).astype(F32) == label).astype(F32).astype(BF)
                net[...] += price(0, pp)

            if j == 0:
                go(along(1))
                go(along(2))
                go(across(0))
                take(p)
                across_wait(0)
                take(others[0])
                along_wait(1)
                go(along(3))
                go(across(1))
                along_wait(2)
                go(across(2))
                take(mates[1])
                take(mates[2])
                across_wait(1)
                take(others[1])
                across_wait(2)
                take(others[2])
                along_wait(3)
                go(across(3))
                take(mates[3])
                across_wait(3)
                take(others[3])
            else:
                def body(r, _):
                    net[...] += price(j, r)
                    return 0

                lax.fori_loop(0, NP, body, 0, unroll=NP)
            block_f = jnp.maximum(net[...], 0.0)
            block_b = block_f.astype(BF)
            own[j] = block_b
            exp_ref[j * rows:(j + 1) * rows, :] = block_b
            at[j, y] = jnp.transpose(block_f).astype(BF)
            go(ring(0, j))
            go(side(j, 0))
            go(side(j, 1))
        j = t - 2
        if 0 <= j < CH - 1:
            side_wait(j, 0)
            go(side(j, 2))
            side_wait(j, 1)
        for s in range(1, FAR):
            j = t - 1 - s
            if 0 <= j < CH:
                ring(s - 1, j).wait_recv()
                if s < FAR - 1:
                    go(ring(s, j))
                else:
                    copy = ring(s, j)

                    @pl.when(far_ahead == j % 2)
                    def _(copy=copy):
                        copy.start()
        if t == CH:
            side_wait(CH - 1, 0)
            go(side(CH - 1, 2))
            side_wait(CH - 1, 1)
        j = t - 3
        if 0 <= j < CH - 1:
            side_wait(j, 2)
            for d in (0, 1, 2):
                dots(d, j)
        j = t - 4
        if 0 <= j < CH:
            dots(3, j)
        j = t - 1 - FAR
        if 0 <= j < CH:
            @pl.when(far_here == j % 2)
            def _(j=j):
                ring(FAR - 1, j).wait_recv()
                add(FAR, j, jnp.dot(left(j), ring_in[FAR - 1, j // 2], preferred_element_type=F32), j < 2)
        if t == CH + 1:
            side_wait(CH - 1, 2)
            for d in (0, 1):
                dots(d, CH - 1)
                ship(d)
        if t == CH + 2:
            dots(2, CH - 1)
            ship(2)
        if t == CH + 3:
            ship(3)
            pass_on(0)
            pass_on(1)
    ship(FAR)
    collect(0)
    pass_on(2)
    collect(1)
    pass_on(3)
    collect(2)
    pass_on(FAR)
    collect(3)
    collect(FAR)

    delta = lax.rem(p - z + NZ, NZ)
    mom_ref[...] = jnp.zeros_like(mom_ref)
    for k in range(2):
        near = (delta <= FAR) if k == 0 else ((delta >= FAR) | (delta == 0))
        away = ((delta >= FAR) if k == 0 else ((delta <= FAR) & (delta > 0)))
        for i in range(NY):
            @pl.when(near & jnp.logical_not((core == k) & (i == y) & (x == y)))
            def _(k=k, i=i):
                remote(turn.at[0], fa.at[k, i], sa.at[0], ra.at[k, i], 2 * y + k, z * NY + i).wait_recv()

            @pl.when(near)
            def _(k=k, i=i):
                mom_ref[i] += fa[k, i].astype(F32)

            @pl.when(away)
            def _(k=k, i=i):
                remote(turn.at[0], fb.at[k, i], sb.at[0], rb.at[k, i], 2 * i + k, p * NY + y).wait_recv()
                mom_ref[i] += fb[k, i].astype(F32)

    for i, k in enumerate(targets):
        copy = remote(pack.at[i], trades.at[p, place], s1.at[i], r1.at[place], p, k)

        @pl.when(k != c)
        def _(copy=copy):
            copy.wait_send()
    for copy in sends:
        copy.wait_send()
    for j in range(CH):
        copy = ring(FAR - 1, j)

        @pl.when(far_ahead == j % 2)
        def _(copy=copy):
            copy.wait_send()
    for d in range(FAR + 1):
        @pl.when(jnp.logical_not(turned_home(d)))
        def _(d=d):
            turned(d).wait_send()


def on_device(factors, loadings, notional, strike, curvature, trade_cpty):
    count, paths = loadings.shape[1], factors.shape[1]
    rows = paths // CH
    local = (trade_cpty % CP).astype(BF)
    terms = jnp.concatenate(
        [jnp.stack([notional, strike, curvature, local]), jnp.zeros((ROWS - F - 4, count), BF)], axis=0)
    vmem = pl.BlockSpec(memory_space=pltpu.VMEM)
    dma = pltpu.SemaphoreType.DMA
    exposure, moment = pl.pallas_call(
        kernel,
        out_shape=(jax.ShapeDtypeStruct((paths, CP), BF), jax.ShapeDtypeStruct((NY, CP, CP), F32)),
        in_specs=[vmem] * 4,
        out_specs=(vmem, vmem),
        scratch_shapes=[
            pltpu.VMEM((ROWS, count), BF),
            pltpu.VMEM((4, ROWS, SLOT), BF),
            pltpu.VMEM((NP, 4, ROWS, SLOT), BF),
            pltpu.VMEM((NP, CP, 4 * SLOT), BF),
            pltpu.VMEM((paths, F), BF),
            pltpu.VMEM((rows, CP), F32),
            pltpu.VMEM((CH, rows, CP), BF),
            pltpu.VMEM((CH, NY, CP, rows), BF),
            pltpu.VMEM((FAR, CH, rows, CP), BF),
            pltpu.VMEM((FAR + 1, NY * CP, CP), F32),
            pltpu.VMEM((FAR + 1, NY, CP, CP), BF),
            pltpu.VMEM((FAR + 1, CP, CP), BF),
            pltpu.VMEM((FAR + 1, 3, CP, CP), BF),
            pltpu.VMEM((FAR + 1, CP, CP), BF),
            pltpu.VMEM((FAR + 1, CP, CP), BF),
            pltpu.VMEM((2, NY, CP, CP), BF),
            pltpu.VMEM((2, NX, CP, CP), BF),
            dma((4,)), dma((4,)), dma((NP,)), dma((NP,)),
            dma((CH, 3)), dma((CH, 3)), dma((FAR, CH)), dma((FAR, CH)),
            dma((FAR + 1, 3)), dma((FAR + 1, 3)),
            dma((FAR + 1,)), dma((2, NY)), dma((FAR + 1,)), dma((2, NX)),
        ],
        compiler_params=pltpu.CompilerParams(
            collective_id=0, has_side_effects=True, vmem_limit_bytes=50 * 1024 * 1024),
    )(factors, loadings, terms, trade_cpty[None, :])
    return exposure, moment.reshape(NY * CP, CP)


def solution(mesh):
    in_specs = (P(None, "paths"), P(None, "cpty"), P("cpty"), P("cpty"), P("cpty"), P("cpty"))
    out_specs = (P("paths", "cpty"), P("paths", "cpty"))
    return jax.shard_map(
        on_device, mesh=mesh, in_specs=in_specs, out_specs=out_specs, check_vma=False
    )
```

```python
import jax
import jax.numpy as jnp
from jax import lax
from jax.experimental import pallas as pl
from jax.experimental.pallas import tpu as pltpu
from jax.sharding import PartitionSpec as P

NP, NX, NZ, NY = 8, 4, 8, 4
FAR = 4
CP = 128
ROWS = 80
SLOT = 128
F = 64
SIZES = (512, 512, 384, 128)
STARTS = (0, 512, 1024, 1408)
CH = len(SIZES)
FAR_SIDE = (0, 1, 1, 0)
BF, F32 = jnp.bfloat16, jnp.float32
NT = (((1,), (1,)), ((), ()))


def remote(src, dst, ssem, rsem, p, c):
    return pltpu.make_async_remote_copy(
        src_ref=src, dst_ref=dst, send_sem=ssem, recv_sem=rsem,
        device_id={"paths": p, "cpty": c}, device_id_type=pl.DeviceIdType.MESH,
    )


def kernel(fac_hbm, load_hbm, not_hbm, str_hbm, cur_hbm, id_hbm, exp_ref, mom_ref,
           fac_ref, term_in, id_ref, desc, pack, trades, hot, ft, net, own, at0, at1, at2, at3,
           ring_in, acc, rsb, mid, rr, keep, turn, fa, fb, sin,
           s1, r1, s2, r2, sy, ry, sz, rz, srs, rrs, sa, ra, sb, rb):
    p = lax.axis_index("paths")
    c = lax.axis_index("cpty")
    z, y = c // NY, c % NY
    at = (at0, at1, at2, at3)
    paths = fac_ref.shape[1]
    count = id_ref.shape[1]
    first = lax.rem(p - c + 32, 8)
    targets = [first + 8 * i for i in range(4)]
    x, core = p // 2, p % 2
    sign = 1 - 2 * core
    ahead, behind = lax.rem(z - sign + NZ, NZ), lax.rem(z + sign + NZ, NZ)
    y_ahead, y_back = lax.rem(y - sign + NY, NY), lax.rem(y + sign + NY, NY)
    far_here, far_ahead = z // FAR, ahead // FAR

    barrier = pltpu.get_barrier_semaphore()

    def greet(pp, cc):
        pl.semaphore_signal(barrier, inc=1, device_id={"paths": pp, "cpty": cc},
                            device_id_type=pl.DeviceIdType.MESH)

    for k in targets:
        @pl.when(k != c)
        def _(k=k):
            greet(p, k)
    for r in range(1, NP):
        greet(lax.rem(p + r, NP), c)
    greet(p, ahead * NY + y)
    greet(p, behind * NY + y)
    for r in range(1, NY):
        greet(p, z * NY + lax.rem(y + r, NY))

    loads = [
        pltpu.make_async_copy(src, dst, sin.at[i])
        for i, (src, dst) in enumerate((
            (id_hbm, id_ref), (not_hbm, term_in.at[0]), (str_hbm, term_in.at[1]),
            (cur_hbm, term_in.at[2]), (load_hbm, desc.at[0:F, :]), (fac_hbm, fac_ref)))
    ]
    for copy in loads:
        copy.start()
    loads[0].wait()

    ids = id_ref[...]
    owner = ids // CP
    block = 256
    upper = (lax.broadcasted_iota(jnp.int32, (block, block), 0)
             < lax.broadcasted_iota(jnp.int32, (block, block), 1)).astype(BF)
    eq = (lax.broadcasted_iota(jnp.int32, (NZ * NY, count), 0) == owner).astype(F32)
    base = jnp.zeros((NZ * NY, 1), F32)
    ranks = []
    for b in range(count // block):
        part = eq[:, b * block:(b + 1) * block]
        before = jnp.dot(part.astype(BF), upper, preferred_element_type=F32) + base
        base = base + jnp.sum(part, axis=1, keepdims=True)
        ranks.append(jnp.sum(part * before, axis=0, keepdims=True))
    rank = jnp.concatenate(ranks, axis=1).astype(jnp.int32)
    mine = lax.rem(owner + c, 8) == p
    code = jnp.where(mine, (owner // 8) * SLOT + rank, -1)
    for copy in loads[1:5]:
        copy.wait()
    line = lax.broadcasted_iota(jnp.int32, (ROWS - F, count), 0)
    extra = jnp.where(line == 3, (ids % CP).astype(F32), 0.0)
    for i in range(3):
        cells = term_in[i].astype(F32)
        flat = jnp.concatenate([cells[k:k + 1, :] for k in range(count // CP)], axis=1)
        extra = jnp.where(line == i, flat, extra)
    desc[F:ROWS, :] = extra.astype(BF)
    total = jnp.zeros((ROWS, 4 * SLOT), F32)
    step = 512
    for b in range(count // step):
        cols = slice(b * step, (b + 1) * step)
        chosen = (lax.broadcasted_iota(jnp.int32, (4 * SLOT, step), 0) == code[:, cols]).astype(F32).astype(BF)
        total = total + lax.dot_general(desc[:, cols], chosen, NT, preferred_element_type=F32)
    for i in range(4):
        pack[i] = total[:, i * SLOT:(i + 1) * SLOT].astype(BF)

    pl.semaphore_wait(barrier, NP - 1 + 2 + NY - 1 + 4 - (lax.rem(2 * c, 8) == p).astype(jnp.int32))

    place = c // 8
    for i, k in enumerate(targets):
        copy = remote(pack.at[i], trades.at[p, place], s1.at[i], r1.at[place], p, k)

        @pl.when(k != c)
        def _(copy=copy):
            copy.start()

        @pl.when(k == c)
        def _(i=i):
            trades[p, place] = pack[i]
    loads[5].wait()
    ft[...] = jnp.transpose(fac_ref[...].astype(F32)).astype(BF)
    for i, k in enumerate(targets):
        arrive = remote(pack.at[i], trades.at[p, i], s1.at[i], r1.at[i], p, k)

        @pl.when(k != c)
        def _(arrive=arrive):
            arrive.wait_recv()
    sends = []

    def go(copy):
        copy.start()
        sends.append(copy)

    x_ahead, x_back, x_far = lax.rem(x - sign + NX, NX), lax.rem(x + sign + NX, NX), lax.rem(x + 2, NX)
    partner = 2 * x + 1 - core
    mates = [2 * i + core for i in (x, x_back, x_ahead, x_far)]
    others = [2 * i + 1 - core for i in (x, x_ahead, x_back, x_far)]

    def across(i):
        return remote(trades.at[mates[i]], trades.at[mates[i]], s2.at[i], r2.at[i], partner, c)

    def across_wait(i):
        remote(trades.at[others[i]], trades.at[others[i]], s2.at[i], r2.at[i], partner, c).wait_recv()

    def along(i):
        src = mates[1] if i == 3 else p
        dst = mates[1] if i == 2 else mates[2]
        return remote(trades.at[src], trades.at[src], s2.at[NX + i], r2.at[NX + i], dst, c)

    def along_wait(i):
        remote(trades.at[mates[i]], trades.at[mates[i]], s2.at[NX + i], r2.at[NX + i], partner, c).wait_recv()

    def span(j):
        return slice(STARTS[j], STARTS[j] + SIZES[j])

    def cut(j):
        return pl.ds(STARTS[j], SIZES[j])

    def tile_of(pp):
        t = trades[pp]
        return jnp.concatenate([t[i] for i in range(4)], axis=1)

    def price(j, pp):
        full = tile_of(pp)
        terms = full[F:ROWS, :].astype(F32)
        lin = jnp.dot(ft[span(j), :], full[0:F, :], preferred_element_type=F32)
        value = terms[0:1, :] * (lin + terms[2:3, :] * jnp.tanh(lin - terms[1:2, :]))
        return lax.dot_general(value.astype(BF), hot[pp], NT, preferred_element_type=F32)

    def ring(s, j):
        src = own.at[cut(j)] if s == 0 else ring_in.at[s - 1, cut(j)]
        return remote(src, ring_in.at[s, cut(j)], sz.at[s, j], rz.at[s, j], p, ahead * NY + y)

    def side(j, way):
        origin = y if way < 2 else y_back
        target = y_back if way == 1 else y_ahead
        return remote(at[j].at[origin], at[j].at[origin], sy.at[j, way], ry.at[j, way], p, z * NY + target)

    def side_wait(j, way):
        origin = (y_back, y_ahead, lax.rem(y + 2, NY))[way]
        remote(at[j].at[origin], at[j].at[origin], sy.at[j, way], ry.at[j, way], p, z * NY + y_back).wait_recv()

    def add(d, j, value, start):
        if start:
            acc[d] = value
        else:
            acc[d] += value

    def left(j):
        return at[j][...].reshape(NY * CP, SIZES[j])

    def dots(d, j, start=None):
        right = own[span(j), :] if d == 0 else ring_in[d - 1, span(j), :]
        add(d, j, jnp.dot(left(j), right, preferred_element_type=F32), j == 0 if start is None else start)

    def cell(d):
        return lax.rem(z + sign * d + NZ, NZ)

    near_x, wide_x = x + 1 - 2 * (x % 2), NX - 1 - x
    first_x = near_x + core * (wide_x - near_x)
    second_x = wide_x + core * (near_x - wide_x)
    passed = 6 - x - first_x - second_x

    def tile(d, i):
        return acc[d, pl.ds(pl.multiple_of(i * CP, CP), CP), :]

    def reduce(d, i):
        if d < 3:
            src, to = ((rsb.at[d, first_x], first_x), (rsb.at[d, passed], first_x), (mid.at[d], second_x))[i]
        else:
            to = lax.rem(x + i + 1, NX)
            src = rsb.at[d, to]
        return remote(src, rr.at[d, i], srs.at[d, i], rrs.at[d, i], 2 * to + core, c)

    def ship(d):
        rsb[d] = acc[d].reshape(NY, CP, CP).astype(BF)
        for i in ((1, 0) if d < 3 else (1, 0, 2)):
            go(reduce(d, i))

    def pass_on(d):
        reduce(d, 1).wait_recv()
        mid[d] = (tile(d, second_x) + rr[d, 1].astype(F32)).astype(BF)
        go(reduce(d, 2))

    def turned(d):
        return remote(turn.at[d], fa.at[core, y], sa.at[d], ra.at[core, y], cell(d), z * NY + x)

    def turned_home(d):
        return (cell(d) == p) & (x == y)

    def direct(d):
        return remote(keep.at[d], fb.at[core, x], sb.at[d], rb.at[core, x], z, cell(d) * NY + y)

    def collect(d):
        whole = tile(d, x)
        for i in ((0, 2) if d < 3 else (0, 1, 2)):
            reduce(d, i).wait_recv()
            whole = whole + rr[d, i].astype(F32)
        whole = whole * (1.0 / (paths * NP))
        if d > 0:
            keep[d] = whole.astype(BF)
            go(direct(d))
        turn[d] = jnp.transpose(whole).astype(BF)

        @pl.when(jnp.logical_not(turned_home(d)))
        def _():
            turned(d).start()

        @pl.when(turned_home(d))
        def _():
            fa[core, y] = turn[d]

    for t in range(CH + FAR + 1):
        if t < CH:
            j = t
            here = net.at[0:SIZES[j], :]

            def take(*group):
                for pp in group:
                    t4 = trades[pp]
                    label = jnp.concatenate([t4[i][F:ROWS, :] for i in range(4)], axis=1).astype(F32)[3:4, :]
                    hot[pp] = (lax.broadcasted_iota(jnp.int32, (CP, 4 * SLOT), 0).astype(F32) == label).astype(F32).astype(BF)
                here[...] += sum(price(0, pp) for pp in group)

            if j == 0:
                go(along(1))
                go(along(2))
                go(across(0))
                here[...] = jnp.zeros_like(here)
                across_wait(0)
                take(p, others[0])
                along_wait(1)
                go(along(3))
                go(across(1))
                along_wait(2)
                go(across(2))
                take(mates[1], mates[2])
                across_wait(1)
                across_wait(2)
                take(others[1], others[2])
                along_wait(3)
                go(across(3))
                across_wait(3)
                take(mates[3], others[3])
            else:
                here[...] = jnp.zeros_like(here)

                def body(r, _):
                    here[...] += price(j, r)
                    return 0

                lax.fori_loop(0, NP, body, 0, unroll=NP)
            block_f = jnp.maximum(here[...], 0.0)
            block_b = block_f.astype(BF)
            own[span(j), :] = block_b
            exp_ref[span(j), :] = block_b
            at[j][y] = jnp.transpose(block_f).astype(BF)
            go(ring(0, j))
            go(side(j, 0))
            go(side(j, 1))
        for s in range(1, FAR):
            j = t - 1 - s
            if 0 <= j < CH:
                ring(s - 1, j).wait_recv()
                if s < FAR - 1:
                    go(ring(s, j))
                else:
                    copy = ring(s, j)

                    @pl.when(far_ahead == FAR_SIDE[j])
                    def _(copy=copy):
                        copy.start()
        for j in {2: (0,), 3: (1,), 4: (2, 3)}.get(t, ()):
            side_wait(j, 0)
            go(side(j, 2))
            side_wait(j, 1)
        j = t - 3
        if 0 <= j < CH - 1:
            side_wait(j, 2)
            for d in (0, 1, 2):
                dots(d, j)
        j = t - 4
        if 0 <= j < CH:
            dots(3, j)
        j = t - 1 - FAR
        if 0 <= j < CH:
            @pl.when(far_here == FAR_SIDE[j])
            def _(j=j):
                ring(FAR - 1, j).wait_recv()
                dots(FAR, j, j < 2)
        if t == CH + 1:
            side_wait(CH - 1, 2)
            for d in (0, 1):
                dots(d, CH - 1)
                ship(d)
        if t == CH + 2:
            dots(2, CH - 1)
            ship(2)
        if t == CH + 3:
            ship(3)
            pass_on(0)
            pass_on(1)
            pass_on(2)
    ship(FAR)
    for d in range(FAR + 1):
        collect(d)

    delta = lax.rem(p - z + NZ, NZ)
    mom_ref[...] = jnp.zeros_like(mom_ref)
    for k in range(2):
        near = (delta <= FAR) if k == 0 else ((delta >= FAR) | (delta == 0))
        away = ((delta >= FAR) if k == 0 else ((delta <= FAR) & (delta > 0)))
        for i in range(NY):
            @pl.when(near & jnp.logical_not((core == k) & (i == y) & (x == y)))
            def _(k=k, i=i):
                remote(turn.at[0], fa.at[k, i], sa.at[0], ra.at[k, i], 2 * y + k, z * NY + i).wait_recv()

            @pl.when(near)
            def _(k=k, i=i):
                mom_ref[i] += fa[k, i].astype(F32)

            @pl.when(away)
            def _(k=k, i=i):
                remote(turn.at[0], fb.at[k, i], sb.at[0], rb.at[k, i], 2 * i + k, p * NY + y).wait_recv()
                mom_ref[i] += fb[k, i].astype(F32)

    for i, k in enumerate(targets):
        copy = remote(pack.at[i], trades.at[p, place], s1.at[i], r1.at[place], p, k)

        @pl.when(k != c)
        def _(copy=copy):
            copy.wait_send()
    for copy in sends:
        copy.wait_send()
    for j in range(CH):
        copy = ring(FAR - 1, j)

        @pl.when(far_ahead == FAR_SIDE[j])
        def _(copy=copy):
            copy.wait_send()
    for d in range(FAR + 1):
        @pl.when(jnp.logical_not(turned_home(d)))
        def _(d=d):
            turned(d).wait_send()


def on_device(factors, loadings, notional, strike, curvature, trade_cpty):
    count, paths = loadings.shape[1], factors.shape[1]
    vmem = pl.BlockSpec(memory_space=pltpu.VMEM)
    dma = pltpu.SemaphoreType.DMA
    exposure, moment = pl.pallas_call(
        kernel,
        out_shape=(jax.ShapeDtypeStruct((paths, CP), BF), jax.ShapeDtypeStruct((NY, CP, CP), F32)),
        in_specs=[pl.BlockSpec(memory_space=pl.ANY)] * 6,
        out_specs=(vmem, vmem),
        scratch_shapes=[
            pltpu.VMEM((F, paths), BF),
            pltpu.VMEM((3, count // CP, CP), BF),
            pltpu.VMEM((1, count), jnp.int32),
            pltpu.VMEM((ROWS, count), BF),
            pltpu.VMEM((4, ROWS, SLOT), BF),
            pltpu.VMEM((NP, 4, ROWS, SLOT), BF),
            pltpu.VMEM((NP, CP, 4 * SLOT), BF),
            pltpu.VMEM((paths, F), BF),
            pltpu.VMEM((max(SIZES), CP), F32),
            pltpu.VMEM((paths, CP), BF),
            *[pltpu.VMEM((NY, CP, n), BF) for n in SIZES],
            pltpu.VMEM((FAR, paths, CP), BF),
            pltpu.VMEM((FAR + 1, NY * CP, CP), F32),
            pltpu.VMEM((FAR + 1, NY, CP, CP), BF),
            pltpu.VMEM((FAR + 1, CP, CP), BF),
            pltpu.VMEM((FAR + 1, 3, CP, CP), BF),
            pltpu.VMEM((FAR + 1, CP, CP), BF),
            pltpu.VMEM((FAR + 1, CP, CP), BF),
            pltpu.VMEM((2, NY, CP, CP), BF),
            pltpu.VMEM((2, NX, CP, CP), BF),
            dma((6,)), dma((4,)), dma((4,)), dma((NP,)), dma((NP,)),
            dma((CH, 3)), dma((CH, 3)), dma((FAR, CH)), dma((FAR, CH)),
            dma((FAR + 1, 3)), dma((FAR + 1, 3)),
            dma((FAR + 1,)), dma((2, NY)), dma((FAR + 1,)), dma((2, NX)),
        ],
        compiler_params=pltpu.CompilerParams(
            collective_id=0, has_side_effects=True, vmem_limit_bytes=67043328),
    )(factors, loadings, *[a.reshape(count // CP, CP) for a in (notional, strike, curvature)],
      trade_cpty[None, :])
    return exposure, moment.reshape(NY * CP, CP)


def solution(mesh):
    in_specs = (P(None, "paths"), P(None, "cpty"), P("cpty"), P("cpty"), P("cpty"), P("cpty"))
    out_specs = (P("paths", "cpty"), P("paths", "cpty"))
    return jax.shard_map(
        on_device, mesh=mesh, in_specs=in_specs, out_specs=out_specs, check_vma=False
    )
```

```python
import jax
import jax.numpy as jnp
from jax import lax
from jax.experimental import pallas as pl
from jax.experimental.pallas import tpu as pltpu
from jax.sharding import PartitionSpec as P

NP, NX, NZ, NY = 8, 4, 8, 4
FAR = 4
CP = 128
ROWS = 80
SLOT = 128
F = 64
SIZES = (640, 512, 384)
STARTS = (0, 640, 1152)
CH = len(SIZES)
FAR_SIDE = (0, 1, 1)
NQ, PER = 4, 8
BF, F32 = jnp.bfloat16, jnp.float32
NT = (((1,), (1,)), ((), ()))


def remote(src, dst, ssem, rsem, p, c):
    return pltpu.make_async_remote_copy(
        src_ref=src, dst_ref=dst, send_sem=ssem, recv_sem=rsem,
        device_id={"paths": p, "cpty": c}, device_id_type=pl.DeviceIdType.MESH,
    )


def kernel(fac_hbm, load_hbm, not_hbm, str_hbm, cur_hbm, id_hbm, exp_ref, mom_ref,
           fac_ref, term_in, id_ref, desc, pack, trades, hot, ft, net, own, at0, at1, at2,
           ring_in, acc, rsb, mid, rr, keep, turn, fa, fb, sin,
           s1, r1, s2, r2, sy, ry, sz, rz, srs, rrs, sa, ra, sb, rb):
    p = lax.axis_index("paths")
    c = lax.axis_index("cpty")
    z, y = c // NY, c % NY
    at = (at0, at1, at2)
    paths = fac_ref.shape[1]
    count = id_ref.shape[1]
    quarter = 2 * (p // 2 % 2) + p % 2
    first = lax.rem(quarter - c + NZ * NY, NQ)
    targets = [first + NQ * i for i in range(PER)]
    x, core = p // 2, p % 2
    sign = 1 - 2 * core
    ahead, behind = lax.rem(z - sign + NZ, NZ), lax.rem(z + sign + NZ, NZ)
    y_ahead, y_back = lax.rem(y - sign + NY, NY), lax.rem(y + sign + NY, NY)
    far_here, far_ahead = z // FAR, ahead // FAR

    barrier = pltpu.get_barrier_semaphore()

    def greet(pp, cc):
        pl.semaphore_signal(barrier, inc=1, device_id={"paths": pp, "cpty": cc},
                            device_id_type=pl.DeviceIdType.MESH)

    for k in targets:
        @pl.when(k != c)
        def _(k=k):
            greet(p, k)
    for r in range(1, NP):
        greet(lax.rem(p + r, NP), c)
    greet(p, ahead * NY + y)
    greet(p, behind * NY + y)
    for r in range(1, NY):
        greet(p, z * NY + lax.rem(y + r, NY))

    loads = [
        pltpu.make_async_copy(src, dst, sin.at[i])
        for i, (src, dst) in enumerate((
            (id_hbm, id_ref), (not_hbm, term_in.at[0]), (str_hbm, term_in.at[1]),
            (cur_hbm, term_in.at[2]), (load_hbm, desc.at[0:F, :]), (fac_hbm, fac_ref)))
    ]
    for copy in loads:
        copy.start()
    loads[0].wait()

    ids = id_ref[...]
    owner = ids // CP
    block = 256
    upper = (lax.broadcasted_iota(jnp.int32, (block, block), 0)
             < lax.broadcasted_iota(jnp.int32, (block, block), 1)).astype(BF)
    eq = (lax.broadcasted_iota(jnp.int32, (NZ * NY, count), 0) == owner).astype(F32)
    base = jnp.zeros((NZ * NY, 1), F32)
    ranks = []
    for b in range(count // block):
        part = eq[:, b * block:(b + 1) * block]
        before = jnp.dot(part.astype(BF), upper, preferred_element_type=F32) + base
        base = base + jnp.sum(part, axis=1, keepdims=True)
        ranks.append(jnp.sum(part * before, axis=0, keepdims=True))
    rank = jnp.concatenate(ranks, axis=1).astype(jnp.int32)
    mine = lax.rem(owner + c, NQ) == quarter
    code = jnp.where(mine, (owner // NQ) * SLOT + rank, -1)
    for copy in loads[1:5]:
        copy.wait()
    line = lax.broadcasted_iota(jnp.int32, (ROWS - F, count), 0)
    extra = jnp.where(line == 3, (ids % CP).astype(F32), 0.0)
    for i in range(3):
        cells = term_in[i].astype(F32)
        flat = jnp.concatenate([cells[k:k + 1, :] for k in range(count // CP)], axis=1)
        extra = jnp.where(line == i, flat, extra)
    desc[F:ROWS, :] = extra.astype(BF)
    total = jnp.zeros((ROWS, PER * SLOT), F32)
    step = 512
    for b in range(count // step):
        cols = slice(b * step, (b + 1) * step)
        chosen = (lax.broadcasted_iota(jnp.int32, (PER * SLOT, step), 0) == code[:, cols]).astype(F32).astype(BF)
        total = total + lax.dot_general(desc[:, cols], chosen, NT, preferred_element_type=F32)
    for i in range(PER):
        pack[i] = total[:, i * SLOT:(i + 1) * SLOT].astype(BF)

    pl.semaphore_wait(barrier, NP - 1 + 2 + NY - 1 + PER - (lax.rem(2 * c, NQ) == quarter).astype(jnp.int32))

    place = c // NQ
    for i, k in enumerate(targets):
        copy = remote(pack.at[i], trades.at[quarter, place], s1.at[i], r1.at[place], p, k)

        @pl.when(k != c)
        def _(copy=copy):
            copy.start()

        @pl.when(k == c)
        def _(i=i):
            trades[quarter, place] = pack[i]
    loads[5].wait()
    ft[...] = jnp.transpose(fac_ref[...].astype(F32)).astype(BF)
    for i, k in enumerate(targets):
        arrive = remote(pack.at[i], trades.at[quarter, i], s1.at[i], r1.at[i], p, k)

        @pl.when(k != c)
        def _(arrive=arrive):
            arrive.wait_recv()
    sends = []

    def go(copy):
        copy.start()
        sends.append(copy)

    x_ahead = lax.rem(x - sign + NX, NX)
    partner = 2 * x + 1 - core
    own_q, mate_q = quarter, quarter + 1 - 2 * core
    beside_q, last_q = lax.rem(own_q + 2, NQ), lax.rem(mate_q + 2, NQ)

    def give(i):
        part = beside_q if i == 2 else own_q
        to = 2 * x_ahead + core if i == 1 else partner
        return remote(trades.at[part], trades.at[part], s2.at[i], r2.at[i], to, c)

    def given(i):
        part = (mate_q, beside_q, last_q)[i]
        remote(trades.at[part], trades.at[part], s2.at[i], r2.at[i], partner, c).wait_recv()

    def span(j):
        return slice(STARTS[j], STARTS[j] + SIZES[j])

    def cut(j):
        return pl.ds(STARTS[j], SIZES[j])

    def tile_of(g, h):
        return jnp.concatenate([trades[g, 4 * h + i] for i in range(4)], axis=1)

    def price(j, g, h):
        full = tile_of(g, h)
        terms = full[F:ROWS, :].astype(F32)
        lin = jnp.dot(ft[span(j), :], full[0:F, :], preferred_element_type=F32)
        value = terms[0:1, :] * (lin + terms[2:3, :] * jnp.tanh(lin - terms[1:2, :]))
        return lax.dot_general(value.astype(BF), hot[2 * g + h], NT, preferred_element_type=F32)

    def ring(s, j):
        src = own.at[cut(j)] if s == 0 else ring_in.at[s - 1, cut(j)]
        return remote(src, ring_in.at[s, cut(j)], sz.at[s, j], rz.at[s, j], p, ahead * NY + y)

    def side(j, way):
        origin = y if way < 2 else y_back
        target = y_back if way == 1 else y_ahead
        return remote(at[j].at[origin], at[j].at[origin], sy.at[j, way], ry.at[j, way], p, z * NY + target)

    def side_wait(j, way):
        origin = (y_back, y_ahead, lax.rem(y + 2, NY))[way]
        remote(at[j].at[origin], at[j].at[origin], sy.at[j, way], ry.at[j, way], p, z * NY + y_back).wait_recv()

    def add(d, j, value, start):
        if start:
            acc[d] = value
        else:
            acc[d] += value

    def left(j):
        return at[j][...].reshape(NY * CP, SIZES[j])

    def dots(d, j, start=None):
        right = own[span(j), :] if d == 0 else ring_in[d - 1, span(j), :]
        add(d, j, jnp.dot(left(j), right, preferred_element_type=F32), j == 0 if start is None else start)

    def cell(d):
        return lax.rem(z + sign * d + NZ, NZ)

    near_x, wide_x = x + 1 - 2 * (x % 2), NX - 1 - x
    first_x = near_x + core * (wide_x - near_x)
    second_x = wide_x + core * (near_x - wide_x)
    passed = 6 - x - first_x - second_x

    def tile(d, i):
        return acc[d, pl.ds(pl.multiple_of(i * CP, CP), CP), :]

    def reduce(d, i):
        if d < 3:
            src, to = ((rsb.at[d, first_x], first_x), (rsb.at[d, passed], first_x), (mid.at[d], second_x))[i]
        else:
            to = lax.rem(x + i + 1, NX)
            src = rsb.at[d, to]
        return remote(src, rr.at[d, i], srs.at[d, i], rrs.at[d, i], 2 * to + core, c)

    def ship(d):
        rsb[d] = acc[d].reshape(NY, CP, CP).astype(BF)
        for i in ((1, 0) if d < 3 else (1, 0, 2)):
            go(reduce(d, i))

    def pass_on(d):
        reduce(d, 1).wait_recv()
        mid[d] = (tile(d, second_x) + rr[d, 1].astype(F32)).astype(BF)
        go(reduce(d, 2))

    def turned(d):
        return remote(turn.at[d], fa.at[core, y], sa.at[d], ra.at[core, y], cell(d), z * NY + x)

    def turned_home(d):
        return (cell(d) == p) & (x == y)

    def direct(d):
        return remote(keep.at[d], fb.at[core, x], sb.at[d], rb.at[core, x], z, cell(d) * NY + y)

    def collect(d):
        whole = tile(d, x)
        for i in ((0, 2) if d < 3 else (0, 1, 2)):
            reduce(d, i).wait_recv()
            whole = whole + rr[d, i].astype(F32)
        whole = whole * (1.0 / (paths * NP))
        if d > 0:
            keep[d] = whole.astype(BF)
            go(direct(d))
        turn[d] = jnp.transpose(whole).astype(BF)

        @pl.when(jnp.logical_not(turned_home(d)))
        def _():
            turned(d).start()

        @pl.when(turned_home(d))
        def _():
            fa[core, y] = turn[d]

    for t in range(CH + FAR):
        if t < CH:
            j = t
            here = net.at[0:SIZES[j], :]

            def take(g):
                for h in range(2):
                    label = tile_of(g, h)[F:ROWS, :].astype(F32)[3:4, :]
                    hot[2 * g + h] = (lax.broadcasted_iota(jnp.int32, (CP, 4 * SLOT), 0).astype(F32) == label).astype(F32).astype(BF)
                return price(0, g, 0) + price(0, g, 1)

            if j == 0:
                for i in range(2):
                    go(give(i))
                here[...] = take(own_q)
                given(0)
                here[...] += take(mate_q)
                given(1)
                go(give(2))
                here[...] += take(beside_q)
                given(2)
                here[...] += take(last_q)
            else:
                here[...] = jnp.zeros_like(here)
                for g in range(NQ):
                    for h in range(2):
                        here[...] += price(j, g, h)
            block_f = jnp.maximum(here[...], 0.0)
            block_b = block_f.astype(BF)
            own[span(j), :] = block_b
            exp_ref[span(j), :] = block_b
            at[j][y] = jnp.transpose(block_f).astype(BF)
            go(ring(0, j))
            go(side(j, 0))
            go(side(j, 1))
        for s in range(1, FAR):
            j = t - s
            if 0 <= j < CH:
                ring(s - 1, j).wait_recv()
                if s < FAR - 1:
                    go(ring(s, j))
                else:
                    copy = ring(s, j)

                    @pl.when(far_ahead == FAR_SIDE[j])
                    def _(copy=copy):
                        copy.start()
        for j in {2: (0,), 3: (1, 2)}.get(t, ()):
            side_wait(j, 0)
            go(side(j, 2))
            side_wait(j, 1)
        j = t - 3
        if 0 <= j < CH - 1:
            side_wait(j, 2)
            for d in (0, 1, 2, 3):
                dots(d, j)
        j = t - FAR
        if 0 <= j < CH:
            @pl.when(far_here == FAR_SIDE[j])
            def _(j=j):
                ring(FAR - 1, j).wait_recv()
                dots(FAR, j, j < 2)
        if t == CH + 1:
            side_wait(CH - 1, 2)
            for d in (0, 1, 2):
                dots(d, CH - 1)
                ship(d)
        if t == CH + 2:
            dots(3, CH - 1)
            ship(3)
            pass_on(0)
            pass_on(1)
            pass_on(2)
    ship(FAR)
    for d in range(FAR + 1):
        collect(d)

    delta = lax.rem(p - z + NZ, NZ)
    mom_ref[...] = jnp.zeros_like(mom_ref)
    for k in range(2):
        near = (delta <= FAR) if k == 0 else ((delta >= FAR) | (delta == 0))
        away = ((delta >= FAR) if k == 0 else ((delta <= FAR) & (delta > 0)))
        for i in range(NY):
            @pl.when(near & jnp.logical_not((core == k) & (i == y) & (x == y)))
            def _(k=k, i=i):
                remote(turn.at[0], fa.at[k, i], sa.at[0], ra.at[k, i], 2 * y + k, z * NY + i).wait_recv()

            @pl.when(near)
            def _(k=k, i=i):
                mom_ref[i] += fa[k, i].astype(F32)

            @pl.when(away)
            def _(k=k, i=i):
                remote(turn.at[0], fb.at[k, i], sb.at[0], rb.at[k, i], 2 * i + k, p * NY + y).wait_recv()
                mom_ref[i] += fb[k, i].astype(F32)

    for i, k in enumerate(targets):
        copy = remote(pack.at[i], trades.at[quarter, place], s1.at[i], r1.at[place], p, k)

        @pl.when(k != c)
        def _(copy=copy):
            copy.wait_send()
    for copy in sends:
        copy.wait_send()
    for j in range(CH):
        copy = ring(FAR - 1, j)

        @pl.when(far_ahead == FAR_SIDE[j])
        def _(copy=copy):
            copy.wait_send()
    for d in range(FAR + 1):
        @pl.when(jnp.logical_not(turned_home(d)))
        def _(d=d):
            turned(d).wait_send()


def on_device(factors, loadings, notional, strike, curvature, trade_cpty):
    count, paths = loadings.shape[1], factors.shape[1]
    vmem = pl.BlockSpec(memory_space=pltpu.VMEM)
    dma = pltpu.SemaphoreType.DMA
    exposure, moment = pl.pallas_call(
        kernel,
        out_shape=(jax.ShapeDtypeStruct((paths, CP), BF), jax.ShapeDtypeStruct((NY, CP, CP), F32)),
        in_specs=[pl.BlockSpec(memory_space=pl.ANY)] * 6,
        out_specs=(vmem, vmem),
        scratch_shapes=[
            pltpu.VMEM((F, paths), BF),
            pltpu.VMEM((3, count // CP, CP), BF),
            pltpu.VMEM((1, count), jnp.int32),
            pltpu.VMEM((ROWS, count), BF),
            pltpu.VMEM((PER, ROWS, SLOT), BF),
            pltpu.VMEM((NQ, PER, ROWS, SLOT), BF),
            pltpu.VMEM((NP, CP, 4 * SLOT), BF),
            pltpu.VMEM((paths, F), BF),
            pltpu.VMEM((max(SIZES), CP), F32),
            pltpu.VMEM((paths, CP), BF),
            *[pltpu.VMEM((NY, CP, n), BF) for n in SIZES],
            pltpu.VMEM((FAR, paths, CP), BF),
            pltpu.VMEM((FAR + 1, NY * CP, CP), F32),
            pltpu.VMEM((FAR + 1, NY, CP, CP), BF),
            pltpu.VMEM((FAR + 1, CP, CP), BF),
            pltpu.VMEM((FAR + 1, 3, CP, CP), BF),
            pltpu.VMEM((FAR + 1, CP, CP), BF),
            pltpu.VMEM((FAR + 1, CP, CP), BF),
            pltpu.VMEM((2, NY, CP, CP), BF),
            pltpu.VMEM((2, NX, CP, CP), BF),
            dma((6,)), dma((PER,)), dma((PER,)), dma((3,)), dma((3,)),
            dma((CH, 3)), dma((CH, 3)), dma((FAR, CH)), dma((FAR, CH)),
            dma((FAR + 1, 3)), dma((FAR + 1, 3)),
            dma((FAR + 1,)), dma((2, NY)), dma((FAR + 1,)), dma((2, NX)),
        ],
        compiler_params=pltpu.CompilerParams(
            collective_id=0, has_side_effects=True, vmem_limit_bytes=67043328),
    )(factors, loadings, *[a.reshape(count // CP, CP) for a in (notional, strike, curvature)],
      trade_cpty[None, :])
    return exposure, moment.reshape(NY * CP, CP)


def solution(mesh):
    in_specs = (P(None, "paths"), P(None, "cpty"), P("cpty"), P("cpty"), P("cpty"), P("cpty"))
    out_specs = (P("paths", "cpty"), P("paths", "cpty"))
    return jax.shard_map(
        on_device, mesh=mesh, in_specs=in_specs, out_specs=out_specs, check_vma=False
    )
```

```python
import jax
import jax.numpy as jnp
from jax import lax
from jax.experimental import pallas as pl
from jax.experimental.pallas import tpu as pltpu
from jax.sharding import PartitionSpec as P

NP, NX, NZ, NY = 8, 4, 8, 4
FAR = 4
CP = 128
ROWS = 80
SLOT = 128
F = 64
SIZES = (640, 512, 384)
STARTS = (0, 640, 1152)
CH = len(SIZES)
FAR_SIDE = (0, 1, 1)
NQ, PER = 4, 8
BF, F32 = jnp.bfloat16, jnp.float32
NT = (((1,), (1,)), ((), ()))


def remote(src, dst, ssem, rsem, p, c):
    return pltpu.make_async_remote_copy(
        src_ref=src, dst_ref=dst, send_sem=ssem, recv_sem=rsem,
        device_id={"paths": p, "cpty": c}, device_id_type=pl.DeviceIdType.MESH,
    )


def kernel(fac_hbm, load_hbm, not_hbm, str_hbm, cur_hbm, id_hbm, exp_ref, mom_ref,
           fac_ref, term_in, id_ref, desc, pack, trades, hot, ft, net, own, at0, at1, at2,
           ring_in, acc, rsb, mid, rr, keep, turn, fa, fb, sin,
           s1, r1, s2, r2, sy, ry, sz, rz, srs, rrs, sa, ra, sb, rb):
    p = lax.axis_index("paths")
    c = lax.axis_index("cpty")
    z, y = c // NY, c % NY
    at = (at0, at1, at2)
    paths = fac_ref.shape[1]
    count = id_ref.shape[1]
    quarter = 2 * (p // 2 % 2) + p % 2
    first = lax.rem(quarter - c + NZ * NY, NQ)
    targets = [first + NQ * i for i in range(PER)]
    x, core = p // 2, p % 2
    sign = 1 - 2 * core
    ahead, behind = lax.rem(z - sign + NZ, NZ), lax.rem(z + sign + NZ, NZ)
    y_ahead, y_back = lax.rem(y - sign + NY, NY), lax.rem(y + sign + NY, NY)
    far_here, far_ahead = z // FAR, ahead // FAR

    barrier = pltpu.get_barrier_semaphore()

    def greet(pp, cc):
        pl.semaphore_signal(barrier, inc=1, device_id={"paths": pp, "cpty": cc},
                            device_id_type=pl.DeviceIdType.MESH)

    for k in targets:
        @pl.when(k != c)
        def _(k=k):
            greet(p, k)
    for r in range(1, NP):
        greet(lax.rem(p + r, NP), c)
    greet(p, ahead * NY + y)
    greet(p, behind * NY + y)
    for r in range(1, NY):
        greet(p, z * NY + lax.rem(y + r, NY))

    loads = [
        pltpu.make_async_copy(src, dst, sin.at[i])
        for i, (src, dst) in enumerate((
            (id_hbm, id_ref), (not_hbm, term_in.at[0]), (str_hbm, term_in.at[1]),
            (cur_hbm, term_in.at[2]), (load_hbm, desc.at[0:F, :]), (fac_hbm, fac_ref)))
    ]
    for copy in loads:
        copy.start()
    loads[0].wait()

    ids = id_ref[...]
    owner = ids // CP
    block = 256
    upper = (lax.broadcasted_iota(jnp.int32, (block, block), 0)
             < lax.broadcasted_iota(jnp.int32, (block, block), 1)).astype(BF)
    eq = (lax.broadcasted_iota(jnp.int32, (NZ * NY, count), 0) == owner).astype(F32)
    base = jnp.zeros((NZ * NY, 1), F32)
    ranks = []
    for b in range(count // block):
        part = eq[:, b * block:(b + 1) * block]
        before = jnp.dot(part.astype(BF), upper, preferred_element_type=F32) + base
        base = base + jnp.sum(part, axis=1, keepdims=True)
        ranks.append(jnp.sum(part * before, axis=0, keepdims=True))
    rank = jnp.concatenate(ranks, axis=1).astype(jnp.int32)
    mine = lax.rem(owner + c, NQ) == quarter
    code = jnp.where(mine, (owner // NQ) * SLOT + rank, -1)
    for copy in loads[1:5]:
        copy.wait()
    line = lax.broadcasted_iota(jnp.int32, (ROWS - F, count), 0)
    extra = jnp.where(line == 3, (ids % CP).astype(F32), 0.0)
    for i in range(3):
        cells = term_in[i].astype(F32)
        flat = jnp.concatenate([cells[k:k + 1, :] for k in range(count // CP)], axis=1)
        extra = jnp.where(line == i, flat, extra)
    desc[F:ROWS, :] = extra.astype(BF)
    total = jnp.zeros((ROWS, PER * SLOT), F32)
    step = 512
    for b in range(count // step):
        cols = slice(b * step, (b + 1) * step)
        chosen = (lax.broadcasted_iota(jnp.int32, (PER * SLOT, step), 0) == code[:, cols]).astype(F32).astype(BF)
        total = total + lax.dot_general(desc[:, cols], chosen, NT, preferred_element_type=F32)
    for i in range(PER):
        pack[i] = total[:, i * SLOT:(i + 1) * SLOT].astype(BF)

    pl.semaphore_wait(barrier, NP - 1 + 2 + NY - 1 + PER - (lax.rem(2 * c, NQ) == quarter).astype(jnp.int32))

    place = c // NQ
    for i, k in enumerate(targets):
        copy = remote(pack.at[i], trades.at[quarter, place], s1.at[i], r1.at[place], p, k)

        @pl.when(k != c)
        def _(copy=copy):
            copy.start()

        @pl.when(k == c)
        def _(i=i):
            trades[quarter, place] = pack[i]
    loads[5].wait()
    ft[...] = jnp.transpose(fac_ref[...].astype(F32)).astype(BF)
    for i, k in enumerate(targets):
        arrive = remote(pack.at[i], trades.at[quarter, i], s1.at[i], r1.at[i], p, k)

        @pl.when(k != c)
        def _(arrive=arrive):
            arrive.wait_recv()
    sends = []

    def go(copy):
        copy.start()
        sends.append(copy)

    x_ahead = lax.rem(x - sign + NX, NX)
    partner = 2 * x + 1 - core
    own_q, mate_q = quarter, quarter + 1 - 2 * core
    beside_q, last_q = lax.rem(own_q + 2, NQ), lax.rem(mate_q + 2, NQ)

    def give(i):
        part = beside_q if i == 2 else own_q
        to = 2 * x_ahead + core if i == 1 else partner
        return remote(trades.at[part], trades.at[part], s2.at[i], r2.at[i], to, c)

    def given(i):
        part = (mate_q, beside_q, last_q)[i]
        remote(trades.at[part], trades.at[part], s2.at[i], r2.at[i], partner, c).wait_recv()

    def span(j):
        return slice(STARTS[j], STARTS[j] + SIZES[j])

    def cut(j):
        return pl.ds(STARTS[j], SIZES[j])

    def tile_of(g, h):
        return jnp.concatenate([trades[g, 4 * h + i] for i in range(4)], axis=1)

    def price(j, g, h):
        full = tile_of(g, h)
        terms = full[F:ROWS, :].astype(F32)
        lin = jnp.dot(ft[span(j), :], full[0:F, :], preferred_element_type=F32)
        value = terms[0:1, :] * (lin + terms[2:3, :] * jnp.tanh(lin - terms[1:2, :]))
        return lax.dot_general(value.astype(BF), hot[2 * g + h], NT, preferred_element_type=F32)

    def ring(s, j):
        src = own.at[cut(j)] if s == 0 else ring_in.at[s - 1, cut(j)]
        return remote(src, ring_in.at[s, cut(j)], sz.at[s, j], rz.at[s, j], p, ahead * NY + y)

    def side(j, way):
        origin = y if way < 2 else y_back
        target = y_back if way == 1 else y_ahead
        return remote(at[j].at[origin], at[j].at[origin], sy.at[j, way], ry.at[j, way], p, z * NY + target)

    def side_wait(j, way):
        origin = (y_back, y_ahead, lax.rem(y + 2, NY))[way]
        remote(at[j].at[origin], at[j].at[origin], sy.at[j, way], ry.at[j, way], p, z * NY + y_back).wait_recv()

    def add(d, j, value, start):
        if start:
            acc[d] = value
        else:
            acc[d] += value

    def left(j):
        return at[j][...].reshape(NY * CP, SIZES[j])

    def dots(d, j, start=None):
        right = own[span(j), :] if d == 0 else ring_in[d - 1, span(j), :]
        add(d, j, jnp.dot(left(j), right, preferred_element_type=F32), j == 0 if start is None else start)

    def cell(d):
        return lax.rem(z + sign * d + NZ, NZ)

    near_x, wide_x = x + 1 - 2 * (x % 2), NX - 1 - x
    first_x = near_x + core * (wide_x - near_x)
    second_x = wide_x + core * (near_x - wide_x)
    passed = 6 - x - first_x - second_x

    def tile(d, i):
        return acc[d, pl.ds(pl.multiple_of(i * CP, CP), CP), :]

    def reduce(d, i):
        if d < 3:
            src, to = ((rsb.at[d, first_x], first_x), (rsb.at[d, passed], first_x), (mid.at[d], second_x))[i]
        else:
            to = lax.rem(x + i + 1, NX)
            src = rsb.at[d, to]
        return remote(src, rr.at[d, i], srs.at[d, i], rrs.at[d, i], 2 * to + core, c)

    def ship(d):
        rsb[d] = acc[d].reshape(NY, CP, CP).astype(BF)
        for i in ((1, 0) if d < 3 else (1, 0, 2)):
            go(reduce(d, i))

    def pass_on(d):
        reduce(d, 1).wait_recv()
        mid[d] = (tile(d, second_x) + rr[d, 1].astype(F32)).astype(BF)
        go(reduce(d, 2))

    def turned(d):
        return remote(turn.at[d], fa.at[core, y], sa.at[d], ra.at[core, y], cell(d), z * NY + x)

    def turned_home(d):
        return (cell(d) == p) & (x == y)

    def direct(d):
        return remote(keep.at[d], fb.at[core, x], sb.at[d], rb.at[core, x], z, cell(d) * NY + y)

    def collect(d):
        whole = tile(d, x)
        for i in ((0, 2) if d < 3 else (0, 1, 2)):
            reduce(d, i).wait_recv()
            whole = whole + rr[d, i].astype(F32)
        whole = whole * (1.0 / (paths * NP))
        if d > 0:
            keep[d] = whole.astype(BF)
            go(direct(d))
        turn[d] = jnp.transpose(whole).astype(BF)

        @pl.when(jnp.logical_not(turned_home(d)))
        def _():
            turned(d).start()

        @pl.when(turned_home(d))
        def _():
            fa[core, y] = turn[d]

    def relay(s, j):
        ring(s - 1, j).wait_recv()
        if s < FAR - 1:
            go(ring(s, j))
        else:
            copy = ring(s, j)

            @pl.when(far_ahead == FAR_SIDE[j])
            def _():
                copy.start()

    def side_relay(j):
        side_wait(j, 0)
        go(side(j, 2))
        side_wait(j, 1)

    def far(j):
        @pl.when(far_here == FAR_SIDE[j])
        def _():
            ring(FAR - 1, j).wait_recv()
            dots(FAR, j, j < 2)

    for j in range(CH):
        here = net.at[0:SIZES[j], :]

        def take(g):
            for h in range(2):
                label = tile_of(g, h)[F:ROWS, :].astype(F32)[3:4, :]
                hot[2 * g + h] = (lax.broadcasted_iota(jnp.int32, (CP, 4 * SLOT), 0).astype(F32) == label).astype(F32).astype(BF)
            return price(0, g, 0) + price(0, g, 1)

        if j == 0:
            for i in range(2):
                go(give(i))
            here[...] = take(own_q)
            given(0)
            here[...] += take(mate_q)
            given(1)
            go(give(2))
            here[...] += take(beside_q)
            given(2)
            here[...] += take(last_q)
        else:
            here[...] = jnp.zeros_like(here)
            for g in range(NQ):
                for h in range(2):
                    here[...] += price(j, g, h)
        block_f = jnp.maximum(here[...], 0.0)
        block_b = block_f.astype(BF)
        own[span(j), :] = block_b
        exp_ref[span(j), :] = block_b
        at[j][y] = jnp.transpose(block_f).astype(BF)
        go(ring(0, j))
        go(side(j, 0))
        go(side(j, 1))
        if j == 1:
            relay(1, 0)
    relay(1, 1)
    side_relay(0)
    relay(2, 0)
    side_relay(1)
    relay(1, 2)
    relay(2, 1)
    side_relay(2)
    side_wait(0, 2)
    for d in (0, 1, 2):
        dots(d, 0)
    relay(3, 0)
    dots(3, 0)
    relay(2, 2)
    side_wait(1, 2)
    for d in (0, 1, 2):
        dots(d, 1)
    relay(3, 1)
    dots(3, 1)
    side_wait(2, 2)
    for d in (0, 1, 2):
        dots(d, 2)
        ship(d)
    relay(3, 2)
    dots(3, 2)
    ship(3)
    far(0)
    far(1)
    pass_on(0)
    pass_on(1)
    far(2)
    ship(FAR)
    pass_on(2)
    for d in range(FAR + 1):
        collect(d)

    delta = lax.rem(p - z + NZ, NZ)
    mom_ref[...] = jnp.zeros_like(mom_ref)
    for k in range(2):
        near = (delta <= FAR) if k == 0 else ((delta >= FAR) | (delta == 0))
        away = ((delta >= FAR) if k == 0 else ((delta <= FAR) & (delta > 0)))
        for i in range(NY):
            @pl.when(near & jnp.logical_not((core == k) & (i == y) & (x == y)))
            def _(k=k, i=i):
                remote(turn.at[0], fa.at[k, i], sa.at[0], ra.at[k, i], 2 * y + k, z * NY + i).wait_recv()

            @pl.when(near)
            def _(k=k, i=i):
                mom_ref[i] += fa[k, i].astype(F32)

            @pl.when(away)
            def _(k=k, i=i):
                remote(turn.at[0], fb.at[k, i], sb.at[0], rb.at[k, i], 2 * i + k, p * NY + y).wait_recv()
                mom_ref[i] += fb[k, i].astype(F32)

    for i, k in enumerate(targets):
        copy = remote(pack.at[i], trades.at[quarter, place], s1.at[i], r1.at[place], p, k)

        @pl.when(k != c)
        def _(copy=copy):
            copy.wait_send()
    for copy in sends:
        copy.wait_send()
    for j in range(CH):
        copy = ring(FAR - 1, j)

        @pl.when(far_ahead == FAR_SIDE[j])
        def _(copy=copy):
            copy.wait_send()
    for d in range(FAR + 1):
        @pl.when(jnp.logical_not(turned_home(d)))
        def _(d=d):
            turned(d).wait_send()


def on_device(factors, loadings, notional, strike, curvature, trade_cpty):
    count, paths = loadings.shape[1], factors.shape[1]
    vmem = pl.BlockSpec(memory_space=pltpu.VMEM)
    dma = pltpu.SemaphoreType.DMA
    exposure, moment = pl.pallas_call(
        kernel,
        out_shape=(jax.ShapeDtypeStruct((paths, CP), BF), jax.ShapeDtypeStruct((NY, CP, CP), F32)),
        in_specs=[pl.BlockSpec(memory_space=pl.ANY)] * 6,
        out_specs=(vmem, vmem),
        scratch_shapes=[
            pltpu.VMEM((F, paths), BF),
            pltpu.VMEM((3, count // CP, CP), BF),
            pltpu.VMEM((1, count), jnp.int32),
            pltpu.VMEM((ROWS, count), BF),
            pltpu.VMEM((PER, ROWS, SLOT), BF),
            pltpu.VMEM((NQ, PER, ROWS, SLOT), BF),
            pltpu.VMEM((NP, CP, 4 * SLOT), BF),
            pltpu.VMEM((paths, F), BF),
            pltpu.VMEM((max(SIZES), CP), F32),
            pltpu.VMEM((paths, CP), BF),
            *[pltpu.VMEM((NY, CP, n), BF) for n in SIZES],
            pltpu.VMEM((FAR, paths, CP), BF),
            pltpu.VMEM((FAR + 1, NY * CP, CP), F32),
            pltpu.VMEM((FAR + 1, NY, CP, CP), BF),
            pltpu.VMEM((FAR + 1, CP, CP), BF),
            pltpu.VMEM((FAR + 1, 3, CP, CP), BF),
            pltpu.VMEM((FAR + 1, CP, CP), BF),
            pltpu.VMEM((FAR + 1, CP, CP), BF),
            pltpu.VMEM((2, NY, CP, CP), BF),
            pltpu.VMEM((2, NX, CP, CP), BF),
            dma((6,)), dma((PER,)), dma((PER,)), dma((3,)), dma((3,)),
            dma((CH, 3)), dma((CH, 3)), dma((FAR, CH)), dma((FAR, CH)),
            dma((FAR + 1, 3)), dma((FAR + 1, 3)),
            dma((FAR + 1,)), dma((2, NY)), dma((FAR + 1,)), dma((2, NX)),
        ],
        compiler_params=pltpu.CompilerParams(
            collective_id=0, has_side_effects=True, vmem_limit_bytes=67043328),
    )(factors, loadings, *[a.reshape(count // CP, CP) for a in (notional, strike, curvature)],
      trade_cpty[None, :])
    return exposure, moment.reshape(NY * CP, CP)


def solution(mesh):
    in_specs = (P(None, "paths"), P(None, "cpty"), P("cpty"), P("cpty"), P("cpty"), P("cpty"))
    out_specs = (P("paths", "cpty"), P("paths", "cpty"))
    return jax.shard_map(
        on_device, mesh=mesh, in_specs=in_specs, out_specs=out_specs, check_vma=False
    )
```

```python
import jax
import jax.numpy as jnp
from jax import lax
from jax.experimental import pallas as pl
from jax.experimental.pallas import tpu as pltpu
from jax.sharding import PartitionSpec as P

NP, NX, NZ, NY = 8, 4, 8, 4
FAR = 4
CP = 128
ROWS = 80
SLOT = 128
F = 64
SIZES = (640, 512, 384)
STARTS = (0, 640, 1152)
CH = len(SIZES)
FAR_SIDE = (0, 1, 1)
NQ, PER = 4, 8
BF, F32 = jnp.bfloat16, jnp.float32
NT = (((1,), (1,)), ((), ()))


def remote(src, dst, ssem, rsem, p, c):
    return pltpu.make_async_remote_copy(
        src_ref=src, dst_ref=dst, send_sem=ssem, recv_sem=rsem,
        device_id={"paths": p, "cpty": c}, device_id_type=pl.DeviceIdType.MESH,
    )


def kernel(fac_hbm, load_hbm, not_hbm, str_hbm, cur_hbm, id_hbm, exp_ref, mom_ref,
           fac_ref, term_in, id_ref, desc, pack, trades, hot, ft, net, own, at0, at1, at2,
           ring_in, acc, rsb, mid, rr, keep, turn, fa, fb, sin,
           sout, s1, r1, s2, r2, sy, ry, sz, rz, srs, rrs, sa, ra, sb, rb):
    p = lax.axis_index("paths")
    c = lax.axis_index("cpty")
    z, y = c // NY, c % NY
    at = (at0, at1, at2)
    paths = fac_ref.shape[1]
    count = id_ref.shape[1]
    quarter = 2 * (p // 2 % 2) + p % 2
    first = lax.rem(quarter - c + NZ * NY, NQ)
    targets = [first + NQ * i for i in range(PER)]
    x, core = p // 2, p % 2
    sign = 1 - 2 * core
    ahead, behind = lax.rem(z - sign + NZ, NZ), lax.rem(z + sign + NZ, NZ)
    y_ahead, y_back = lax.rem(y - sign + NY, NY), lax.rem(y + sign + NY, NY)
    far_here, far_ahead = z // FAR, ahead // FAR

    barrier = pltpu.get_barrier_semaphore()

    def greet(pp, cc):
        pl.semaphore_signal(barrier, inc=1, device_id={"paths": pp, "cpty": cc},
                            device_id_type=pl.DeviceIdType.MESH)

    for k in targets:
        @pl.when(k != c)
        def _(k=k):
            greet(p, k)
    for r in range(1, NP):
        greet(lax.rem(p + r, NP), c)
    greet(p, ahead * NY + y)
    greet(p, behind * NY + y)
    for r in range(1, NY):
        greet(p, z * NY + lax.rem(y + r, NY))

    loads = [
        pltpu.make_async_copy(src, dst, sin.at[i])
        for i, (src, dst) in enumerate((
            (id_hbm, id_ref), (not_hbm, term_in.at[0]), (str_hbm, term_in.at[1]),
            (cur_hbm, term_in.at[2]), (load_hbm, desc.at[0:F, :]), (fac_hbm, fac_ref)))
    ]
    for copy in loads:
        copy.start()
    loads[0].wait()

    ids = id_ref[...]
    owner = ids // CP
    block = 256
    upper = (lax.broadcasted_iota(jnp.int32, (block, block), 0)
             < lax.broadcasted_iota(jnp.int32, (block, block), 1)).astype(BF)
    eq = (lax.broadcasted_iota(jnp.int32, (NZ * NY, count), 0) == owner).astype(F32)
    base = jnp.zeros((NZ * NY, 1), F32)
    ranks = []
    for b in range(count // block):
        part = eq[:, b * block:(b + 1) * block]
        before = jnp.dot(part.astype(BF), upper, preferred_element_type=F32) + base
        base = base + jnp.sum(part, axis=1, keepdims=True)
        ranks.append(jnp.sum(part * before, axis=0, keepdims=True))
    rank = jnp.concatenate(ranks, axis=1).astype(jnp.int32)
    mine = lax.rem(owner + c, NQ) == quarter
    code = jnp.where(mine, (owner // NQ) * SLOT + rank, -1)
    for copy in loads[1:5]:
        copy.wait()
    line = lax.broadcasted_iota(jnp.int32, (ROWS - F, count), 0)
    extra = jnp.where(line == 3, (ids % CP).astype(F32), 0.0)
    for i in range(3):
        cells = term_in[i].astype(F32)
        flat = jnp.concatenate([cells[k:k + 1, :] for k in range(count // CP)], axis=1)
        extra = jnp.where(line == i, flat, extra)
    desc[F:ROWS, :] = extra.astype(BF)
    total = jnp.zeros((ROWS, PER * SLOT), F32)
    step = 512
    for b in range(count // step):
        cols = slice(b * step, (b + 1) * step)
        chosen = (lax.broadcasted_iota(jnp.int32, (PER * SLOT, step), 0) == code[:, cols]).astype(F32).astype(BF)
        total = total + lax.dot_general(desc[:, cols], chosen, NT, preferred_element_type=F32)
    for i in range(PER):
        pack[i] = total[:, i * SLOT:(i + 1) * SLOT].astype(BF)

    pl.semaphore_wait(barrier, NP - 1 + 2 + NY - 1 + PER - (lax.rem(2 * c, NQ) == quarter).astype(jnp.int32))

    place = c // NQ
    for offset in (4, 3, 5, 2, 6, 1, 7, 0):
        i = lax.rem(z + offset, PER)
        copy = remote(pack.at[i], trades.at[quarter, place], s1.at[i], r1.at[place], p, first + NQ * i)
        if offset:
            copy.start()
        else:
            @pl.when(first != y)
            def _(copy=copy):
                copy.start()

            @pl.when(first == y)
            def _(i=i):
                trades[quarter, place] = pack[i]
    loads[5].wait()
    ft[...] = jnp.transpose(fac_ref[...].astype(F32)).astype(BF)
    for i, k in enumerate(targets):
        arrive = remote(pack.at[i], trades.at[quarter, i], s1.at[i], r1.at[i], p, k)

        @pl.when(k != c)
        def _(arrive=arrive):
            arrive.wait_recv()
    sends = []

    def go(copy):
        copy.start()
        sends.append(copy)

    x_ahead = lax.rem(x - sign + NX, NX)
    partner = 2 * x + 1 - core
    own_q, mate_q = quarter, quarter + 1 - 2 * core
    beside_q, last_q = lax.rem(own_q + 2, NQ), lax.rem(mate_q + 2, NQ)

    def give(i):
        part = beside_q if i == 2 else own_q
        to = 2 * x_ahead + core if i == 1 else partner
        return remote(trades.at[part], trades.at[part], s2.at[i], r2.at[i], to, c)

    def given(i):
        part = (mate_q, beside_q, last_q)[i]
        remote(trades.at[part], trades.at[part], s2.at[i], r2.at[i], partner, c).wait_recv()

    def span(j):
        return slice(STARTS[j], STARTS[j] + SIZES[j])

    def cut(j):
        return pl.ds(STARTS[j], SIZES[j])

    def tile_of(g, h):
        return jnp.concatenate([trades[g, 4 * h + i] for i in range(4)], axis=1)

    def price(j, g, h):
        full = tile_of(g, h)
        terms = full[F:ROWS, :].astype(F32)
        lin = jnp.dot(ft[span(j), :], full[0:F, :], preferred_element_type=F32)
        value = terms[0:1, :] * (lin + terms[2:3, :] * jnp.tanh(lin - terms[1:2, :]))
        return lax.dot_general(value.astype(BF), hot[2 * g + h], NT, preferred_element_type=F32)

    def ring(s, j):
        src = own.at[cut(j)] if s == 0 else ring_in.at[s - 1, cut(j)]
        return remote(src, ring_in.at[s, cut(j)], sz.at[s, j], rz.at[s, j], p, ahead * NY + y)

    def side(j, way):
        origin = y if way < 2 else y_back
        target = y_back if way == 1 else y_ahead
        return remote(at[j].at[origin], at[j].at[origin], sy.at[j, way], ry.at[j, way], p, z * NY + target)

    def side_wait(j, way):
        origin = (y_back, y_ahead, lax.rem(y + 2, NY))[way]
        remote(at[j].at[origin], at[j].at[origin], sy.at[j, way], ry.at[j, way], p, z * NY + y_back).wait_recv()

    def add(d, j, value, start):
        if start:
            acc[d] = value
        else:
            acc[d] += value

    def left(j):
        return at[j][...].reshape(NY * CP, SIZES[j])

    def dots(d, j, start=None):
        right = own[span(j), :] if d == 0 else ring_in[d - 1, span(j), :]
        add(d, j, jnp.dot(left(j), right, preferred_element_type=F32), j == 0 if start is None else start)

    def cell(d):
        return lax.rem(z + sign * d + NZ, NZ)

    near_x, wide_x = x + 1 - 2 * (x % 2), NX - 1 - x
    first_x = near_x + core * (wide_x - near_x)
    second_x = wide_x + core * (near_x - wide_x)
    passed = 6 - x - first_x - second_x

    def tile(d, i):
        return acc[d, pl.ds(pl.multiple_of(i * CP, CP), CP), :]

    def reduce(d, i):
        if d < 3:
            src, to = ((rsb.at[d, first_x], first_x), (rsb.at[d, passed], first_x), (mid.at[d], second_x))[i]
        else:
            to = lax.rem(x + i + 1, NX)
            src = rsb.at[d, to]
        return remote(src, rr.at[d, i], srs.at[d, i], rrs.at[d, i], 2 * to + core, c)

    def ship(d):
        rsb[d] = acc[d].reshape(NY, CP, CP).astype(BF)
        for i in ((1, 0) if d < 3 else (1, 0, 2)):
            go(reduce(d, i))

    def pass_on(d):
        reduce(d, 1).wait_recv()
        mid[d] = (tile(d, second_x) + rr[d, 1].astype(F32)).astype(BF)
        go(reduce(d, 2))

    def turned(d):
        return remote(turn.at[d], fa.at[core, y], sa.at[d], ra.at[core, y], cell(d), z * NY + x)

    def turned_home(d):
        return (cell(d) == p) & (x == y)

    def direct(d):
        return remote(keep.at[d], fb.at[core, x], sb.at[d], rb.at[core, x], z, cell(d) * NY + y)

    def collect(d):
        whole = tile(d, x)
        for i in ((0, 2) if d < 3 else (0, 1, 2)):
            reduce(d, i).wait_recv()
            whole = whole + rr[d, i].astype(F32)
        whole = whole * (1.0 / (paths * NP))
        if d > 0:
            keep[d] = whole.astype(BF)
            go(direct(d))
        turn[d] = jnp.transpose(whole).astype(BF)

        @pl.when(jnp.logical_not(turned_home(d)))
        def _():
            turned(d).start()

        @pl.when(turned_home(d))
        def _():
            fa[core, y] = turn[d]

    def out(j):
        return pltpu.make_async_copy(own.at[cut(j)], exp_ref.at[cut(j)], sout.at[j])

    def relay(s, j):
        ring(s - 1, j).wait_recv()
        if s < FAR - 1:
            go(ring(s, j))
        else:
            copy = ring(s, j)

            @pl.when(far_ahead == FAR_SIDE[j])
            def _():
                copy.start()

    def side_relay(j):
        side_wait(j, 0)
        go(side(j, 2))
        side_wait(j, 1)

    def far(j):
        @pl.when(far_here == FAR_SIDE[j])
        def _():
            ring(FAR - 1, j).wait_recv()
            dots(FAR, j, j < 2)

    for j in range(CH):
        here = net.at[0:SIZES[j], :]

        def take(g):
            for h in range(2):
                label = tile_of(g, h)[F:ROWS, :].astype(F32)[3:4, :]
                hot[2 * g + h] = (lax.broadcasted_iota(jnp.int32, (CP, 4 * SLOT), 0).astype(F32) == label).astype(F32).astype(BF)
            return price(0, g, 0) + price(0, g, 1)

        if j == 0:
            for i in range(2):
                go(give(i))
            here[...] = take(own_q)
            given(0)
            here[...] += take(mate_q)
            given(1)
            go(give(2))
            here[...] += take(beside_q)
            given(2)
            here[...] += take(last_q)
        else:
            here[...] = jnp.zeros_like(here)
            for g in range(NQ):
                for h in range(2):
                    here[...] += price(j, g, h)
        block_f = jnp.maximum(here[...], 0.0)
        block_b = block_f.astype(BF)
        own[span(j), :] = block_b
        at[j][y] = jnp.transpose(block_f).astype(BF)
        go(ring(0, j))
        out(j).start()
        go(side(j, 0))
        go(side(j, 1))
        if j == 1:
            relay(1, 0)
    relay(1, 1)
    side_relay(0)
    relay(2, 0)
    side_relay(1)
    relay(1, 2)
    relay(2, 1)
    side_relay(2)
    side_wait(0, 2)
    for d in (0, 1, 2):
        dots(d, 0)
    relay(2, 2)
    relay(3, 0)
    dots(3, 0)
    side_wait(1, 2)
    for d in (0, 1, 2):
        dots(d, 1)
    relay(3, 1)
    side_wait(2, 2)
    for d in (0, 1, 2):
        dots(d, 2)
        ship(d)
    relay(3, 2)
    for j in (1, 2):
        dots(3, j)
    ship(3)
    far(0)
    far(1)
    for d in (0, 1, 2):
        pass_on(d)
    far(2)
    ship(FAR)
    for d in range(FAR + 1):
        collect(d)

    delta = lax.rem(p - z + NZ, NZ)
    mom_ref[...] = jnp.zeros_like(mom_ref)
    for k in range(2):
        near = (delta <= FAR) if k == 0 else ((delta >= FAR) | (delta == 0))
        away = ((delta >= FAR) if k == 0 else ((delta <= FAR) & (delta > 0)))
        for i in range(NY):
            @pl.when(near & jnp.logical_not((core == k) & (i == y) & (x == y)))
            def _(k=k, i=i):
                remote(turn.at[0], fa.at[k, i], sa.at[0], ra.at[k, i], 2 * y + k, z * NY + i).wait_recv()

            @pl.when(near)
            def _(k=k, i=i):
                mom_ref[i] += fa[k, i].astype(F32)

            @pl.when(away)
            def _(k=k, i=i):
                remote(turn.at[0], fb.at[k, i], sb.at[0], rb.at[k, i], 2 * i + k, p * NY + y).wait_recv()
                mom_ref[i] += fb[k, i].astype(F32)

    for j in range(CH):
        out(j).wait()
    for i, k in enumerate(targets):
        copy = remote(pack.at[i], trades.at[quarter, place], s1.at[i], r1.at[place], p, k)

        @pl.when(k != c)
        def _(copy=copy):
            copy.wait_send()
    for copy in sends:
        copy.wait_send()
    for j in range(CH):
        copy = ring(FAR - 1, j)

        @pl.when(far_ahead == FAR_SIDE[j])
        def _(copy=copy):
            copy.wait_send()
    for d in range(FAR + 1):
        @pl.when(jnp.logical_not(turned_home(d)))
        def _(d=d):
            turned(d).wait_send()


def hand_out(exp_in, mom_in, exp_out, mom_out, exp_buf, mom_buf, sin, sout):
    steps = []
    for a, (src, buf, dst) in enumerate(((exp_in, exp_buf, exp_out), (mom_in, mom_buf, mom_out))):
        rows = src.shape[0] // 4
        for i in range(4):
            part = pl.ds(i * rows, rows)
            steps.append((
                pltpu.make_async_copy(src.at[part], buf.at[part], sin.at[a, i]),
                pltpu.make_async_copy(buf.at[part], dst.at[part], sout.at[a, i])))
    for get, _ in steps:
        get.start()
    for get, put in steps:
        get.wait()
        put.start()
    for _, put in steps:
        put.wait()


def on_device(factors, loadings, notional, strike, curvature, trade_cpty):
    count, paths = loadings.shape[1], factors.shape[1]
    vmem = pl.BlockSpec(memory_space=pltpu.VMEM)
    dma = pltpu.SemaphoreType.DMA
    exposure, moment = pl.pallas_call(
        kernel,
        out_shape=(jax.ShapeDtypeStruct((paths, CP), BF), jax.ShapeDtypeStruct((NY, CP, CP), F32)),
        in_specs=[pl.BlockSpec(memory_space=pl.ANY)] * 6,
        out_specs=(pl.BlockSpec(memory_space=pl.ANY), vmem),
        scratch_shapes=[
            pltpu.VMEM((F, paths), BF),
            pltpu.VMEM((3, count // CP, CP), BF),
            pltpu.VMEM((1, count), jnp.int32),
            pltpu.VMEM((ROWS, count), BF),
            pltpu.VMEM((PER, ROWS, SLOT), BF),
            pltpu.VMEM((NQ, PER, ROWS, SLOT), BF),
            pltpu.VMEM((NP, CP, 4 * SLOT), BF),
            pltpu.VMEM((paths, F), BF),
            pltpu.VMEM((max(SIZES), CP), F32),
            pltpu.VMEM((paths, CP), BF),
            *[pltpu.VMEM((NY, CP, n), BF) for n in SIZES],
            pltpu.VMEM((FAR, paths, CP), BF),
            pltpu.VMEM((FAR + 1, NY * CP, CP), F32),
            pltpu.VMEM((FAR + 1, NY, CP, CP), BF),
            pltpu.VMEM((FAR + 1, CP, CP), BF),
            pltpu.VMEM((FAR + 1, 3, CP, CP), BF),
            pltpu.VMEM((FAR + 1, CP, CP), BF),
            pltpu.VMEM((FAR + 1, CP, CP), BF),
            pltpu.VMEM((2, NY, CP, CP), BF),
            pltpu.VMEM((2, NX, CP, CP), BF),
            dma((6,)), dma((CH,)), dma((PER,)), dma((PER,)), dma((3,)), dma((3,)),
            dma((CH, 3)), dma((CH, 3)), dma((FAR, CH)), dma((FAR, CH)),
            dma((FAR + 1, 3)), dma((FAR + 1, 3)),
            dma((FAR + 1,)), dma((2, NY)), dma((FAR + 1,)), dma((2, NX)),
        ],
        compiler_params=pltpu.CompilerParams(
            collective_id=0, has_side_effects=True, vmem_limit_bytes=67043328),
    )(factors, loadings, *[a.reshape(count // CP, CP) for a in (notional, strike, curvature)],
      trade_cpty[None, :])
    shapes = [(exposure.shape, BF), (moment.shape, F32)]
    anywhere = pl.BlockSpec(memory_space=pl.ANY)
    exposure, moment = pl.pallas_call(
        hand_out,
        out_shape=tuple(jax.ShapeDtypeStruct(*s) for s in shapes),
        in_specs=[anywhere] * 2,
        out_specs=(anywhere,) * 2,
        scratch_shapes=[*[pltpu.VMEM(*s) for s in shapes], dma((2, 4)), dma((2, 4))],
        compiler_params=pltpu.CompilerParams(vmem_limit_bytes=67043328),
    )(exposure, moment)
    return exposure, moment.reshape(NY * CP, CP)


def solution(mesh):
    in_specs = (P(None, "paths"), P(None, "cpty"), P("cpty"), P("cpty"), P("cpty"), P("cpty"))
    out_specs = (P("paths", "cpty"), P("paths", "cpty"))
    return jax.shard_map(
        on_device, mesh=mesh, in_specs=in_specs, out_specs=out_specs, check_vma=False
    )
```

```python
import jax
import jax.numpy as jnp
from jax import lax
from jax.experimental import pallas as pl
from jax.experimental.pallas import tpu as pltpu
from jax.sharding import PartitionSpec as P

NP, NX, NZ, NY = 8, 4, 8, 4
FAR = 4
CP = 128
ROWS = 80
SLOT = 128
F = 64
SIZES = (640, 512, 384)
STARTS = (0, 640, 1152)
CH = len(SIZES)
NQ, PER = 4, 8
BF, F32 = jnp.bfloat16, jnp.float32
NT = (((1,), (1,)), ((), ()))


def remote(src, dst, ssem, rsem, p, c):
    return pltpu.make_async_remote_copy(
        src_ref=src, dst_ref=dst, send_sem=ssem, recv_sem=rsem,
        device_id={"paths": p, "cpty": c}, device_id_type=pl.DeviceIdType.MESH,
    )


def kernel(fac_hbm, load_hbm, not_hbm, str_hbm, cur_hbm, id_hbm, exp_ref, mom_ref,
           fac_ref, term_in, id_ref, desc, pack, trades, hot, ft, net, own, at0, at1, at2,
           ring_in, acc, rsb, mid, rr, keep, turn, fa, fb, sin,
           sout, s1, r1, s2, r2, sy, ry, sz, rz, srs, rrs, sa, ra, sb, rb):
    p = lax.axis_index("paths")
    c = lax.axis_index("cpty")
    z, y = c // NY, c % NY
    at = (at0, at1, at2)
    paths = fac_ref.shape[1]
    count = id_ref.shape[1]
    quarter = 2 * (p // 2 % 2) + p % 2
    first = lax.rem(quarter - c + NZ * NY, NQ)
    targets = [first + NQ * i for i in range(PER)]
    x, core = p // 2, p % 2
    sign = 1 - 2 * core
    ahead, behind = lax.rem(z - sign + NZ, NZ), lax.rem(z + sign + NZ, NZ)
    y_ahead, y_back = lax.rem(y - sign + NY, NY), lax.rem(y + sign + NY, NY)

    barrier = pltpu.get_barrier_semaphore()

    def greet(pp, cc):
        pl.semaphore_signal(barrier, inc=1, device_id={"paths": pp, "cpty": cc},
                            device_id_type=pl.DeviceIdType.MESH)

    for k in targets:
        @pl.when(k != c)
        def _(k=k):
            greet(p, k)
    for r in range(1, NP):
        greet(lax.rem(p + r, NP), c)
    greet(p, ahead * NY + y)
    greet(p, behind * NY + y)
    for r in range(1, NY):
        greet(p, z * NY + lax.rem(y + r, NY))

    loads = [
        pltpu.make_async_copy(src, dst, sin.at[i])
        for i, (src, dst) in enumerate((
            (id_hbm, id_ref), (not_hbm, term_in.at[0]), (str_hbm, term_in.at[1]),
            (cur_hbm, term_in.at[2]), (load_hbm, desc.at[0:F, :]), (fac_hbm, fac_ref)))
    ]
    for copy in loads:
        copy.start()
    loads[0].wait()

    ids = id_ref[...]
    owner = ids // CP
    block = 256
    upper = (lax.broadcasted_iota(jnp.int32, (block, block), 0)
             < lax.broadcasted_iota(jnp.int32, (block, block), 1)).astype(BF)
    eq = (lax.broadcasted_iota(jnp.int32, (NZ * NY, count), 0) == owner).astype(F32)
    base = jnp.zeros((NZ * NY, 1), F32)
    ranks = []
    for b in range(count // block):
        part = eq[:, b * block:(b + 1) * block]
        before = jnp.dot(part.astype(BF), upper, preferred_element_type=F32) + base
        base = base + jnp.sum(part, axis=1, keepdims=True)
        ranks.append(jnp.sum(part * before, axis=0, keepdims=True))
    rank = jnp.concatenate(ranks, axis=1).astype(jnp.int32)
    mine = lax.rem(owner + c, NQ) == quarter
    code = jnp.where(mine, (owner // NQ) * SLOT + rank, -1)
    for copy in loads[1:5]:
        copy.wait()
    line = lax.broadcasted_iota(jnp.int32, (ROWS - F, count), 0)
    extra = jnp.where(line == 3, (ids % CP).astype(F32), 0.0)
    for i in range(3):
        cells = term_in[i].astype(F32)
        flat = jnp.concatenate([cells[k:k + 1, :] for k in range(count // CP)], axis=1)
        extra = jnp.where(line == i, flat, extra)
    desc[F:ROWS, :] = extra.astype(BF)
    total = jnp.zeros((ROWS, PER * SLOT), F32)
    step = 512
    for b in range(count // step):
        cols = slice(b * step, (b + 1) * step)
        chosen = (lax.broadcasted_iota(jnp.int32, (PER * SLOT, step), 0) == code[:, cols]).astype(F32).astype(BF)
        total = total + lax.dot_general(desc[:, cols], chosen, NT, preferred_element_type=F32)
    for i in range(PER):
        pack[i] = total[:, i * SLOT:(i + 1) * SLOT].astype(BF)

    pl.semaphore_wait(barrier, NP - 1 + 2 + NY - 1 + PER - (lax.rem(2 * c, NQ) == quarter).astype(jnp.int32))

    place = c // NQ
    for offset in (4, 3, 5, 2, 6, 1, 7, 0):
        i = lax.rem(z + offset, PER)
        copy = remote(pack.at[i], trades.at[quarter, place], s1.at[i], r1.at[place], p, first + NQ * i)
        if offset:
            copy.start()
        else:
            @pl.when(first != y)
            def _(copy=copy):
                copy.start()

            @pl.when(first == y)
            def _(i=i):
                trades[quarter, place] = pack[i]
    loads[5].wait()
    ft[...] = jnp.transpose(fac_ref[...].astype(F32)).astype(BF)
    for i, k in enumerate(targets):
        arrive = remote(pack.at[i], trades.at[quarter, i], s1.at[i], r1.at[i], p, k)

        @pl.when(k != c)
        def _(arrive=arrive):
            arrive.wait_recv()
    sends = []

    def go(copy):
        copy.start()
        sends.append(copy)

    x_ahead = lax.rem(x - sign + NX, NX)
    partner = 2 * x + 1 - core
    own_q, mate_q = quarter, quarter + 1 - 2 * core
    beside_q, last_q = lax.rem(own_q + 2, NQ), lax.rem(mate_q + 2, NQ)

    def half(part, h):
        return trades.at[part, pl.ds(4 * h, 4)]

    def give(i, h):
        part = beside_q if i == 2 else own_q
        to = 2 * x_ahead + core if i == 1 else partner
        return remote(half(part, h), half(part, h), s2.at[i, h], r2.at[i, h], to, c)

    def given(i, h):
        part = (mate_q, beside_q, last_q)[i]
        remote(half(part, h), half(part, h), s2.at[i, h], r2.at[i, h], partner, c).wait_recv()

    def span(j):
        return slice(STARTS[j], STARTS[j] + SIZES[j])

    def cut(j):
        return pl.ds(STARTS[j], SIZES[j])

    def tile_of(g, h):
        return jnp.concatenate([trades[g, 4 * h + i] for i in range(4)], axis=1)

    def price(j, g, h):
        full = tile_of(g, h)
        terms = full[F:ROWS, :].astype(F32)
        lin = jnp.dot(ft[span(j), :], full[0:F, :], preferred_element_type=F32)
        value = terms[0:1, :] * (lin + terms[2:3, :] * jnp.tanh(lin - terms[1:2, :]))
        return lax.dot_general(value.astype(BF), hot[2 * g + h], NT, preferred_element_type=F32)

    def ring(s, j):
        src = own.at[cut(j)] if s == 0 else ring_in.at[s - 1, cut(j)]
        return remote(src, ring_in.at[s, cut(j)], sz.at[s, j], rz.at[s, j], p, ahead * NY + y)

    def side(j, way):
        origin = y if way < 2 else y_back
        target = y_back if way == 1 else y_ahead
        return remote(at[j].at[origin], at[j].at[origin], sy.at[j, way], ry.at[j, way], p, z * NY + target)

    def side_wait(j, way):
        origin = (y_back, y_ahead, lax.rem(y + 2, NY))[way]
        remote(at[j].at[origin], at[j].at[origin], sy.at[j, way], ry.at[j, way], p, z * NY + y_back).wait_recv()

    def add(d, j, value, start):
        if start:
            acc[d] = value
        else:
            acc[d] += value

    def left(j):
        return at[j][...].reshape(NY * CP, SIZES[j])

    def dots(d, j):
        right = own[span(j), :] if d == 0 else ring_in[d - 1, span(j), :]
        add(d, j, jnp.dot(left(j), right, preferred_element_type=F32), j == 0)

    def cell(d):
        return lax.rem(z + sign * d + NZ, NZ)

    near_x, wide_x = x + 1 - 2 * (x % 2), NX - 1 - x
    first_x = near_x + core * (wide_x - near_x)
    second_x = wide_x + core * (near_x - wide_x)
    passed = 6 - x - first_x - second_x

    def tile(d, i):
        return acc[d, pl.ds(pl.multiple_of(i * CP, CP), CP), :]

    def reduce(d, i):
        if d < 3:
            src, to = ((rsb.at[d, first_x], first_x), (rsb.at[d, passed], first_x), (mid.at[d], second_x))[i]
        else:
            to = lax.rem(x + i + 1, NX)
            src = rsb.at[d, to]
        return remote(src, rr.at[d, i], srs.at[d, i], rrs.at[d, i], 2 * to + core, c)

    def ship(d):
        rsb[d] = acc[d].reshape(NY, CP, CP).astype(BF)
        for i in ((1, 0) if d < 3 else (1, 0, 2)):
            go(reduce(d, i))

    def pass_on(d):
        reduce(d, 1).wait_recv()
        mid[d] = (tile(d, second_x) + rr[d, 1].astype(F32)).astype(BF)
        go(reduce(d, 2))

    def turned(d):
        return remote(turn.at[d], fa.at[core, y], sa.at[d], ra.at[core, y], cell(d), z * NY + x)

    def turned_home(d):
        return (cell(d) == p) & (x == y)

    def direct(d):
        return remote(keep.at[d], fb.at[core, x], sb.at[d], rb.at[core, x], z, cell(d) * NY + y)

    def collect(d):
        whole = tile(d, x)
        for i in ((0, 2) if d < 3 else (0, 1, 2)):
            reduce(d, i).wait_recv()
            whole = whole + rr[d, i].astype(F32)
        whole = whole * (1.0 / (paths * NP))
        if 0 < d < FAR:
            keep[d] = whole.astype(BF)
            go(direct(d))
        turn[d] = jnp.transpose(whole).astype(BF)

        @pl.when(jnp.logical_not(turned_home(d)))
        def _():
            turned(d).start()

        @pl.when(turned_home(d))
        def _():
            fa[core, y] = turn[d]

    def out(j):
        return pltpu.make_async_copy(own.at[cut(j)], exp_ref.at[cut(j)], sout.at[j])

    def relay(s, j):
        ring(s - 1, j).wait_recv()
        go(ring(s, j))

    def side_relay(j):
        side_wait(j, 0)
        go(side(j, 2))
        side_wait(j, 1)

    def far(j):
        ring(FAR - 1, j).wait_recv()
        dots(FAR, j)

    for j in range(CH):
        here = net.at[0:SIZES[j], :]

        def take(g, halves=(0, 1)):
            for h in halves:
                label = tile_of(g, h)[F:ROWS, :].astype(F32)[3:4, :]
                hot[2 * g + h] = (lax.broadcasted_iota(jnp.int32, (CP, 4 * SLOT), 0).astype(F32) == label).astype(F32).astype(BF)
            return sum(price(0, g, h) for h in halves)

        if j == 0:
            for i in (1, 0):
                for h in range(2):
                    go(give(i, h))
            here[...] = take(own_q)
            for h in range(2):
                given(0, h)
            here[...] += take(mate_q)
            for h in range(2):
                given(1, h)
                go(give(2, h))
            here[...] += take(beside_q)
            given(2, 0)
            here[...] += take(last_q, (0,))
            given(2, 1)
            here[...] += take(last_q, (1,))
        else:
            here[...] = jnp.zeros_like(here)
            for g in range(NQ):
                for h in range(2):
                    here[...] += price(j, g, h)
        block_f = jnp.maximum(here[...], 0.0)
        block_b = block_f.astype(BF)
        own[span(j), :] = block_b
        at[j][y] = jnp.transpose(block_f).astype(BF)
        go(ring(0, j))
        out(j).start()
        go(side(j, 0))
        go(side(j, 1))
        if j == 1:
            relay(1, 0)
    relay(1, 1)
    side_relay(0)
    relay(2, 0)
    side_relay(1)
    relay(1, 2)
    relay(2, 1)
    side_relay(2)
    side_wait(0, 2)
    for d in (0, 1, 2):
        dots(d, 0)
    relay(2, 2)
    relay(3, 0)
    dots(3, 0)
    side_wait(1, 2)
    for d in (0, 1, 2):
        dots(d, 1)
    relay(3, 1)
    side_wait(2, 2)
    for d in (0, 1, 2):
        dots(d, 2)
        ship(d)
    relay(3, 2)
    for j in (1, 2):
        dots(3, j)
    ship(3)
    far(0)
    far(1)
    for d in (0, 1, 2):
        pass_on(d)
    far(2)
    ship(FAR)
    for d in (3, 0, 1, 2, FAR):
        collect(d)

    delta = lax.rem(p - z + NZ, NZ)
    mom_ref[...] = jnp.zeros_like(mom_ref)
    for k in range(2):
        near = (delta <= FAR) if k == 0 else ((delta >= FAR) | (delta == 0))
        away = (delta > FAR) if k == 0 else ((delta < FAR) & (delta > 0))
        for i in range(NY):
            @pl.when(near & jnp.logical_not((core == k) & (i == y) & (x == y)))
            def _(k=k, i=i):
                remote(turn.at[0], fa.at[k, i], sa.at[0], ra.at[k, i], 2 * y + k, z * NY + i).wait_recv()

            @pl.when(near)
            def _(k=k, i=i):
                mom_ref[i] += fa[k, i].astype(F32)

            @pl.when(away)
            def _(k=k, i=i):
                remote(turn.at[0], fb.at[k, i], sb.at[0], rb.at[k, i], 2 * i + k, p * NY + y).wait_recv()
                mom_ref[i] += fb[k, i].astype(F32)

    for j in range(CH):
        out(j).wait()
    for i, k in enumerate(targets):
        copy = remote(pack.at[i], trades.at[quarter, place], s1.at[i], r1.at[place], p, k)

        @pl.when(k != c)
        def _(copy=copy):
            copy.wait_send()
    for copy in sends:
        copy.wait_send()
    for d in range(FAR + 1):
        @pl.when(jnp.logical_not(turned_home(d)))
        def _(d=d):
            turned(d).wait_send()


def hand_out(exp_in, mom_in, exp_out, mom_out, exp_buf, mom_buf, sin, sout):
    steps = []
    for a, (src, buf, dst) in enumerate(((exp_in, exp_buf, exp_out), (mom_in, mom_buf, mom_out))):
        rows = src.shape[0] // 4
        for i in range(4):
            part = pl.ds(i * rows, rows)
            steps.append((
                pltpu.make_async_copy(src.at[part], buf.at[part], sin.at[a, i]),
                pltpu.make_async_copy(buf.at[part], dst.at[part], sout.at[a, i])))
    for get, _ in steps:
        get.start()
    for get, put in steps:
        get.wait()
        put.start()
    for _, put in steps:
        put.wait()


def on_device(factors, loadings, notional, strike, curvature, trade_cpty):
    count, paths = loadings.shape[1], factors.shape[1]
    vmem = pl.BlockSpec(memory_space=pltpu.VMEM)
    dma = pltpu.SemaphoreType.DMA
    exposure, moment = pl.pallas_call(
        kernel,
        out_shape=(jax.ShapeDtypeStruct((paths, CP), BF), jax.ShapeDtypeStruct((NY, CP, CP), F32)),
        in_specs=[pl.BlockSpec(memory_space=pl.ANY)] * 6,
        out_specs=(pl.BlockSpec(memory_space=pl.ANY), vmem),
        scratch_shapes=[
            pltpu.VMEM((F, paths), BF),
            pltpu.VMEM((3, count // CP, CP), BF),
            pltpu.VMEM((1, count), jnp.int32),
            pltpu.VMEM((ROWS, count), BF),
            pltpu.VMEM((PER, ROWS, SLOT), BF),
            pltpu.VMEM((NQ, PER, ROWS, SLOT), BF),
            pltpu.VMEM((NP, CP, 4 * SLOT), BF),
            pltpu.VMEM((paths, F), BF),
            pltpu.VMEM((max(SIZES), CP), F32),
            pltpu.VMEM((paths, CP), BF),
            *[pltpu.VMEM((NY, CP, n), BF) for n in SIZES],
            pltpu.VMEM((FAR, paths, CP), BF),
            pltpu.VMEM((FAR + 1, NY * CP, CP), F32),
            pltpu.VMEM((FAR + 1, NY, CP, CP), BF),
            pltpu.VMEM((FAR + 1, CP, CP), BF),
            pltpu.VMEM((FAR + 1, 3, CP, CP), BF),
            pltpu.VMEM((FAR + 1, CP, CP), BF),
            pltpu.VMEM((FAR + 1, CP, CP), BF),
            pltpu.VMEM((2, NY, CP, CP), BF),
            pltpu.VMEM((2, NX, CP, CP), BF),
            dma((6,)), dma((CH,)), dma((PER,)), dma((PER,)), dma((3, 2)), dma((3, 2)),
            dma((CH, 3)), dma((CH, 3)), dma((FAR, CH)), dma((FAR, CH)),
            dma((FAR + 1, 3)), dma((FAR + 1, 3)),
            dma((FAR + 1,)), dma((2, NY)), dma((FAR + 1,)), dma((2, NX)),
        ],
        compiler_params=pltpu.CompilerParams(
            collective_id=0, has_side_effects=True, vmem_limit_bytes=67043328),
    )(factors, loadings, *[a.reshape(count // CP, CP) for a in (notional, strike, curvature)],
      trade_cpty[None, :])
    shapes = [(exposure.shape, BF), (moment.shape, F32)]
    anywhere = pl.BlockSpec(memory_space=pl.ANY)
    exposure, moment = pl.pallas_call(
        hand_out,
        out_shape=tuple(jax.ShapeDtypeStruct(*s) for s in shapes),
        in_specs=[anywhere] * 2,
        out_specs=(anywhere,) * 2,
        scratch_shapes=[*[pltpu.VMEM(*s) for s in shapes], dma((2, 4)), dma((2, 4))],
        compiler_params=pltpu.CompilerParams(vmem_limit_bytes=67043328),
    )(exposure, moment)
    return exposure, moment.reshape(NY * CP, CP)


def solution(mesh):
    in_specs = (P(None, "paths"), P(None, "cpty"), P("cpty"), P("cpty"), P("cpty"), P("cpty"))
    out_specs = (P("paths", "cpty"), P("paths", "cpty"))
    return jax.shard_map(
        on_device, mesh=mesh, in_specs=in_specs, out_specs=out_specs, check_vma=False
    )
```

```python
import jax
import jax.numpy as jnp
from jax import lax
from jax.experimental import pallas as pl
from jax.experimental.pallas import tpu as pltpu
from jax.sharding import PartitionSpec as P

NP, NX, NZ, NY = 8, 4, 8, 4
FAR = 4
CP = 128
ROWS = 80
SLOT = 128
F = 64
SIZES = (640, 512, 384)
STARTS = (0, 640, 1152)
CH = len(SIZES)
NQ, PER = 4, 8
BF, F32 = jnp.bfloat16, jnp.float32
NT = (((1,), (1,)), ((), ()))


def remote(src, dst, ssem, rsem, p, c):
    return pltpu.make_async_remote_copy(
        src_ref=src, dst_ref=dst, send_sem=ssem, recv_sem=rsem,
        device_id={"paths": p, "cpty": c}, device_id_type=pl.DeviceIdType.MESH,
    )


def kernel(fac_hbm, load_hbm, not_hbm, str_hbm, cur_hbm, id_hbm, exp_ref, mom_ref,
           fac_ref, term_in, id_ref, desc, pack, trades, hot, ft, net, own, at0, at1, at2,
           ring_in, acc, rsb, mid, rr, keep, turn, fa, fb, sin,
           sout, s1, r1, s2, r2, sy, ry, sz, rz, srs, rrs, sa, ra, sb, rb):
    p = lax.axis_index("paths")
    c = lax.axis_index("cpty")
    z, y = c // NY, c % NY
    at = (at0, at1, at2)
    paths = fac_ref.shape[1]
    count = id_ref.shape[1]
    quarter = 2 * (p // 2 % 2) + p % 2
    first = lax.rem(quarter - c + NZ * NY, NQ)
    targets = [first + NQ * i for i in range(PER)]
    x, core = p // 2, p % 2
    sign = 1 - 2 * core
    ahead, behind = lax.rem(z - sign + NZ, NZ), lax.rem(z + sign + NZ, NZ)
    y_ahead, y_back = lax.rem(y - sign + NY, NY), lax.rem(y + sign + NY, NY)

    loads = [
        pltpu.make_async_copy(src, dst, sin.at[i])
        for i, (src, dst) in enumerate((
            (id_hbm, id_ref), (not_hbm, term_in.at[0]), (str_hbm, term_in.at[1]),
            (cur_hbm, term_in.at[2]), (load_hbm, desc.at[0:F, :]), (fac_hbm, fac_ref)))
    ]
    for copy in loads:
        copy.start()

    barrier = pltpu.get_barrier_semaphore()

    def greet(pp, cc):
        pl.semaphore_signal(barrier, inc=1, device_id={"paths": pp, "cpty": cc},
                            device_id_type=pl.DeviceIdType.MESH)

    for k in targets:
        @pl.when(k != c)
        def _(k=k):
            greet(p, k)
    for r in range(1, NP):
        greet(lax.rem(p + r, NP), c)
    greet(p, ahead * NY + y)
    greet(p, behind * NY + y)
    for r in range(1, NY):
        greet(p, z * NY + lax.rem(y + r, NY))

    loads[0].wait()

    ids = id_ref[...]
    owner = ids // CP
    block = 256
    upper = (lax.broadcasted_iota(jnp.int32, (block, block), 0)
             < lax.broadcasted_iota(jnp.int32, (block, block), 1)).astype(BF)
    eq = (lax.broadcasted_iota(jnp.int32, (NZ * NY, count), 0) == owner).astype(F32)
    base = jnp.zeros((NZ * NY, 1), F32)
    ranks = []
    for b in range(count // block):
        part = eq[:, b * block:(b + 1) * block]
        before = jnp.dot(part.astype(BF), upper, preferred_element_type=F32) + base
        base = base + jnp.sum(part, axis=1, keepdims=True)
        ranks.append(jnp.sum(part * before, axis=0, keepdims=True))
    rank = jnp.concatenate(ranks, axis=1).astype(jnp.int32)
    mine = lax.rem(owner + c, NQ) == quarter
    code = jnp.where(mine, (owner // NQ) * SLOT + rank, -1)
    for copy in loads[1:5]:
        copy.wait()
    line = lax.broadcasted_iota(jnp.int32, (ROWS - F, count), 0)
    extra = jnp.where(line == 3, (ids % CP).astype(F32), 0.0)
    for i in range(3):
        cells = term_in[i].astype(F32)
        flat = jnp.concatenate([cells[k:k + 1, :] for k in range(count // CP)], axis=1)
        extra = jnp.where(line == i, flat, extra)
    desc[F:ROWS, :] = extra.astype(BF)
    total = jnp.zeros((ROWS, PER * SLOT), F32)
    step = 512
    for b in range(count // step):
        cols = slice(b * step, (b + 1) * step)
        chosen = (lax.broadcasted_iota(jnp.int32, (PER * SLOT, step), 0) == code[:, cols]).astype(F32).astype(BF)
        total = total + lax.dot_general(desc[:, cols], chosen, NT, preferred_element_type=F32)
    for i in range(PER):
        pack[i] = total[:, i * SLOT:(i + 1) * SLOT].astype(BF)

    pl.semaphore_wait(barrier, NP - 1 + 2 + NY - 1 + PER - (lax.rem(2 * c, NQ) == quarter).astype(jnp.int32))

    place = c // NQ
    for offset in (4, 3, 5, 2, 6, 1, 7, 0):
        i = lax.rem(z + offset, PER)
        copy = remote(pack.at[i], trades.at[quarter, place], s1.at[i], r1.at[place], p, first + NQ * i)
        if offset:
            copy.start()
        else:
            @pl.when(first != y)
            def _(copy=copy):
                copy.start()

            @pl.when(first == y)
            def _(i=i):
                trades[quarter, place] = pack[i]
    loads[5].wait()
    ft[...] = jnp.transpose(fac_ref[...].astype(F32)).astype(BF)
    for i, k in enumerate(targets):
        arrive = remote(pack.at[i], trades.at[quarter, i], s1.at[i], r1.at[i], p, k)

        @pl.when(k != c)
        def _(arrive=arrive):
            arrive.wait_recv()
    sends = []

    def go(copy):
        copy.start()
        sends.append(copy)

    x_ahead = lax.rem(x - sign + NX, NX)
    partner = 2 * x + 1 - core
    own_q, mate_q = quarter, quarter + 1 - 2 * core
    beside_q, last_q = lax.rem(own_q + 2, NQ), lax.rem(mate_q + 2, NQ)

    def half(part, h):
        return trades.at[part, pl.ds(4 * h, 4)]

    def give(i, h):
        part = beside_q if i == 2 else own_q
        to = 2 * x_ahead + core if i == 1 else partner
        return remote(half(part, h), half(part, h), s2.at[i, h], r2.at[i, h], to, c)

    def given(i, h):
        part = (mate_q, beside_q, last_q)[i]
        remote(half(part, h), half(part, h), s2.at[i, h], r2.at[i, h], partner, c).wait_recv()

    def span(j):
        return slice(STARTS[j], STARTS[j] + SIZES[j])

    def cut(j):
        return pl.ds(STARTS[j], SIZES[j])

    def tile_of(g, h):
        return jnp.concatenate([trades[g, 4 * h + i] for i in range(4)], axis=1)

    def price(j, g, h):
        full = tile_of(g, h)
        terms = full[F:ROWS, :].astype(F32)
        lin = jnp.dot(ft[span(j), :], full[0:F, :], preferred_element_type=F32)
        value = terms[0:1, :] * (lin + terms[2:3, :] * jnp.tanh(lin - terms[1:2, :]))
        return lax.dot_general(value.astype(BF), hot[2 * g + h], NT, preferred_element_type=F32)

    def ring(s, j):
        src = own.at[cut(j)] if s == 0 else ring_in.at[s - 1, cut(j)]
        return remote(src, ring_in.at[s, cut(j)], sz.at[s, j], rz.at[s, j], p, ahead * NY + y)

    def side(j, way):
        origin = y if way < 2 else y_back
        target = y_back if way == 1 else y_ahead
        return remote(at[j].at[origin], at[j].at[origin], sy.at[j, way], ry.at[j, way], p, z * NY + target)

    def side_wait(j, way):
        origin = (y_back, y_ahead, lax.rem(y + 2, NY))[way]
        remote(at[j].at[origin], at[j].at[origin], sy.at[j, way], ry.at[j, way], p, z * NY + y_back).wait_recv()

    def add(d, j, value, start):
        if start:
            acc[d] = value
        else:
            acc[d] += value

    def left(j):
        return at[j][...].reshape(NY * CP, SIZES[j])

    def dots(d, j):
        right = own[span(j), :] if d == 0 else ring_in[d - 1, span(j), :]
        add(d, j, jnp.dot(left(j), right, preferred_element_type=F32), j == 0)

    def cell(d):
        return lax.rem(z + sign * d + NZ, NZ)

    near_x, wide_x = x + 1 - 2 * (x % 2), NX - 1 - x
    first_x = near_x + core * (wide_x - near_x)
    second_x = wide_x + core * (near_x - wide_x)
    passed = 6 - x - first_x - second_x

    def tile(d, i):
        return acc[d, pl.ds(pl.multiple_of(i * CP, CP), CP), :]

    def reduce(d, i):
        if d < 3:
            src, to = ((rsb.at[d, first_x], first_x), (rsb.at[d, passed], first_x), (mid.at[d], second_x))[i]
        else:
            to = lax.rem(x + i + 1, NX)
            src = rsb.at[d, to]
        return remote(src, rr.at[d, i], srs.at[d, i], rrs.at[d, i], 2 * to + core, c)

    def ship(d):
        rsb[d] = acc[d].reshape(NY, CP, CP).astype(BF)
        for i in ((1, 0) if d < 3 else (1, 0, 2)):
            go(reduce(d, i))

    def pass_on(d):
        reduce(d, 1).wait_recv()
        mid[d] = (tile(d, second_x) + rr[d, 1].astype(F32)).astype(BF)
        go(reduce(d, 2))

    def turned(d):
        return remote(turn.at[d], fa.at[core, y], sa.at[d], ra.at[core, y], cell(d), z * NY + x)

    def turned_home(d):
        return (cell(d) == p) & (x == y)

    def direct(d):
        return remote(keep.at[d], fb.at[core, x], sb.at[d], rb.at[core, x], z, cell(d) * NY + y)

    def collect(d):
        whole = tile(d, x)
        for i in ((0, 2) if d < 3 else (0, 1, 2)):
            reduce(d, i).wait_recv()
            whole = whole + rr[d, i].astype(F32)
        whole = whole * (1.0 / (paths * NP))
        if 0 < d < FAR:
            keep[d] = whole.astype(BF)
            go(direct(d))
        turn[d] = jnp.transpose(whole).astype(BF)

        @pl.when(jnp.logical_not(turned_home(d)))
        def _():
            turned(d).start()

        @pl.when(turned_home(d))
        def _():
            fa[core, y] = turn[d]

    def out(j):
        return pltpu.make_async_copy(own.at[cut(j)], exp_ref.at[cut(j)], sout.at[j])

    def relay(s, j):
        ring(s - 1, j).wait_recv()
        go(ring(s, j))

    def side_relay(j):
        side_wait(j, 0)
        go(side(j, 2))
        side_wait(j, 1)

    def far(j):
        ring(FAR - 1, j).wait_recv()
        dots(FAR, j)

    for j in range(CH):
        here = net.at[0:SIZES[j], :]

        def take(g, halves=(0, 1)):
            for h in halves:
                label = tile_of(g, h)[F:ROWS, :].astype(F32)[3:4, :]
                hot[2 * g + h] = (lax.broadcasted_iota(jnp.int32, (CP, 4 * SLOT), 0).astype(F32) == label).astype(F32).astype(BF)
            return sum(price(0, g, h) for h in halves)

        if j == 0:
            for i in (1, 0):
                for h in range(2):
                    go(give(i, h))
            here[...] = take(own_q)
            for h in range(2):
                given(0, h)
            here[...] += take(mate_q)
            for h in range(2):
                given(1, h)
                go(give(2, h))
            here[...] += take(beside_q)
            given(2, 0)
            here[...] += take(last_q, (0,))
            given(2, 1)
            here[...] += take(last_q, (1,))
        else:
            here[...] = jnp.zeros_like(here)
            for g in range(NQ):
                for h in range(2):
                    here[...] += price(j, g, h)
        block_f = jnp.maximum(here[...], 0.0)
        block_b = block_f.astype(BF)
        own[span(j), :] = block_b
        at[j][y] = jnp.transpose(block_f).astype(BF)
        go(ring(0, j))
        out(j).start()
        go(side(j, 0))
        go(side(j, 1))
        if j == 1:
            relay(1, 0)
    relay(1, 1)
    side_relay(0)
    relay(2, 0)
    side_relay(1)
    relay(1, 2)
    relay(2, 1)
    side_relay(2)
    relay(3, 0)
    side_wait(0, 2)
    for d in (0, 1, 2):
        dots(d, 0)
    relay(2, 2)
    dots(3, 0)
    side_wait(1, 2)
    for d in (0, 1, 2):
        dots(d, 1)
    relay(3, 1)
    side_wait(2, 2)
    for d in (0, 1, 2):
        dots(d, 2)
        ship(d)
    relay(3, 2)
    for j in (1, 2):
        dots(3, j)
    ship(3)
    far(0)
    far(1)
    for d in (0, 1, 2):
        pass_on(d)
    far(2)
    ship(FAR)
    for d in (3, 0, 1, 2, FAR):
        collect(d)

    delta = lax.rem(p - z + NZ, NZ)
    mom_ref[...] = jnp.zeros_like(mom_ref)
    for k in range(2):
        near = (delta <= FAR) if k == 0 else ((delta >= FAR) | (delta == 0))
        away = (delta > FAR) if k == 0 else ((delta < FAR) & (delta > 0))
        for i in range(NY):
            @pl.when(near & jnp.logical_not((core == k) & (i == y) & (x == y)))
            def _(k=k, i=i):
                remote(turn.at[0], fa.at[k, i], sa.at[0], ra.at[k, i], 2 * y + k, z * NY + i).wait_recv()

            @pl.when(near)
            def _(k=k, i=i):
                mom_ref[i] += fa[k, i].astype(F32)

            @pl.when(away)
            def _(k=k, i=i):
                remote(turn.at[0], fb.at[k, i], sb.at[0], rb.at[k, i], 2 * i + k, p * NY + y).wait_recv()
                mom_ref[i] += fb[k, i].astype(F32)

    for j in range(CH):
        out(j).wait()
    for i, k in enumerate(targets):
        copy = remote(pack.at[i], trades.at[quarter, place], s1.at[i], r1.at[place], p, k)

        @pl.when(k != c)
        def _(copy=copy):
            copy.wait_send()
    for copy in sends:
        copy.wait_send()
    for d in range(FAR + 1):
        @pl.when(jnp.logical_not(turned_home(d)))
        def _(d=d):
            turned(d).wait_send()


def hand_out(exp_in, mom_in, exp_out, mom_out, exp_buf, mom_buf, sin, sout):
    steps = []
    for a, (src, buf, dst) in enumerate(((exp_in, exp_buf, exp_out), (mom_in, mom_buf, mom_out))):
        rows = src.shape[0] // 4
        for i in range(4):
            part = pl.ds(i * rows, rows)
            steps.append((
                pltpu.make_async_copy(src.at[part], buf.at[part], sin.at[a, i]),
                pltpu.make_async_copy(buf.at[part], dst.at[part], sout.at[a, i])))
    for get, _ in steps:
        get.start()
    for get, put in steps:
        get.wait()
        put.start()
    for _, put in steps:
        put.wait()


def on_device(factors, loadings, notional, strike, curvature, trade_cpty):
    count, paths = loadings.shape[1], factors.shape[1]
    vmem = pl.BlockSpec(memory_space=pltpu.VMEM)
    dma = pltpu.SemaphoreType.DMA
    exposure, moment = pl.pallas_call(
        kernel,
        out_shape=(jax.ShapeDtypeStruct((paths, CP), BF), jax.ShapeDtypeStruct((NY, CP, CP), F32)),
        in_specs=[pl.BlockSpec(memory_space=pl.ANY)] * 6,
        out_specs=(pl.BlockSpec(memory_space=pl.ANY), vmem),
        scratch_shapes=[
            pltpu.VMEM((F, paths), BF),
            pltpu.VMEM((3, count // CP, CP), BF),
            pltpu.VMEM((1, count), jnp.int32),
            pltpu.VMEM((ROWS, count), BF),
            pltpu.VMEM((PER, ROWS, SLOT), BF),
            pltpu.VMEM((NQ, PER, ROWS, SLOT), BF),
            pltpu.VMEM((NP, CP, 4 * SLOT), BF),
            pltpu.VMEM((paths, F), BF),
            pltpu.VMEM((max(SIZES), CP), F32),
            pltpu.VMEM((paths, CP), BF),
            *[pltpu.VMEM((NY, CP, n), BF) for n in SIZES],
            pltpu.VMEM((FAR, paths, CP), BF),
            pltpu.VMEM((FAR + 1, NY * CP, CP), F32),
            pltpu.VMEM((FAR + 1, NY, CP, CP), BF),
            pltpu.VMEM((FAR + 1, CP, CP), BF),
            pltpu.VMEM((FAR + 1, 3, CP, CP), BF),
            pltpu.VMEM((FAR + 1, CP, CP), BF),
            pltpu.VMEM((FAR + 1, CP, CP), BF),
            pltpu.VMEM((2, NY, CP, CP), BF),
            pltpu.VMEM((2, NX, CP, CP), BF),
            dma((6,)), dma((CH,)), dma((PER,)), dma((PER,)), dma((3, 2)), dma((3, 2)),
            dma((CH, 3)), dma((CH, 3)), dma((FAR, CH)), dma((FAR, CH)),
            dma((FAR + 1, 3)), dma((FAR + 1, 3)),
            dma((FAR + 1,)), dma((2, NY)), dma((FAR + 1,)), dma((2, NX)),
        ],
        compiler_params=pltpu.CompilerParams(
            collective_id=0, has_side_effects=True, vmem_limit_bytes=67043328),
    )(factors, loadings, *[a.reshape(count // CP, CP) for a in (notional, strike, curvature)],
      trade_cpty[None, :])
    shapes = [(exposure.shape, BF), (moment.shape, F32)]
    anywhere = pl.BlockSpec(memory_space=pl.ANY)
    exposure, moment = pl.pallas_call(
        hand_out,
        out_shape=tuple(jax.ShapeDtypeStruct(*s) for s in shapes),
        in_specs=[anywhere] * 2,
        out_specs=(anywhere,) * 2,
        scratch_shapes=[*[pltpu.VMEM(*s) for s in shapes], dma((2, 4)), dma((2, 4))],
        compiler_params=pltpu.CompilerParams(vmem_limit_bytes=67043328),
    )(exposure, moment)
    return exposure, moment.reshape(NY * CP, CP)


def solution(mesh):
    in_specs = (P(None, "paths"), P(None, "cpty"), P("cpty"), P("cpty"), P("cpty"), P("cpty"))
    out_specs = (P("paths", "cpty"), P("paths", "cpty"))
    return jax.shard_map(
        on_device, mesh=mesh, in_specs=in_specs, out_specs=out_specs, check_vma=False
    )
```

```python
import jax
import jax.numpy as jnp
from jax import lax
from jax.experimental import pallas as pl
from jax.experimental.pallas import tpu as pltpu
from jax.sharding import PartitionSpec as P

NP, NX, NZ, NY = 8, 4, 8, 4
FAR = 4
CP = 128
ROWS = 80
SLOT = 128
F = 64
SIZES = (640, 512, 384)
STARTS = (0, 640, 1152)
CH = len(SIZES)
NQ, PER = 4, 8
BF, F32 = jnp.bfloat16, jnp.float32
NT = (((1,), (1,)), ((), ()))


def remote(src, dst, ssem, rsem, p, c):
    return pltpu.make_async_remote_copy(
        src_ref=src, dst_ref=dst, send_sem=ssem, recv_sem=rsem,
        device_id={"paths": p, "cpty": c}, device_id_type=pl.DeviceIdType.MESH,
    )


def kernel(fac_hbm, load_hbm, not_hbm, str_hbm, cur_hbm, id_hbm, exp_ref, mom_ref,
           fac_ref, term_in, id_ref, desc, pack, trades, hot, ft, net, own, at0, at1, at2,
           ring_in, acc, rsb, mid, rr, keep, turn, fa, fb, sin,
           sout, s1, r1, s2, r2, sy, ry, sz, rz, srs, rrs, sa, ra, sb, rb):
    p = lax.axis_index("paths")
    c = lax.axis_index("cpty")
    z, y = c // NY, c % NY
    at = (at0, at1, at2)
    paths = fac_ref.shape[1]
    count = id_ref.shape[1]
    quarter = 2 * (p // 2 % 2) + p % 2
    first = lax.rem(quarter - c + NZ * NY, NQ)
    targets = [first + NQ * i for i in range(PER)]
    x, core = p // 2, p % 2
    sign = 1 - 2 * core
    ahead, behind = lax.rem(z - sign + NZ, NZ), lax.rem(z + sign + NZ, NZ)
    y_ahead, y_back = lax.rem(y - sign + NY, NY), lax.rem(y + sign + NY, NY)

    loads = [
        pltpu.make_async_copy(src, dst, sin.at[i])
        for i, (src, dst) in enumerate((
            (id_hbm, id_ref), (not_hbm, term_in.at[0]), (str_hbm, term_in.at[1]),
            (cur_hbm, term_in.at[2]), (load_hbm, desc.at[0:F, :]), (fac_hbm, fac_ref)))
    ]
    for copy in loads:
        copy.start()

    barrier = pltpu.get_barrier_semaphore()

    def greet(pp, cc):
        pl.semaphore_signal(barrier, inc=1, device_id={"paths": pp, "cpty": cc},
                            device_id_type=pl.DeviceIdType.MESH)

    for k in targets:
        @pl.when(k != c)
        def _(k=k):
            greet(p, k)
    for r in range(1, NP):
        greet(lax.rem(p + r, NP), c)
    greet(p, ahead * NY + y)
    greet(p, behind * NY + y)
    for r in range(1, NY):
        greet(p, z * NY + lax.rem(y + r, NY))

    loads[0].wait()

    ids = id_ref[...]
    owner = ids // CP
    block = 256
    upper = (lax.broadcasted_iota(jnp.int32, (block, block), 0)
             < lax.broadcasted_iota(jnp.int32, (block, block), 1)).astype(BF)
    eq = (lax.broadcasted_iota(jnp.int32, (NZ * NY, count), 0) == owner).astype(F32)
    base = jnp.zeros((NZ * NY, 1), F32)
    ranks = []
    for b in range(count // block):
        part = eq[:, b * block:(b + 1) * block]
        before = jnp.dot(part.astype(BF), upper, preferred_element_type=F32) + base
        base = base + jnp.sum(part, axis=1, keepdims=True)
        ranks.append(jnp.sum(part * before, axis=0, keepdims=True))
    rank = jnp.concatenate(ranks, axis=1).astype(jnp.int32)
    mine = lax.rem(owner + c, NQ) == quarter
    code = jnp.where(mine, lax.rem(owner // NQ + 6 + NZ - z, NZ) * SLOT + rank, -1)
    for copy in loads[1:5]:
        copy.wait()
    line = lax.broadcasted_iota(jnp.int32, (ROWS - F, count), 0)
    extra = jnp.where(line == 3, (ids % CP).astype(F32), 0.0)
    for i in range(3):
        cells = term_in[i].astype(F32)
        flat = jnp.concatenate([cells[k:k + 1, :] for k in range(count // CP)], axis=1)
        extra = jnp.where(line == i, flat, extra)
    desc[F:ROWS, :] = extra.astype(BF)
    place = c // NQ

    def fill(group):
        step, wide = 512, PER // 2
        total = jnp.zeros((ROWS, wide * SLOT), F32)
        for b in range(count // step):
            cols = slice(b * step, (b + 1) * step)
            slots = lax.broadcasted_iota(jnp.int32, (wide * SLOT, step), 0) + group * wide * SLOT
            chosen = (slots == code[:, cols]).astype(F32).astype(BF)
            total = total + lax.dot_general(desc[:, cols], chosen, NT, preferred_element_type=F32)
        for i in range(wide):
            pack[group * wide + i] = total[:, i * SLOT:(i + 1) * SLOT].astype(BF)

    def hand_over(g):
        to = first + NQ * lax.rem(z + g + 2, NZ)
        return remote(pack.at[g], trades.at[quarter, place], s1.at[g], r1.at[place], p, to)

    fill(0)
    pl.semaphore_wait(barrier, NP - 1 + 2 + NY - 1 + PER - (lax.rem(2 * c, NQ) == quarter).astype(jnp.int32))
    for g in (2, 1, 3, 0):
        hand_over(g).start()
    fill(1)
    for g in (4, 5, 7):
        hand_over(g).start()

    @pl.when(first != y)
    def _():
        hand_over(6).start()

    @pl.when(first == y)
    def _():
        trades[quarter, place] = pack[6]

    loads[5].wait()
    ft[...] = jnp.transpose(fac_ref[...].astype(F32)).astype(BF)
    for i, k in enumerate(targets):
        arrive = remote(pack.at[i], trades.at[quarter, i], s1.at[i], r1.at[i], p, k)

        @pl.when(k != c)
        def _(arrive=arrive):
            arrive.wait_recv()
    sends = []

    def go(copy):
        copy.start()
        sends.append(copy)

    x_ahead = lax.rem(x - sign + NX, NX)
    partner = 2 * x + 1 - core
    own_q, mate_q = quarter, quarter + 1 - 2 * core
    beside_q, last_q = lax.rem(own_q + 2, NQ), lax.rem(mate_q + 2, NQ)

    def half(part, h):
        return trades.at[part, pl.ds(4 * h, 4)]

    def give(i, h):
        part = beside_q if i == 2 else own_q
        to = 2 * x_ahead + core if i == 1 else partner
        return remote(half(part, h), half(part, h), s2.at[i, h], r2.at[i, h], to, c)

    def given(i, h):
        part = (mate_q, beside_q, last_q)[i]
        remote(half(part, h), half(part, h), s2.at[i, h], r2.at[i, h], partner, c).wait_recv()

    def span(j):
        return slice(STARTS[j], STARTS[j] + SIZES[j])

    def cut(j):
        return pl.ds(STARTS[j], SIZES[j])

    def tile_of(g, h):
        return jnp.concatenate([trades[g, 4 * h + i] for i in range(4)], axis=1)

    def price(j, g, h):
        full = tile_of(g, h)
        terms = full[F:ROWS, :].astype(F32)
        lin = jnp.dot(ft[span(j), :], full[0:F, :], preferred_element_type=F32)
        value = terms[0:1, :] * (lin + terms[2:3, :] * jnp.tanh(lin - terms[1:2, :]))
        return lax.dot_general(value.astype(BF), hot[2 * g + h], NT, preferred_element_type=F32)

    def ring(s, j):
        src = own.at[cut(j)] if s == 0 else ring_in.at[s - 1, cut(j)]
        return remote(src, ring_in.at[s, cut(j)], sz.at[s, j], rz.at[s, j], p, ahead * NY + y)

    def side(j, way):
        origin = y if way < 2 else y_back
        target = y_back if way == 1 else y_ahead
        return remote(at[j].at[origin], at[j].at[origin], sy.at[j, way], ry.at[j, way], p, z * NY + target)

    def side_wait(j, way):
        origin = (y_back, y_ahead, lax.rem(y + 2, NY))[way]
        remote(at[j].at[origin], at[j].at[origin], sy.at[j, way], ry.at[j, way], p, z * NY + y_back).wait_recv()

    def add(d, j, value, start):
        if start:
            acc[d] = value
        else:
            acc[d] += value

    def left(j):
        return at[j][...].reshape(NY * CP, SIZES[j])

    def dots(d, j):
        right = own[span(j), :] if d == 0 else ring_in[d - 1, span(j), :]
        add(d, j, jnp.dot(left(j), right, preferred_element_type=F32), j == 0)

    def cell(d):
        return lax.rem(z + sign * d + NZ, NZ)

    near_x, wide_x = x + 1 - 2 * (x % 2), NX - 1 - x
    first_x = near_x + core * (wide_x - near_x)
    second_x = wide_x + core * (near_x - wide_x)
    passed = 6 - x - first_x - second_x

    def tile(d, i):
        return acc[d, pl.ds(pl.multiple_of(i * CP, CP), CP), :]

    def reduce(d, i):
        if d < 3:
            src, to = ((rsb.at[d, first_x], first_x), (rsb.at[d, passed], first_x), (mid.at[d], second_x))[i]
        else:
            to = lax.rem(x + i + 1, NX)
            src = rsb.at[d, to]
        return remote(src, rr.at[d, i], srs.at[d, i], rrs.at[d, i], 2 * to + core, c)

    def ship(d):
        rsb[d] = acc[d].reshape(NY, CP, CP).astype(BF)
        for i in ((1, 0) if d < 3 else (1, 0, 2)):
            go(reduce(d, i))

    def pass_on(d):
        reduce(d, 1).wait_recv()
        mid[d] = (tile(d, second_x) + rr[d, 1].astype(F32)).astype(BF)
        go(reduce(d, 2))

    def turned(d):
        return remote(turn.at[d], fa.at[core, y], sa.at[d], ra.at[core, y], cell(d), z * NY + x)

    def turned_home(d):
        return (cell(d) == p) & (x == y)

    def direct(d):
        return remote(keep.at[d], fb.at[core, x], sb.at[d], rb.at[core, x], z, cell(d) * NY + y)

    def collect(d):
        whole = tile(d, x)
        for i in ((0, 2) if d < 3 else (0, 1, 2)):
            reduce(d, i).wait_recv()
            whole = whole + rr[d, i].astype(F32)
        whole = whole * (1.0 / (paths * NP))
        if 0 < d < FAR:
            keep[d] = whole.astype(BF)
            go(direct(d))
        turn[d] = jnp.transpose(whole).astype(BF)

        @pl.when(jnp.logical_not(turned_home(d)))
        def _():
            turned(d).start()

        @pl.when(turned_home(d))
        def _():
            fa[core, y] = turn[d]

    def out(j):
        return pltpu.make_async_copy(own.at[cut(j)], exp_ref.at[cut(j)], sout.at[j])

    def relay(s, j):
        ring(s - 1, j).wait_recv()
        go(ring(s, j))

    def side_relay(j):
        side_wait(j, 0)
        go(side(j, 2))
        side_wait(j, 1)

    def far(j):
        ring(FAR - 1, j).wait_recv()
        dots(FAR, j)

    for j in range(CH):
        here = net.at[0:SIZES[j], :]

        def take(g, halves=(0, 1)):
            for h in halves:
                label = tile_of(g, h)[F:ROWS, :].astype(F32)[3:4, :]
                hot[2 * g + h] = (lax.broadcasted_iota(jnp.int32, (CP, 4 * SLOT), 0).astype(F32) == label).astype(F32).astype(BF)
            return sum(price(0, g, h) for h in halves)

        if j == 0:
            for i in (1, 0):
                for h in range(2):
                    go(give(i, h))
            here[...] = take(own_q)
            for h in range(2):
                given(0, h)
            here[...] += take(mate_q)
            for h in range(2):
                given(1, h)
                go(give(2, h))
            here[...] += take(beside_q)
            given(2, 0)
            here[...] += take(last_q, (0,))
            given(2, 1)
            here[...] += take(last_q, (1,))
        else:
            here[...] = jnp.zeros_like(here)
            for g in range(NQ):
                for h in range(2):
                    here[...] += price(j, g, h)
        block_f = jnp.maximum(here[...], 0.0)
        block_b = block_f.astype(BF)
        own[span(j), :] = block_b
        at[j][y] = jnp.transpose(block_f).astype(BF)
        go(ring(0, j))
        out(j).start()
        go(side(j, 0))
        go(side(j, 1))
        if j == 1:
            relay(1, 0)
    relay(1, 1)
    side_relay(0)
    relay(2, 0)
    side_relay(1)
    relay(1, 2)
    relay(2, 1)
    side_relay(2)
    side_wait(0, 2)
    for d in (0, 1, 2):
        dots(d, 0)
    relay(2, 2)
    relay(3, 0)
    dots(3, 0)
    side_wait(1, 2)
    for d in (0, 1, 2):
        dots(d, 1)
    relay(3, 1)
    side_wait(2, 2)
    for d in (0, 1, 2):
        dots(d, 2)
        ship(d)
    relay(3, 2)
    for j in (1, 2):
        dots(3, j)
    ship(3)
    far(0)
    far(1)
    for d in (0, 1, 2):
        pass_on(d)
    far(2)
    ship(FAR)
    for d in (3, 0, 1, 2, FAR):
        collect(d)

    delta = lax.rem(p - z + NZ, NZ)
    mom_ref[...] = jnp.zeros_like(mom_ref)
    for k in range(2):
        near = (delta <= FAR) if k == 0 else ((delta >= FAR) | (delta == 0))
        away = (delta > FAR) if k == 0 else ((delta < FAR) & (delta > 0))
        for i in range(NY):
            @pl.when(near & jnp.logical_not((core == k) & (i == y) & (x == y)))
            def _(k=k, i=i):
                remote(turn.at[0], fa.at[k, i], sa.at[0], ra.at[k, i], 2 * y + k, z * NY + i).wait_recv()

            @pl.when(near)
            def _(k=k, i=i):
                mom_ref[i] += fa[k, i].astype(F32)

            @pl.when(away)
            def _(k=k, i=i):
                remote(turn.at[0], fb.at[k, i], sb.at[0], rb.at[k, i], 2 * i + k, p * NY + y).wait_recv()
                mom_ref[i] += fb[k, i].astype(F32)

    for j in range(CH):
        out(j).wait()
    for g in (0, 1, 2, 3, 4, 5, 7):
        hand_over(g).wait_send()

    @pl.when(first != y)
    def _():
        hand_over(6).wait_send()

    for copy in sends:
        copy.wait_send()
    for d in range(FAR + 1):
        @pl.when(jnp.logical_not(turned_home(d)))
        def _(d=d):
            turned(d).wait_send()


def hand_out(exp_in, mom_in, exp_out, mom_out, exp_buf, mom_buf, sin, sout):
    steps = []
    for a, (src, buf, dst) in enumerate(((exp_in, exp_buf, exp_out), (mom_in, mom_buf, mom_out))):
        rows = src.shape[0] // 4
        for i in range(4):
            part = pl.ds(i * rows, rows)
            steps.append((
                pltpu.make_async_copy(src.at[part], buf.at[part], sin.at[a, i]),
                pltpu.make_async_copy(buf.at[part], dst.at[part], sout.at[a, i])))
    for get, _ in steps:
        get.start()
    for get, put in steps:
        get.wait()
        put.start()
    for _, put in steps:
        put.wait()


def on_device(factors, loadings, notional, strike, curvature, trade_cpty):
    count, paths = loadings.shape[1], factors.shape[1]
    vmem = pl.BlockSpec(memory_space=pltpu.VMEM)
    dma = pltpu.SemaphoreType.DMA
    exposure, moment = pl.pallas_call(
        kernel,
        out_shape=(jax.ShapeDtypeStruct((paths, CP), BF), jax.ShapeDtypeStruct((NY, CP, CP), F32)),
        in_specs=[pl.BlockSpec(memory_space=pl.ANY)] * 6,
        out_specs=(pl.BlockSpec(memory_space=pl.ANY), vmem),
        scratch_shapes=[
            pltpu.VMEM((F, paths), BF),
            pltpu.VMEM((3, count // CP, CP), BF),
            pltpu.VMEM((1, count), jnp.int32),
            pltpu.VMEM((ROWS, count), BF),
            pltpu.VMEM((PER, ROWS, SLOT), BF),
            pltpu.VMEM((NQ, PER, ROWS, SLOT), BF),
            pltpu.VMEM((NP, CP, 4 * SLOT), BF),
            pltpu.VMEM((paths, F), BF),
            pltpu.VMEM((max(SIZES), CP), F32),
            pltpu.VMEM((paths, CP), BF),
            *[pltpu.VMEM((NY, CP, n), BF) for n in SIZES],
            pltpu.VMEM((FAR, paths, CP), BF),
            pltpu.VMEM((FAR + 1, NY * CP, CP), F32),
            pltpu.VMEM((FAR + 1, NY, CP, CP), BF),
            pltpu.VMEM((FAR + 1, CP, CP), BF),
            pltpu.VMEM((FAR + 1, 3, CP, CP), BF),
            pltpu.VMEM((FAR + 1, CP, CP), BF),
            pltpu.VMEM((FAR + 1, CP, CP), BF),
            pltpu.VMEM((2, NY, CP, CP), BF),
            pltpu.VMEM((2, NX, CP, CP), BF),
            dma((6,)), dma((CH,)), dma((PER,)), dma((PER,)), dma((3, 2)), dma((3, 2)),
            dma((CH, 3)), dma((CH, 3)), dma((FAR, CH)), dma((FAR, CH)),
            dma((FAR + 1, 3)), dma((FAR + 1, 3)),
            dma((FAR + 1,)), dma((2, NY)), dma((FAR + 1,)), dma((2, NX)),
        ],
        compiler_params=pltpu.CompilerParams(
            collective_id=0, has_side_effects=True, vmem_limit_bytes=67043328),
    )(factors, loadings, *[a.reshape(count // CP, CP) for a in (notional, strike, curvature)],
      trade_cpty[None, :])
    shapes = [(exposure.shape, BF), (moment.shape, F32)]
    anywhere = pl.BlockSpec(memory_space=pl.ANY)
    exposure, moment = pl.pallas_call(
        hand_out,
        out_shape=tuple(jax.ShapeDtypeStruct(*s) for s in shapes),
        in_specs=[anywhere] * 2,
        out_specs=(anywhere,) * 2,
        scratch_shapes=[*[pltpu.VMEM(*s) for s in shapes], dma((2, 4)), dma((2, 4))],
        compiler_params=pltpu.CompilerParams(vmem_limit_bytes=67043328),
    )(exposure, moment)
    return exposure, moment.reshape(NY * CP, CP)


def solution(mesh):
    in_specs = (P(None, "paths"), P(None, "cpty"), P("cpty"), P("cpty"), P("cpty"), P("cpty"))
    out_specs = (P("paths", "cpty"), P("paths", "cpty"))
    return jax.shard_map(
        on_device, mesh=mesh, in_specs=in_specs, out_specs=out_specs, check_vma=False
    )
```

```python
import jax
import jax.numpy as jnp
from jax import lax
from jax.experimental import pallas as pl
from jax.experimental.pallas import tpu as pltpu
from jax.sharding import PartitionSpec as P

NP, NX, NZ, NY = 8, 4, 8, 4
FAR = 4
CP = 128
ROWS = 80
SLOT = 128
F = 64
SIZES = (640, 512, 384)
STARTS = (0, 640, 1152)
CH = len(SIZES)
NQ, PER = 4, 8
BF, F32 = jnp.bfloat16, jnp.float32
NT = (((1,), (1,)), ((), ()))


def remote(src, dst, ssem, rsem, p, c):
    return pltpu.make_async_remote_copy(
        src_ref=src, dst_ref=dst, send_sem=ssem, recv_sem=rsem,
        device_id={"paths": p, "cpty": c}, device_id_type=pl.DeviceIdType.MESH,
    )


def kernel(fac_hbm, load_hbm, not_hbm, str_hbm, cur_hbm, id_hbm, exp_ref, mom_ref,
           fac_ref, term_in, id_ref, desc, pack, trades, hot, ft, net, own, at0, at1, at2,
           ring_in, acc, rsb, mid, rr, keep, turn, fa, fb, sin,
           sout, s1, r1, s2, r2, sy, ry, sz, rz, srs, rrs, sa, ra, sb, rb):
    p = lax.axis_index("paths")
    c = lax.axis_index("cpty")
    z, y = c // NY, c % NY
    at = (at0, at1, at2)
    paths = fac_ref.shape[1]
    count = id_ref.shape[1]
    quarter = 2 * (p // 2 % 2) + p % 2
    first = lax.rem(quarter - c + NZ * NY, NQ)
    targets = [first + NQ * i for i in range(PER)]
    x, core = p // 2, p % 2
    sign = 1 - 2 * core
    ahead, behind = lax.rem(z - sign + NZ, NZ), lax.rem(z + sign + NZ, NZ)
    y_ahead, y_back = lax.rem(y - sign + NY, NY), lax.rem(y + sign + NY, NY)

    loads = [
        pltpu.make_async_copy(src, dst, sin.at[i])
        for i, (src, dst) in enumerate((
            (id_hbm, id_ref), (not_hbm, term_in.at[0]), (str_hbm, term_in.at[1]),
            (cur_hbm, term_in.at[2]), (load_hbm, desc.at[0:F, :]), (fac_hbm, fac_ref)))
    ]
    for copy in loads:
        copy.start()

    barrier = pltpu.get_barrier_semaphore()

    def greet(pp, cc):
        pl.semaphore_signal(barrier, inc=1, device_id={"paths": pp, "cpty": cc},
                            device_id_type=pl.DeviceIdType.MESH)

    for k in targets:
        @pl.when(k != c)
        def _(k=k):
            greet(p, k)
    for r in range(1, NP):
        greet(lax.rem(p + r, NP), c)
    greet(p, ahead * NY + y)
    greet(p, behind * NY + y)
    for r in range(1, NY):
        greet(p, z * NY + lax.rem(y + r, NY))

    loads[0].wait()

    ids = id_ref[...]
    owner = ids // CP
    block = 256
    upper = (lax.broadcasted_iota(jnp.int32, (block, block), 0)
             < lax.broadcasted_iota(jnp.int32, (block, block), 1)).astype(BF)
    eq = (lax.broadcasted_iota(jnp.int32, (NZ * NY, count), 0) == owner).astype(F32)
    base = jnp.zeros((NZ * NY, 1), F32)
    ranks = []
    for b in range(count // block):
        part = eq[:, b * block:(b + 1) * block]
        before = jnp.dot(part.astype(BF), upper, preferred_element_type=F32) + base
        base = base + jnp.sum(part, axis=1, keepdims=True)
        ranks.append(jnp.sum(part * before, axis=0, keepdims=True))
    rank = jnp.concatenate(ranks, axis=1).astype(jnp.int32)
    mine = lax.rem(owner + c, NQ) == quarter
    code = jnp.where(mine, (owner // NQ) * SLOT + rank, -1)
    for copy in loads[1:5]:
        copy.wait()
    line = lax.broadcasted_iota(jnp.int32, (ROWS - F, count), 0)
    extra = jnp.where(line == 3, (ids % CP).astype(F32), 0.0)
    for i in range(3):
        cells = term_in[i].astype(F32)
        flat = jnp.concatenate([cells[k:k + 1, :] for k in range(count // CP)], axis=1)
        extra = jnp.where(line == i, flat, extra)
    desc[F:ROWS, :] = extra.astype(BF)
    total = jnp.zeros((ROWS, PER * SLOT), F32)
    step = 512
    for b in range(count // step):
        cols = slice(b * step, (b + 1) * step)
        chosen = (lax.broadcasted_iota(jnp.int32, (PER * SLOT, step), 0) == code[:, cols]).astype(F32).astype(BF)
        total = total + lax.dot_general(desc[:, cols], chosen, NT, preferred_element_type=F32)
    for i in range(PER):
        pack[i] = total[:, i * SLOT:(i + 1) * SLOT].astype(BF)

    pl.semaphore_wait(barrier, NP - 1 + 2 + NY - 1 + PER - (lax.rem(2 * c, NQ) == quarter).astype(jnp.int32))

    place = c // NQ
    for offset in (4, 3, 5, 2, 6, 1, 7, 0):
        i = lax.rem(z + offset, PER)
        copy = remote(pack.at[i], trades.at[quarter, place], s1.at[i], r1.at[place], p, first + NQ * i)
        if offset:
            copy.start()
        else:
            @pl.when(first != y)
            def _(copy=copy):
                copy.start()

            @pl.when(first == y)
            def _(i=i):
                trades[quarter, place] = pack[i]
    loads[5].wait()
    ft[...] = jnp.transpose(fac_ref[...].astype(F32)).astype(BF)
    for i, k in enumerate(targets):
        arrive = remote(pack.at[i], trades.at[quarter, i], s1.at[i], r1.at[i], p, k)

        @pl.when(k != c)
        def _(arrive=arrive):
            arrive.wait_recv()
    sends = []

    def go(copy):
        copy.start()
        sends.append(copy)

    x_ahead = lax.rem(x - sign + NX, NX)
    partner = 2 * x + 1 - core
    own_q, mate_q = quarter, quarter + 1 - 2 * core
    beside_q, last_q = lax.rem(own_q + 2, NQ), lax.rem(mate_q + 2, NQ)

    def half(part, h):
        return trades.at[part, pl.ds(4 * h, 4)]

    def give(i, h):
        part = beside_q if i == 2 else own_q
        to = 2 * x_ahead + core if i == 1 else partner
        return remote(half(part, h), half(part, h), s2.at[i, h], r2.at[i, h], to, c)

    def given(i, h):
        part = (mate_q, beside_q, last_q)[i]
        remote(half(part, h), half(part, h), s2.at[i, h], r2.at[i, h], partner, c).wait_recv()

    def span(j):
        return slice(STARTS[j], STARTS[j] + SIZES[j])

    def cut(j):
        return pl.ds(STARTS[j], SIZES[j])

    def tile_of(g, h):
        return jnp.concatenate([trades[g, 4 * h + i] for i in range(4)], axis=1)

    def price(j, g, h):
        full = tile_of(g, h)
        terms = full[F:ROWS, :].astype(F32)
        lin = jnp.dot(ft[span(j), :], full[0:F, :], preferred_element_type=F32)
        value = terms[0:1, :] * (lin + terms[2:3, :] * jnp.tanh(lin - terms[1:2, :]))
        return lax.dot_general(value.astype(BF), hot[2 * g + h], NT, preferred_element_type=F32)

    def ring(s, j):
        src = own.at[cut(j)] if s == 0 else ring_in.at[s - 1, cut(j)]
        return remote(src, ring_in.at[s, cut(j)], sz.at[s, j], rz.at[s, j], p, ahead * NY + y)

    def side(j, way):
        origin = y if way < 2 else y_back
        target = y_back if way == 1 else y_ahead
        return remote(at[j].at[origin], at[j].at[origin], sy.at[j, way], ry.at[j, way], p, z * NY + target)

    def side_wait(j, way):
        origin = (y_back, y_ahead, lax.rem(y + 2, NY))[way]
        remote(at[j].at[origin], at[j].at[origin], sy.at[j, way], ry.at[j, way], p, z * NY + y_back).wait_recv()

    def add(d, j, value, start):
        if start:
            acc[d] = value
        else:
            acc[d] += value

    def left(j):
        return at[j][...].reshape(NY * CP, SIZES[j])

    def dots(d, j):
        right = own[span(j), :] if d == 0 else ring_in[d - 1, span(j), :]
        add(d, j, jnp.dot(left(j), right, preferred_element_type=F32), j == 0)

    def cell(d):
        return lax.rem(z + sign * d + NZ, NZ)

    near_x, wide_x = x + 1 - 2 * (x % 2), NX - 1 - x
    first_x = near_x + core * (wide_x - near_x)
    second_x = wide_x + core * (near_x - wide_x)
    passed = 6 - x - first_x - second_x

    def tile(d, i):
        return acc[d, pl.ds(pl.multiple_of(i * CP, CP), CP), :]

    def reduce(d, i):
        if d < 3:
            src, to = ((rsb.at[d, first_x], first_x), (rsb.at[d, passed], first_x), (mid.at[d], second_x))[i]
        else:
            to = lax.rem(x + i + 1, NX)
            src = rsb.at[d, to]
        return remote(src, rr.at[d, i], srs.at[d, i], rrs.at[d, i], 2 * to + core, c)

    def ship(d):
        rsb[d] = acc[d].reshape(NY, CP, CP).astype(BF)
        for i in ((1, 0) if d < 3 else (1, 0, 2)):
            go(reduce(d, i))

    def pass_on(d):
        reduce(d, 1).wait_recv()
        mid[d] = (tile(d, second_x) + rr[d, 1].astype(F32)).astype(BF)
        go(reduce(d, 2))

    def turned(d):
        return remote(turn.at[d], fa.at[core, y], sa.at[d], ra.at[core, y], cell(d), z * NY + x)

    def turned_home(d):
        return (cell(d) == p) & (x == y)

    def direct(d):
        return remote(keep.at[d], fb.at[core, x], sb.at[d], rb.at[core, x], z, cell(d) * NY + y)

    def collect(d):
        whole = tile(d, x)
        for i in ((0, 2) if d < 3 else (0, 1, 2)):
            reduce(d, i).wait_recv()
            whole = whole + rr[d, i].astype(F32)
        whole = whole * (1.0 / (paths * NP))
        if 0 < d < FAR:
            keep[d] = whole.astype(BF)
            go(direct(d))
        turn[d] = jnp.transpose(whole).astype(BF)

        @pl.when(jnp.logical_not(turned_home(d)))
        def _():
            turned(d).start()

        @pl.when(turned_home(d))
        def _():
            fa[core, y] = turn[d]

    def out(j):
        return pltpu.make_async_copy(own.at[cut(j)], exp_ref.at[cut(j)], sout.at[j])

    def relay(s, j):
        ring(s - 1, j).wait_recv()
        go(ring(s, j))

    def side_relay(j):
        side_wait(j, 0)
        go(side(j, 2))
        side_wait(j, 1)

    def far(j):
        ring(FAR - 1, j).wait_recv()
        dots(FAR, j)

    for j in range(CH):
        here = net.at[0:SIZES[j], :]

        def take(g, halves=(0, 1)):
            for h in halves:
                label = tile_of(g, h)[F:ROWS, :].astype(F32)[3:4, :]
                hot[2 * g + h] = (lax.broadcasted_iota(jnp.int32, (CP, 4 * SLOT), 0).astype(F32) == label).astype(F32).astype(BF)
            return sum(price(0, g, h) for h in halves)

        if j == 0:
            for i in (1, 0):
                for h in range(2):
                    go(give(i, h))
            here[...] = take(own_q)
            for h in range(2):
                given(0, h)
            here[...] += take(mate_q)
            for h in range(2):
                given(1, h)
                go(give(2, h))
            here[...] += take(beside_q)
            given(2, 0)
            here[...] += take(last_q, (0,))
            given(2, 1)
            here[...] += take(last_q, (1,))
        else:
            here[...] = jnp.zeros_like(here)
            for g in range(NQ):
                for h in range(2):
                    here[...] += price(j, g, h)
        block_f = jnp.maximum(here[...], 0.0)
        block_b = block_f.astype(BF)
        own[span(j), :] = block_b
        at[j][y] = jnp.transpose(block_f).astype(BF)
        go(ring(0, j))
        out(j).start()
        go(side(j, 0))
        go(side(j, 1))
        if j == 1:
            relay(1, 0)
    relay(1, 1)
    side_relay(0)
    relay(2, 0)
    side_relay(1)
    relay(1, 2)
    relay(2, 1)
    side_relay(2)
    side_wait(0, 2)
    for d in (0, 1, 2):
        dots(d, 0)
    relay(2, 2)
    relay(3, 0)
    dots(3, 0)
    side_wait(1, 2)
    for d in (0, 1, 2):
        dots(d, 1)
    relay(3, 1)
    side_wait(2, 2)
    for d in (0, 1, 2):
        dots(d, 2)
        ship(d)
    relay(3, 2)
    for j in (1, 2):
        dots(3, j)
    ship(3)
    far(0)
    pass_on(0)
    pass_on(1)
    far(1)
    pass_on(2)
    far(2)
    ship(FAR)
    for d in (3, 0, 1, 2, FAR):
        collect(d)

    delta = lax.rem(p - z + NZ, NZ)
    mom_ref[...] = jnp.zeros_like(mom_ref)
    for k in range(2):
        near = (delta <= FAR) if k == 0 else ((delta >= FAR) | (delta == 0))
        away = (delta > FAR) if k == 0 else ((delta < FAR) & (delta > 0))
        for i in range(NY):
            @pl.when(near & jnp.logical_not((core == k) & (i == y) & (x == y)))
            def _(k=k, i=i):
                remote(turn.at[0], fa.at[k, i], sa.at[0], ra.at[k, i], 2 * y + k, z * NY + i).wait_recv()

            @pl.when(near)
            def _(k=k, i=i):
                mom_ref[i] += fa[k, i].astype(F32)

            @pl.when(away)
            def _(k=k, i=i):
                remote(turn.at[0], fb.at[k, i], sb.at[0], rb.at[k, i], 2 * i + k, p * NY + y).wait_recv()
                mom_ref[i] += fb[k, i].astype(F32)

    for j in range(CH):
        out(j).wait()
    for i, k in enumerate(targets):
        copy = remote(pack.at[i], trades.at[quarter, place], s1.at[i], r1.at[place], p, k)

        @pl.when(k != c)
        def _(copy=copy):
            copy.wait_send()
    for copy in sends:
        copy.wait_send()
    for d in range(FAR + 1):
        @pl.when(jnp.logical_not(turned_home(d)))
        def _(d=d):
            turned(d).wait_send()


def hand_out(exp_in, mom_in, exp_out, mom_out, exp_buf, mom_buf, sin, sout):
    steps = []
    for a, (src, buf, dst) in enumerate(((exp_in, exp_buf, exp_out), (mom_in, mom_buf, mom_out))):
        rows = src.shape[0] // 4
        for i in range(4):
            part = pl.ds(i * rows, rows)
            steps.append((
                pltpu.make_async_copy(src.at[part], buf.at[part], sin.at[a, i]),
                pltpu.make_async_copy(buf.at[part], dst.at[part], sout.at[a, i])))
    for get, _ in steps:
        get.start()
    for get, put in steps:
        get.wait()
        put.start()
    for _, put in steps:
        put.wait()


def on_device(factors, loadings, notional, strike, curvature, trade_cpty):
    count, paths = loadings.shape[1], factors.shape[1]
    vmem = pl.BlockSpec(memory_space=pltpu.VMEM)
    dma = pltpu.SemaphoreType.DMA
    exposure, moment = pl.pallas_call(
        kernel,
        out_shape=(jax.ShapeDtypeStruct((paths, CP), BF), jax.ShapeDtypeStruct((NY, CP, CP), F32)),
        in_specs=[pl.BlockSpec(memory_space=pl.ANY)] * 6,
        out_specs=(pl.BlockSpec(memory_space=pl.ANY), vmem),
        scratch_shapes=[
            pltpu.VMEM((F, paths), BF),
            pltpu.VMEM((3, count // CP, CP), BF),
            pltpu.VMEM((1, count), jnp.int32),
            pltpu.VMEM((ROWS, count), BF),
            pltpu.VMEM((PER, ROWS, SLOT), BF),
            pltpu.VMEM((NQ, PER, ROWS, SLOT), BF),
            pltpu.VMEM((NP, CP, 4 * SLOT), BF),
            pltpu.VMEM((paths, F), BF),
            pltpu.VMEM((max(SIZES), CP), F32),
            pltpu.VMEM((paths, CP), BF),
            *[pltpu.VMEM((NY, CP, n), BF) for n in SIZES],
            pltpu.VMEM((FAR, paths, CP), BF),
            pltpu.VMEM((FAR + 1, NY * CP, CP), F32),
            pltpu.VMEM((FAR + 1, NY, CP, CP), BF),
            pltpu.VMEM((FAR + 1, CP, CP), BF),
            pltpu.VMEM((FAR + 1, 3, CP, CP), BF),
            pltpu.VMEM((FAR + 1, CP, CP), BF),
            pltpu.VMEM((FAR + 1, CP, CP), BF),
            pltpu.VMEM((2, NY, CP, CP), BF),
            pltpu.VMEM((2, NX, CP, CP), BF),
            dma((6,)), dma((CH,)), dma((PER,)), dma((PER,)), dma((3, 2)), dma((3, 2)),
            dma((CH, 3)), dma((CH, 3)), dma((FAR, CH)), dma((FAR, CH)),
            dma((FAR + 1, 3)), dma((FAR + 1, 3)),
            dma((FAR + 1,)), dma((2, NY)), dma((FAR + 1,)), dma((2, NX)),
        ],
        compiler_params=pltpu.CompilerParams(
            collective_id=0, has_side_effects=True, vmem_limit_bytes=67043328),
    )(factors, loadings, *[a.reshape(count // CP, CP) for a in (notional, strike, curvature)],
      trade_cpty[None, :])
    shapes = [(exposure.shape, BF), (moment.shape, F32)]
    anywhere = pl.BlockSpec(memory_space=pl.ANY)
    exposure, moment = pl.pallas_call(
        hand_out,
        out_shape=tuple(jax.ShapeDtypeStruct(*s) for s in shapes),
        in_specs=[anywhere] * 2,
        out_specs=(anywhere,) * 2,
        scratch_shapes=[*[pltpu.VMEM(*s) for s in shapes], dma((2, 4)), dma((2, 4))],
        compiler_params=pltpu.CompilerParams(vmem_limit_bytes=67043328),
    )(exposure, moment)
    return exposure, moment.reshape(NY * CP, CP)


def solution(mesh):
    in_specs = (P(None, "paths"), P(None, "cpty"), P("cpty"), P("cpty"), P("cpty"), P("cpty"))
    out_specs = (P("paths", "cpty"), P("paths", "cpty"))
    return jax.shard_map(
        on_device, mesh=mesh, in_specs=in_specs, out_specs=out_specs, check_vma=False
    )
```
